32 devices in a mesh: graph: 2 (over x), col: 4 (over z), row: 4 (over y, core).
Axes of the slice: x: 2, y: 2, z: 4, core: 2. Of those that a mesh axis runs over, the one named last changes fastest.
Arguments:
- flow_init: float32 [8192, 4096], P(('graph', 'row'), 'col'), parts along dimension 0
- flow_graph: float32 [8192, 4096], P(('graph', 'row'), 'col'), parts along dimension 0
Outputs:
- output: float32 [8192, 4096], P(('graph', 'row'), 'col'), parts along dimension 0
There are 2 independent parts. The reference program is written for one: setup_inputs(seed, part) draws one part's arguments, and reference() takes and returns one part's arrays. A program takes and returns all parts, laid end to end along the dimension named above; each array names one.
All inputs are finite; a program needn't handle non-finite values.
Results may differ from the reference program's by a relative error of at most 0.001.
Values are sent between devices in bfloat16 or wider.
A program may use at most 1 GiB of HBM per device.

```python
import jax
import jax.numpy as jnp
from jax import lax

N = 4096
ITERATIONS = 3


def draw_flow(key, floor_level):
    key_width, key_noise = jax.random.split(key)
    node_index = jnp.arange(N, dtype=jnp.float32)
    band_width = N * jax.random.uniform(key_width, (N,), minval=0.01, maxval=0.15)
    raw_offset = jnp.abs(node_index[:, None] - node_index[None, :])
    cyclic_dist = jnp.minimum(raw_offset, N - raw_offset)
    noise_fac = jax.random.uniform(key_noise, (N, N), minval=0.5, maxval=1.5)
    weight = (floor_level + jnp.exp(-cyclic_dist / band_width[None, :])) * noise_fac
    return weight / jnp.sum(weight, axis=0, keepdims=True)


def setup_inputs(seed: int = 0, part: int = 0) -> dict:
    key = jax.random.fold_in(jax.random.key(seed), part)
    key_init, key_graph = jax.random.split(key)
    flow_init = N * draw_flow(key_init, 0.05)
    flow_graph = draw_flow(key_graph, 0.1)
    return {"flow_init": flow_init.astype(jnp.float32), "flow_graph": flow_graph.astype(jnp.float32)}


def reference(flow_init, flow_graph):
    graph_bf = flow_graph.astype(jnp.bfloat16)

    def iteration(flow_cur, unused):
        expanded = jnp.dot(flow_cur.astype(jnp.bfloat16), graph_bf, preferred_element_type=jnp.float32)
        inflated = expanded * expanded
        col_sum = jnp.sum(inflated, axis=0)
        return inflated * (N / col_sum), None

    flow_out, _ = lax.scan(iteration, flow_init, None, length=ITERATIONS)
    return flow_out
```

```python
import functools

import jax
import jax.numpy as jnp
from jax import lax
from jax.experimental import pallas as pl
from jax.experimental.pallas import tpu as pltpu
from jax.sharding import PartitionSpec as P

ITERATIONS = 3
CHUNKS = 8
TAIL_CHUNKS = 8
MESH = pl.DeviceIdType.MESH


def mcl_kernel(a_hbm, g_hbm, m_out, s_out, g, a, snd, acc, fin, psum, ar, sc, scin,
               load_sem, rg, rp, ra, send_sem, fin_send, ar_send, ar_recv, fin_recv, sc_sem, out_sem):
    n_col = g.shape[0]
    blk = g.shape[2]
    n = g.shape[1]
    half = blk // 2
    rows_c = blk // CHUNKS
    rows_t = half // TAIL_CHUNKS

    z = lax.axis_index("col")
    r = lax.axis_index("row")
    y = r // 2
    c = r % 2
    side = z // 2
    middle = jnp.logical_or(z == 1, z == 2)
    zm = 1 + side
    zc = 3 * side
    zmo = 2 - side
    zco = 3 - 3 * side
    r_y = 2 * (1 - y) + c
    r_p = 2 * y + 1 - c

    def dev(zq, rq):
        return {"col": zq, "row": rq}

    def remote(src, dst, ssem, rsem, d):
        return pltpu.make_async_remote_copy(
            src_ref=src, dst_ref=dst, send_sem=ssem, recv_sem=rsem, device_id=d, device_id_type=MESH)

    def g_piece(zq, rq, ch):
        return g.at[zq, pl.ds(pl.multiple_of(rq * blk + ch * rows_c, rows_c), rows_c), :]

    def g_block(zq, rq):
        return g.at[zq, pl.ds(pl.multiple_of(rq * blk, blk), blk), :]

    def send_g(link, zq, rq, ch, d):
        piece = g_piece(zq, rq, ch)
        remote(piece, piece, send_sem.at[link, zq, rq // 2], rg.at[zq, rq // 2, ch], d).start()

    def send_g_partner(zq, rq, ch):
        piece = g_piece(zq, rq, ch)
        remote(piece, piece, send_sem.at[2, zq, rq // 2], rp.at[zq, rq // 2, ch], dev(zm, r_p)).start()

    def wait_g(zq, rq, ch):
        piece = g_piece(zq, rq, ch)
        remote(piece, piece, send_sem.at[0, 0, 0], rg.at[zq, rq // 2, ch], dev(z, r)).wait_recv()

    def wait_g_partner(zq, rq, ch):
        piece = g_piece(zq, rq, ch)
        remote(piece, piece, send_sem.at[0, 0, 0], rp.at[zq, rq // 2, ch], dev(z, r)).wait_recv()

    def wait_sent(link, zq, rq):
        block = g_block(zq, rq)
        remote(block, block, send_sem.at[link, zq, rq // 2], rg.at[0, 0, 0], dev(z, r)).wait_send()

    def a_cols(zq):
        return a.at[:, pl.ds(pl.multiple_of(zq * blk, blk), blk)]

    def send_a(src, dst, link, idx, d):
        return remote(src, dst, send_sem.at[link, idx, 2], ra.at[idx], d)

    barrier = pltpu.get_barrier_semaphore()

    @pl.when(middle)
    def _():
        for dz in range(2):
            for dr in range(n_col):
                peer_z = zm if dz == 0 else zmo
                peer_r = (r + dr) % n_col
                if dz == 0 and dr == 0:
                    peer_z = zc
                pl.semaphore_signal(barrier, inc=1, device_id=dev(peer_z, peer_r), device_id_type=MESH)

    @pl.when(jnp.logical_not(middle))
    def _():
        pl.semaphore_signal(barrier, inc=1, device_id=dev(zm, r), device_id_type=MESH)
        pl.semaphore_signal(barrier, inc=1, device_id=dev(zc, r_y), device_id_type=MESH)

    loads = []
    for h in range(2):
        loads.append(pltpu.make_async_copy(g_hbm.at[pl.ds(h * half, half), :], acc.at[2 + h], load_sem.at[2 + h]))
    for h in range(2):
        loads.append(pltpu.make_async_copy(a_hbm.at[pl.ds(h * half, half), :], acc.at[h], load_sem.at[h]))
    for load in loads:
        load.start()
    for h in range(2):
        loads[h].wait()
        g[z, pl.ds(pl.multiple_of(r * blk + h * half, half), half), :] = acc[2 + h].astype(jnp.bfloat16)
    for h in range(2):
        loads[2 + h].wait()
    snd[0] = acc[1 - side].astype(jnp.bfloat16)
    a[:, pl.ds(pl.multiple_of(z * blk, blk), blk)] = acc[side].astype(jnp.bfloat16)

    @pl.when(jnp.logical_not(middle))
    def _():
        pl.semaphore_wait(barrier, 2)

        @pl.loop(0, CHUNKS)
        def _(ch):
            send_g(3, z, r, ch, dev(zm, r))
            send_g(1, z, r, ch, dev(zc, r_y))

        to_other = send_a(snd.at[0], snd.at[1], 3, 0, dev(zm, r))
        to_middle = send_a(a_cols(z), a_cols(z), 3, 1, dev(zm, r))
        to_other.start()
        to_middle.start()

        @pl.loop(0, CHUNKS)
        def _(ch):
            wait_g(z, r_y, ch)
            send_g(3, z, r_y, ch, dev(zm, r))

        wait_sent(3, z, r)
        wait_sent(1, z, r)
        wait_sent(3, z, r_y)
        to_other.wait_send()
        to_middle.wait_send()

        remote(fin.at[side], fin.at[side], fin_send.at[0], fin_recv.at[1, 0], dev(z, r)).wait_recv()
        own = pltpu.make_async_copy(fin.at[side], m_out.at[pl.ds(pl.multiple_of(side * half, half), half), :], out_sem.at[0])
        own.start()

        @pl.loop(0, TAIL_CHUNKS)
        def _(ch):
            piece = fin.at[1 - side, pl.ds(pl.multiple_of(ch * rows_t, rows_t), rows_t), :]
            remote(piece, piece, fin_send.at[0], fin_recv.at[2, ch], dev(z, r)).wait_recv()
            dst = m_out.at[pl.ds(pl.multiple_of((1 - side) * half + ch * rows_t, rows_t), rows_t), :]
            pltpu.make_async_copy(piece, dst, out_sem.at[1]).start()

        remote(scin, scin, sc_sem.at[0], sc_sem.at[1], dev(z, r)).wait_recv()
        scale_copy = pltpu.make_async_copy(scin, s_out, out_sem.at[2])
        scale_copy.start()
        own.wait()
        pltpu.make_async_copy(
            fin.at[1 - side], m_out.at[pl.ds(pl.multiple_of((1 - side) * half, half), half), :], out_sem.at[1]).wait()
        scale_copy.wait()

    @pl.when(middle)
    def _():
        pl.semaphore_wait(barrier, 2 * n_col)
        other = dev(zmo, r)
        across = dev(zm, r_y)
        corner = dev(zc, r)
        me = side * n_col + r

        @pl.loop(0, CHUNKS)
        def _(ch):
            send_g(0, zm, r, ch, other)
            send_g(1, zm, r, ch, across)
            send_g_partner(zm, r, ch)

        own_a = send_a(snd.at[0], a_cols(zm), 0, 2, other)
        own_a.start()

        @pl.loop(0, CHUNKS)
        def _(ch):
            wait_g(zmo, r, ch)
            send_g(1, zmo, r, ch, across)
            send_g_partner(zmo, r, ch)
            wait_g(zc, r, ch)
            send_g(0, zc, r, ch, other)
            send_g_partner(zc, r, ch)
            wait_g(zm, r_y, ch)
            send_g_partner(zm, r_y, ch)

        relay_a = send_a(snd.at[1], a_cols(zc), 0, 3, other)

        @pl.loop(0, CHUNKS // 2)
        def _(ch):
            wait_g(zmo, r_y, ch)
            send_g_partner(zmo, r_y, ch)

        remote(snd.at[1], snd.at[1], send_sem.at[0, 0, 2], ra.at[0], dev(z, r)).wait_recv()
        relay_a.start()

        @pl.loop(0, CHUNKS // 2)
        def _(ch):
            wait_g(zco, r, ch)
            send_g(1, zco, r, ch, across)
            send_g_partner(zco, r, ch)
            wait_g(zmo, r_y, ch + CHUNKS // 2)
            send_g_partner(zmo, r_y, ch + CHUNKS // 2)

        @pl.loop(0, CHUNKS)
        def _(ch):
            @pl.when(ch < CHUNKS // 2)
            def _():
                wait_g(zco, r, ch + CHUNKS // 2)
                send_g(1, zco, r, ch + CHUNKS // 2, across)
                send_g_partner(zco, r, ch + CHUNKS // 2)
            wait_g(zc, r_y, ch)
            send_g_partner(zc, r_y, ch)
            wait_g(zco, r_y, ch)
            send_g_partner(zco, r_y, ch)

        for idx, zq in ((1, zc), (2, zmo), (3, zco)):
            remote(a_cols(zq), a_cols(zq), send_sem.at[0, 0, 2], ra.at[idx], dev(z, r)).wait_recv()

        @pl.loop(0, CHUNKS)
        def _(ch):
            for zq in range(n_col):
                for yq in range(2):
                    wait_g_partner(zq, 2 * yq + 1 - c, ch)

        tile = 256
        per_block = blk // tile

        def expand(zq):
            @pl.loop(0, per_block)
            def _(j):
                cols = pl.ds(pl.multiple_of(j * tile, tile), tile)
                acc[zq, :, cols] = jnp.dot(a[...], g[zq, :, cols], preferred_element_type=jnp.float32)

        def inflate(t, zq):
            total = jnp.zeros((8, blk), jnp.float32)
            step = 64

            def body(i, total):
                rows = pl.ds(pl.multiple_of(i * step, step), step)
                value = acc[zq, rows, :]
                value = value * value
                acc[zq, rows, :] = value
                return total + jnp.sum(value.reshape(step // 8, 8, blk), axis=0)

            total = lax.fori_loop(0, half // step, body, total)
            psum[t, zq] = jnp.sum(total, axis=0, keepdims=True)

        def ar_copy(t, k, peer_z, peer_r):
            return remote(psum.at[t], ar.at[t, me], ar_send.at[t, k], ar_recv.at[t, me], dev(peer_z, peer_r))

        def peers():
            for dz in range(2):
                for dr in range(n_col):
                    if dz or dr:
                        yield dz * n_col + dr, (zmo if dz else zm), (r + dr) % n_col

        def column_scales(t):
            for k, pz, pr in peers():
                ar_copy(t, k, pz, pr).start()
            ar[t, me] = psum[t]
            for k, pz, pr in peers():
                src = (1 - side if k >= n_col else side) * n_col + pr
                remote(psum.at[t], ar.at[t, src], ar_send.at[t, k], ar_recv.at[t, src], dev(z, r)).wait_recv()
            total = ar[t, 0]
            for src in range(1, 2 * n_col):
                total = total + ar[t, src]
            sc[...] = n / total

        for t in range(ITERATIONS - 1):
            @pl.loop(0, n_col)
            def _(zq):
                expand(zq)
                inflate(t, zq)

            column_scales(t)

            @pl.loop(0, n_col)
            def _(zq):
                a[:, pl.ds(pl.multiple_of(zq * blk, blk), blk)] = (acc[zq] * sc[zq]).astype(jnp.bfloat16)

        t = ITERATIONS - 1
        expand(zco)
        inflate(t, zco)

        def tail_piece(ref, lead, ch):
            return ref.at[lead, pl.ds(pl.multiple_of(ch * rows_t, rows_t), rows_t), :]

        @pl.loop(0, TAIL_CHUNKS)
        def _(ch):
            remote(tail_piece(acc, zco, ch), tail_piece(fin, 1, ch), fin_send.at[0], fin_recv.at[2, ch], other).start()

        expand(zc)
        inflate(t, zc)
        to_corner = remote(acc.at[zc], fin.at[side], fin_send.at[1], fin_recv.at[1, 0], corner)
        to_corner.start()
        expand(zmo)
        inflate(t, zmo)
        to_other = remote(acc.at[zmo], fin.at[0], fin_send.at[2], fin_recv.at[0, 0], other)
        to_other.start()
        expand(zm)
        inflate(t, zm)
        own = pltpu.make_async_copy(acc.at[zm], m_out.at[pl.ds(pl.multiple_of(side * half, half), half), :], out_sem.at[0])
        own.start()
        column_scales(t)
        scale_corner = remote(sc.at[zc], scin, sc_sem.at[0], sc_sem.at[1], corner)
        scale_corner.start()
        scale_own = pltpu.make_async_copy(sc.at[zm], s_out, out_sem.at[2])
        scale_own.start()

        @pl.loop(0, TAIL_CHUNKS)
        def _(ch):
            piece = tail_piece(fin, 1, ch)
            remote(piece, piece, fin_send.at[0], fin_recv.at[2, ch], dev(z, r)).wait_recv()
            remote(piece, tail_piece(fin, 1 - side, ch), fin_send.at[3], fin_recv.at[2, ch], corner).start()

        remote(fin.at[0], fin.at[0], fin_send.at[0], fin_recv.at[0, 0], dev(z, r)).wait_recv()
        rest = pltpu.make_async_copy(
            fin.at[0], m_out.at[pl.ds(pl.multiple_of((1 - side) * half, half), half), :], out_sem.at[1])
        rest.start()

        wait_sent(0, zm, r)
        wait_sent(0, zc, r)
        wait_sent(1, zm, r)
        wait_sent(1, zmo, r)
        wait_sent(1, zco, r)
        for zq in range(n_col):
            for yq in range(2):
                wait_sent(2, zq, 2 * yq + c)
        own_a.wait_send()
        relay_a.wait_send()
        for t in range(ITERATIONS):
            for k, pz, pr in peers():
                ar_copy(t, k, pz, pr).wait_send()
        remote(acc.at[zco], fin.at[1], fin_send.at[0], fin_recv.at[0, 0], other).wait_send()
        to_corner.wait_send()
        to_other.wait_send()
        remote(fin.at[1], fin.at[1], fin_send.at[3], fin_recv.at[0, 0], corner).wait_send()
        scale_corner.wait_send()
        own.wait()
        rest.wait()
        scale_own.wait()


def solution(mesh):
    num_cols = mesh.shape["col"]
    num_rows = mesh.shape["row"]
    block_spec = P(("graph", "row"), "col")

    def device_step(init_blk, graph_blk):
        blk = init_blk.shape[0]
        n = blk * num_rows
        half = blk // 2
        any_spec = pl.BlockSpec(memory_space=pl.ANY)
        squares, scale = pl.pallas_call(
            mcl_kernel,
            out_shape=(jax.ShapeDtypeStruct((blk, blk), jnp.float32), jax.ShapeDtypeStruct((1, blk), jnp.float32)),
            in_specs=[any_spec, any_spec],
            out_specs=(any_spec, any_spec),
            scratch_shapes=[
                pltpu.VMEM((num_cols, n, blk), jnp.bfloat16),
                pltpu.VMEM((half, n), jnp.bfloat16),
                pltpu.VMEM((2, half, blk), jnp.bfloat16),
                pltpu.VMEM((num_cols, half, blk), jnp.float32),
                pltpu.VMEM((2, half, blk), jnp.float32),
                pltpu.VMEM((ITERATIONS, num_cols, 1, blk), jnp.float32),
                pltpu.VMEM((ITERATIONS, 2 * num_rows, num_cols, 1, blk), jnp.float32),
                pltpu.VMEM((num_cols, 1, blk), jnp.float32),
                pltpu.VMEM((1, blk), jnp.float32),
                pltpu.SemaphoreType.DMA((4,)),
                pltpu.SemaphoreType.DMA((num_cols, 2, CHUNKS)),
                pltpu.SemaphoreType.DMA((num_cols, 2, CHUNKS)),
                pltpu.SemaphoreType.DMA((4,)),
                pltpu.SemaphoreType.DMA((4, num_cols, 3)),
                pltpu.SemaphoreType.DMA((4,)),
                pltpu.SemaphoreType.DMA((ITERATIONS, 2 * num_rows)),
                pltpu.SemaphoreType.DMA((ITERATIONS, 2 * num_rows)),
                pltpu.SemaphoreType.DMA((3, TAIL_CHUNKS)),
                pltpu.SemaphoreType.DMA((2,)),
                pltpu.SemaphoreType.DMA((3,)),
            ],
            compiler_params=pltpu.CompilerParams(
                collective_id=0, has_side_effects=True, vmem_limit_bytes=67_000_000),
        )(init_blk, graph_blk)
        return squares * scale

    return jax.shard_map(device_step, mesh=mesh, in_specs=(block_spec, block_spec), out_specs=block_spec, check_vma=False)
```

```python
import functools

import jax
import jax.numpy as jnp
from jax import lax
from jax.experimental import pallas as pl
from jax.experimental.pallas import tpu as pltpu
from jax.sharding import PartitionSpec as P

ITERATIONS = 3
CHUNKS = 8
TAIL_CHUNKS = 8
MESH = pl.DeviceIdType.MESH


def mcl_kernel(a_hbm, g_hbm, m_out, s_out, g, a, snd, acc, fin, psum, ar, sc, scin,
               load_sem, rg, rp, ra, send_sem, fin_send, ar_send, ar_recv, fin_recv, sc_sem, out_sem):
    n_col = g.shape[0]
    blk = g.shape[2]
    n = g.shape[1]
    half = blk // 2
    rows_c = blk // CHUNKS
    rows_t = half // TAIL_CHUNKS

    z = lax.axis_index("col")
    r = lax.axis_index("row")
    y = r // 2
    c = r % 2
    side = z // 2
    middle = jnp.logical_or(z == 1, z == 2)
    zm = 1 + side
    zc = 3 * side
    zmo = 2 - side
    zco = 3 - 3 * side
    r_y = 2 * (1 - y) + c
    r_p = 2 * y + 1 - c

    def dev(zq, rq):
        return {"col": zq, "row": rq}

    def remote(src, dst, ssem, rsem, d):
        return pltpu.make_async_remote_copy(
            src_ref=src, dst_ref=dst, send_sem=ssem, recv_sem=rsem, device_id=d, device_id_type=MESH)

    def g_piece(zq, rq, ch):
        return g.at[zq, pl.ds(pl.multiple_of(rq * blk + ch * rows_c, rows_c), rows_c), :]

    def g_block(zq, rq):
        return g.at[zq, pl.ds(pl.multiple_of(rq * blk, blk), blk), :]

    def send_g(link, zq, rq, ch, d):
        piece = g_piece(zq, rq, ch)
        remote(piece, piece, send_sem.at[link, zq, rq // 2], rg.at[zq, rq // 2, ch], d).start()

    def send_g_partner(zq, rq, ch):
        piece = g_piece(zq, rq, ch)
        remote(piece, piece, send_sem.at[2, zq, rq // 2], rp.at[zq, rq // 2, ch], dev(zm, r_p)).start()

    def wait_g(zq, rq, ch):
        piece = g_piece(zq, rq, ch)
        remote(piece, piece, send_sem.at[0, 0, 0], rg.at[zq, rq // 2, ch], dev(z, r)).wait_recv()

    def wait_g_partner(zq, rq, ch):
        piece = g_piece(zq, rq, ch)
        remote(piece, piece, send_sem.at[0, 0, 0], rp.at[zq, rq // 2, ch], dev(z, r)).wait_recv()

    def wait_sent(link, zq, rq):
        block = g_block(zq, rq)
        remote(block, block, send_sem.at[link, zq, rq // 2], rg.at[0, 0, 0], dev(z, r)).wait_send()

    def a_cols(zq):
        return a.at[:, pl.ds(pl.multiple_of(zq * blk, blk), blk)]

    def send_a(src, dst, link, idx, d):
        return remote(src, dst, send_sem.at[link, idx, 2], ra.at[idx], d)

    barrier = pltpu.get_barrier_semaphore()

    @pl.when(middle)
    def _():
        for dz in range(2):
            for dr in range(n_col):
                peer_z = zm if dz == 0 else zmo
                peer_r = (r + dr) % n_col
                if dz == 0 and dr == 0:
                    peer_z = zc
                pl.semaphore_signal(barrier, inc=1, device_id=dev(peer_z, peer_r), device_id_type=MESH)

    @pl.when(jnp.logical_not(middle))
    def _():
        pl.semaphore_signal(barrier, inc=1, device_id=dev(zm, r), device_id_type=MESH)
        pl.semaphore_signal(barrier, inc=1, device_id=dev(zc, r_y), device_id_type=MESH)

    loads = []
    for h in range(2):
        loads.append(pltpu.make_async_copy(g_hbm.at[pl.ds(h * half, half), :], acc.at[2 + h], load_sem.at[2 + h]))
    for h in range(2):
        loads.append(pltpu.make_async_copy(a_hbm.at[pl.ds(h * half, half), :], acc.at[h], load_sem.at[h]))
    for load in loads:
        load.start()
    for h in range(2):
        loads[h].wait()
        g[z, pl.ds(pl.multiple_of(r * blk + h * half, half), half), :] = acc[2 + h].astype(jnp.bfloat16)
    for h in range(2):
        loads[2 + h].wait()
    snd[0] = acc[1 - side].astype(jnp.bfloat16)
    a[:, pl.ds(pl.multiple_of(z * blk, blk), blk)] = acc[side].astype(jnp.bfloat16)

    @pl.when(jnp.logical_not(middle))
    def _():
        pl.semaphore_wait(barrier, 2)

        @pl.loop(0, CHUNKS)
        def _(ch):
            send_g(3, z, r, ch, dev(zm, r))
            send_g(1, z, r, ch, dev(zc, r_y))

        to_other = send_a(snd.at[0], snd.at[1], 3, 0, dev(zm, r))
        to_middle = send_a(a_cols(z), a_cols(z), 3, 1, dev(zm, r))
        to_other.start()
        to_middle.start()

        @pl.loop(0, CHUNKS)
        def _(ch):
            wait_g(z, r_y, ch)
            send_g(3, z, r_y, ch, dev(zm, r))

        wait_sent(3, z, r)
        wait_sent(1, z, r)
        wait_sent(3, z, r_y)
        to_other.wait_send()
        to_middle.wait_send()

        remote(fin.at[side], fin.at[side], fin_send.at[0], fin_recv.at[1, 0], dev(z, r)).wait_recv()
        own = pltpu.make_async_copy(fin.at[side], m_out.at[pl.ds(pl.multiple_of(side * half, half), half), :], out_sem.at[0])
        own.start()

        @pl.loop(0, TAIL_CHUNKS)
        def _(ch):
            piece = fin.at[1 - side, pl.ds(pl.multiple_of(ch * rows_t, rows_t), rows_t), :]
            remote(piece, piece, fin_send.at[0], fin_recv.at[2, ch], dev(z, r)).wait_recv()
            dst = m_out.at[pl.ds(pl.multiple_of((1 - side) * half + ch * rows_t, rows_t), rows_t), :]
            pltpu.make_async_copy(piece, dst, out_sem.at[1]).start()

        remote(scin, scin, sc_sem.at[0], sc_sem.at[1], dev(z, r)).wait_recv()
        scale_copy = pltpu.make_async_copy(scin, s_out, out_sem.at[2])
        scale_copy.start()
        own.wait()
        pltpu.make_async_copy(
            fin.at[1 - side], m_out.at[pl.ds(pl.multiple_of((1 - side) * half, half), half), :], out_sem.at[1]).wait()
        scale_copy.wait()

    @pl.when(middle)
    def _():
        pl.semaphore_wait(barrier, 2 * n_col)
        other = dev(zmo, r)
        across = dev(zm, r_y)
        corner = dev(zc, r)
        me = side * n_col + r

        @pl.loop(0, CHUNKS)
        def _(ch):
            send_g(0, zm, r, ch, other)
            send_g(1, zm, r, ch, across)
            send_g_partner(zm, r, ch)

        own_a = send_a(snd.at[0], a_cols(zm), 0, 2, other)
        own_a.start()

        @pl.loop(0, CHUNKS)
        def _(ch):
            wait_g(zmo, r, ch)
            send_g(1, zmo, r, ch, across)
            send_g_partner(zmo, r, ch)
            wait_g(zc, r, ch)
            send_g(0, zc, r, ch, other)
            send_g_partner(zc, r, ch)
            wait_g(zm, r_y, ch)
            send_g_partner(zm, r_y, ch)

        relay_a = send_a(snd.at[1], a_cols(zc), 0, 3, other)

        @pl.loop(0, CHUNKS // 2)
        def _(ch):
            wait_g(zmo, r_y, ch)
            send_g_partner(zmo, r_y, ch)

        remote(snd.at[1], snd.at[1], send_sem.at[0, 0, 2], ra.at[0], dev(z, r)).wait_recv()
        relay_a.start()

        @pl.loop(0, CHUNKS // 2)
        def _(ch):
            wait_g(zco, r, ch)
            send_g(1, zco, r, ch, across)
            send_g_partner(zco, r, ch)
            wait_g(zmo, r_y, ch + CHUNKS // 2)
            send_g_partner(zmo, r_y, ch + CHUNKS // 2)

        @pl.loop(0, CHUNKS)
        def _(ch):
            @pl.when(ch < CHUNKS // 2)
            def _():
                wait_g(zco, r, ch + CHUNKS // 2)
                send_g(1, zco, r, ch + CHUNKS // 2, across)
                send_g_partner(zco, r, ch + CHUNKS // 2)
            wait_g(zc, r_y, ch)
            send_g_partner(zc, r_y, ch)
            wait_g(zco, r_y, ch)
            send_g_partner(zco, r_y, ch)

        for idx, zq in ((1, zc), (2, zmo), (3, zco)):
            remote(a_cols(zq), a_cols(zq), send_sem.at[0, 0, 2], ra.at[idx], dev(z, r)).wait_recv()

        @pl.loop(0, CHUNKS)
        def _(ch):
            for zq in range(n_col):
                for yq in range(2):
                    wait_g_partner(zq, 2 * yq + 1 - c, ch)

        tile = 256
        per_block = blk // tile

        def expand(zq):
            @pl.loop(0, per_block)
            def _(j):
                cols = pl.ds(pl.multiple_of(j * tile, tile), tile)
                acc[zq, :, cols] = jnp.dot(a[...], g[zq, :, cols], preferred_element_type=jnp.float32)

        def inflate(t, zq):
            total = jnp.zeros((8, blk), jnp.float32)
            step = 64

            def body(i, total):
                rows = pl.ds(pl.multiple_of(i * step, step), step)
                value = acc[zq, rows, :]
                value = value * value
                acc[zq, rows, :] = value
                return total + jnp.sum(value.reshape(step // 8, 8, blk), axis=0)

            total = lax.fori_loop(0, half // step, body, total)
            psum[t, zq] = jnp.sum(total, axis=0, keepdims=True)

        def ar_copy(t, k, peer_z, peer_r):
            return remote(psum.at[t], ar.at[t, me], ar_send.at[t, k], ar_recv.at[t, me], dev(peer_z, peer_r))

        def peers():
            for dz in range(2):
                for dr in range(n_col):
                    if dz or dr:
                        yield dz * n_col + dr, (zmo if dz else zm), (r + dr) % n_col

        def send_sums(t):
            for k, pz, pr in peers():
                ar_copy(t, k, pz, pr).start()
            ar[t, me] = psum[t]

        def column_scales(t):
            for k, pz, pr in peers():
                src = (1 - side if k >= n_col else side) * n_col + pr
                remote(psum.at[t], ar.at[t, src], ar_send.at[t, k], ar_recv.at[t, src], dev(z, r)).wait_recv()
            total = ar[t, 0]
            for src in range(1, 2 * n_col):
                total = total + ar[t, src]
            sc[...] = n / total

        for t in range(ITERATIONS - 1):
            @pl.loop(0, n_col)
            def _(zq):
                expand(zq)
                inflate(t, zq)

            send_sums(t)
            column_scales(t)

            @pl.loop(0, n_col)
            def _(zq):
                a[:, pl.ds(pl.multiple_of(zq * blk, blk), blk)] = (acc[zq] * sc[zq]).astype(jnp.bfloat16)

        t = ITERATIONS - 1
        expand(zco)
        inflate(t, zco)

        def tail_piece(ref, lead, ch):
            return ref.at[lead, pl.ds(pl.multiple_of(ch * rows_t, rows_t), rows_t), :]

        @pl.loop(0, TAIL_CHUNKS)
        def _(ch):
            remote(tail_piece(acc, zco, ch), tail_piece(fin, 1, ch), fin_send.at[0], fin_recv.at[2, ch], other).start()

        expand(zc)
        inflate(t, zc)
        to_corner = remote(acc.at[zc], fin.at[side], fin_send.at[1], fin_recv.at[1, 0], corner)
        to_corner.start()
        expand(zmo)
        inflate(t, zmo)
        expand(zm)
        inflate(t, zm)
        send_sums(t)
        to_other = remote(acc.at[zmo], fin.at[0], fin_send.at[2], fin_recv.at[0, 0], other)
        to_other.start()
        own = pltpu.make_async_copy(acc.at[zm], m_out.at[pl.ds(pl.multiple_of(side * half, half), half), :], out_sem.at[0])
        own.start()

        @pl.loop(0, TAIL_CHUNKS)
        def _(ch):
            piece = tail_piece(fin, 1, ch)
            remote(piece, piece, fin_send.at[0], fin_recv.at[2, ch], dev(z, r)).wait_recv()
            remote(piece, tail_piece(fin, 1 - side, ch), fin_send.at[3], fin_recv.at[2, ch], corner).start()

        column_scales(t)
        scale_corner = remote(sc.at[zc], scin, sc_sem.at[0], sc_sem.at[1], corner)
        scale_corner.start()
        scale_own = pltpu.make_async_copy(sc.at[zm], s_out, out_sem.at[2])
        scale_own.start()

        remote(fin.at[0], fin.at[0], fin_send.at[0], fin_recv.at[0, 0], dev(z, r)).wait_recv()
        rest = pltpu.make_async_copy(
            fin.at[0], m_out.at[pl.ds(pl.multiple_of((1 - side) * half, half), half), :], out_sem.at[1])
        rest.start()

        wait_sent(0, zm, r)
        wait_sent(0, zc, r)
        wait_sent(1, zm, r)
        wait_sent(1, zmo, r)
        wait_sent(1, zco, r)
        for zq in range(n_col):
            for yq in range(2):
                wait_sent(2, zq, 2 * yq + c)
        own_a.wait_send()
        relay_a.wait_send()
        for t in range(ITERATIONS):
            for k, pz, pr in peers():
                ar_copy(t, k, pz, pr).wait_send()
        remote(acc.at[zco], fin.at[1], fin_send.at[0], fin_recv.at[0, 0], other).wait_send()
        to_corner.wait_send()
        to_other.wait_send()
        remote(fin.at[1], fin.at[1], fin_send.at[3], fin_recv.at[0, 0], corner).wait_send()
        scale_corner.wait_send()
        own.wait()
        rest.wait()
        scale_own.wait()


def solution(mesh):
    num_cols = mesh.shape["col"]
    num_rows = mesh.shape["row"]
    block_spec = P(("graph", "row"), "col")

    def device_step(init_blk, graph_blk):
        blk = init_blk.shape[0]
        n = blk * num_rows
        half = blk // 2
        any_spec = pl.BlockSpec(memory_space=pl.ANY)
        squares, scale = pl.pallas_call(
            mcl_kernel,
            out_shape=(jax.ShapeDtypeStruct((blk, blk), jnp.float32), jax.ShapeDtypeStruct((1, blk), jnp.float32)),
            in_specs=[any_spec, any_spec],
            out_specs=(any_spec, any_spec),
            scratch_shapes=[
                pltpu.VMEM((num_cols, n, blk), jnp.bfloat16),
                pltpu.VMEM((half, n), jnp.bfloat16),
                pltpu.VMEM((2, half, blk), jnp.bfloat16),
                pltpu.VMEM((num_cols, half, blk), jnp.float32),
                pltpu.VMEM((2, half, blk), jnp.float32),
                pltpu.VMEM((ITERATIONS, num_cols, 1, blk), jnp.float32),
                pltpu.VMEM((ITERATIONS, 2 * num_rows, num_cols, 1, blk), jnp.float32),
                pltpu.VMEM((num_cols, 1, blk), jnp.float32),
                pltpu.VMEM((1, blk), jnp.float32),
                pltpu.SemaphoreType.DMA((4,)),
                pltpu.SemaphoreType.DMA((num_cols, 2, CHUNKS)),
                pltpu.SemaphoreType.DMA((num_cols, 2, CHUNKS)),
                pltpu.SemaphoreType.DMA((4,)),
                pltpu.SemaphoreType.DMA((4, num_cols, 3)),
                pltpu.SemaphoreType.DMA((4,)),
                pltpu.SemaphoreType.DMA((ITERATIONS, 2 * num_rows)),
                pltpu.SemaphoreType.DMA((ITERATIONS, 2 * num_rows)),
                pltpu.SemaphoreType.DMA((3, TAIL_CHUNKS)),
                pltpu.SemaphoreType.DMA((2,)),
                pltpu.SemaphoreType.DMA((3,)),
            ],
            compiler_params=pltpu.CompilerParams(
                collective_id=0, has_side_effects=True, vmem_limit_bytes=67_000_000),
        )(init_blk, graph_blk)
        return squares * scale

    return jax.shard_map(device_step, mesh=mesh, in_specs=(block_spec, block_spec), out_specs=block_spec, check_vma=False)
```

```python
import jax
import jax.numpy as jnp
from jax import lax
from jax.experimental import pallas as pl
from jax.experimental.pallas import tpu as pltpu
from jax.sharding import PartitionSpec as P

SUBS = 4
TILE = 256
AHEAD = 2
MESH = pl.DeviceIdType.MESH


def mcl_kernel(a_hbm, g_hbm, m_out, s_out, g, a, a1, snd, acc, fin, ps_mid, ar_mid, ps_edge, ar_edge, ps, ar, sc, scin,
               load_sem, rg, rp, ra, send_sem, fin_send, ar_send, ar_recv, fin_recv, sc_sem, out_sem):
    n_col = g.shape[0]
    blk = g.shape[2]
    n = g.shape[1]
    half = blk // 2
    pieces = blk // TILE
    rows_s = blk // SUBS
    rows_a = half // SUBS

    z = lax.axis_index("col")
    r = lax.axis_index("row")
    y = r // 2
    c = r % 2
    side = z // 2
    middle = jnp.logical_or(z == 1, z == 2)
    zm = 1 + side
    zc = 3 * side
    zmo = 2 - side
    zco = 3 - 3 * side
    r_y = 2 * (1 - y) + c
    r_p = 2 * y + 1 - c

    def dev(zq, rq):
        return {"col": zq, "row": rq}

    def remote(src, dst, ssem, rsem, d):
        return pltpu.make_async_remote_copy(
            src_ref=src, dst_ref=dst, send_sem=ssem, recv_sem=rsem, device_id=d, device_id_type=MESH)

    def cols(j):
        return pl.ds(pl.multiple_of(j * TILE, TILE), TILE)

    def g_sub(zq, rq, j, s):
        return g.at[zq, pl.ds(pl.multiple_of(rq * blk + s * rows_s, rows_s), rows_s), cols(j)]

    def g_piece(zq, rq, j):
        return g.at[zq, pl.ds(pl.multiple_of(rq * blk, blk), blk), cols(j)]

    def g_block(zq, rq):
        return g.at[zq, pl.ds(pl.multiple_of(rq * blk, blk), blk), :]

    def send_sub(link, zq, rq, j, s, d):
        ref = g_sub(zq, rq, j, s)
        remote(ref, ref, send_sem.at[link, zq, rq // 2], rg.at[zq, rq // 2, j, s], d).start()

    def wait_sub(zq, rq, j, s):
        ref = g_sub(zq, rq, j, s)
        remote(ref, ref, send_sem.at[0, 0, 0], rg.at[zq, rq // 2, j, s], dev(z, r)).wait_recv()

    def send_partner(zq, rq, j):
        ref = g_piece(zq, rq, j)
        remote(ref, ref, send_sem.at[2, zq, rq // 2], rp.at[zq, rq // 2, j], dev(zm, r_p)).start()

    def wait_partner(zq, j):
        for yq in range(2):
            ref = g_piece(zq, 2 * yq + 1 - c, j)
            remote(ref, ref, send_sem.at[0, 0, 0], rp.at[zq, yq, j], dev(z, r)).wait_recv()

    def wait_sent(link, zq, rq):
        block = g_block(zq, rq)
        remote(block, block, send_sem.at[link, zq, rq // 2], rg.at[0, 0, 0, 0], dev(z, r)).wait_send()

    def quarter(zq):
        return pl.ds(pl.multiple_of(zq * blk, blk), blk)

    def a_sub(s):
        return pl.ds(pl.multiple_of(s * rows_a, rows_a), rows_a)

    def send_a(idx, src, dst, link, s, d):
        remote(src.at[a_sub(s), :], dst.at[a_sub(s), :], send_sem.at[link, idx, 2], ra.at[idx, s], d).start()

    def wait_a(idx, s):
        ref = snd.at[1, a_sub(s), :]
        remote(ref, ref, send_sem.at[0, 0, 2], ra.at[idx, s], dev(z, r)).wait_recv()

    def wait_a_sent(idx, link):
        remote(snd.at[1], snd.at[1], send_sem.at[link, idx, 2], ra.at[0, 0], dev(z, r)).wait_send()

    barrier = pltpu.get_barrier_semaphore()

    @pl.when(middle)
    def _():
        for dz in range(2):
            for dr in range(n_col):
                peer_z = zm if dz == 0 else zmo
                if dz == 0 and dr == 0:
                    peer_z = zc
                pl.semaphore_signal(barrier, inc=1, device_id=dev(peer_z, (r + dr) % n_col), device_id_type=MESH)

    @pl.when(jnp.logical_not(middle))
    def _():
        pl.semaphore_signal(barrier, inc=1, device_id=dev(zm, r), device_id_type=MESH)
        pl.semaphore_signal(barrier, inc=1, device_id=dev(zc, r_y), device_id_type=MESH)

    loads = []
    for h in range(2):
        loads.append(pltpu.make_async_copy(a_hbm.at[pl.ds(h * half, half), :], acc.at[h], load_sem.at[h]))
    for h in range(2):
        loads.append(pltpu.make_async_copy(g_hbm.at[pl.ds(h * half, half), :], acc.at[2 + h], load_sem.at[2 + h]))
    for load in loads:
        load.start()
    for h in range(2):
        loads[h].wait()
    snd[0] = acc[1 - side].astype(jnp.bfloat16)
    a[:, quarter(z)] = acc[side].astype(jnp.bfloat16)
    for h in range(2):
        loads[2 + h].wait()
        g[z, pl.ds(pl.multiple_of(r * blk + h * half, half), half), :] = acc[2 + h].astype(jnp.bfloat16)

    def a_quarter(zq):
        return a.at[:, quarter(zq)]

    def out_rows(h):
        return pl.ds(pl.multiple_of(h * half, half), half)

    @pl.when(jnp.logical_not(middle))
    def _():
        pl.semaphore_wait(barrier, 2)
        inner = dev(zm, r)

        @pl.loop(0, SUBS)
        def _(s):
            send_a(0, snd.at[0], snd.at[1], 3, s, inner)

        @pl.loop(0, SUBS)
        def _(s):
            send_a(1, a_quarter(z), a_quarter(z), 3, s, inner)

        @pl.loop(0, pieces * SUBS)
        def _(i):
            send_sub(1, z, r, i // SUBS, i % SUBS, dev(zc, r_y))
            send_sub(3, z, r, i // SUBS, i % SUBS, inner)

        @pl.loop(0, pieces * SUBS)
        def _(i):
            wait_sub(z, r_y, i // SUBS, i % SUBS)
            send_sub(3, z, r_y, i // SUBS, i % SUBS, inner)

        wait_a_sent(0, 3)
        wait_a_sent(1, 3)
        wait_sent(3, z, r)
        wait_sent(1, z, r)
        wait_sent(3, z, r_y)

        for kind, h in ((1, side), (2, 1 - side)):
            @pl.loop(0, pieces)
            def _(j):
                ref = fin.at[h, :, cols(j)]
                remote(ref, ref, fin_send.at[0], fin_recv.at[kind, j], dev(z, r)).wait_recv()
                pltpu.make_async_copy(ref, m_out.at[out_rows(h), cols(j)], out_sem.at[kind - 1]).start()

        remote(scin, scin, sc_sem.at[0], sc_sem.at[1], dev(z, r)).wait_recv()
        scale_copy = pltpu.make_async_copy(scin, s_out, out_sem.at[2])
        scale_copy.start()
        for kind, h in ((1, side), (2, 1 - side)):
            pltpu.make_async_copy(fin.at[h], m_out.at[out_rows(h), :], out_sem.at[kind - 1]).wait()
        scale_copy.wait()

    @pl.when(middle)
    def _():
        pl.semaphore_wait(barrier, 2 * n_col)
        other = dev(zmo, r)
        across = dev(zm, r_y)
        corner = dev(zc, r)
        me = side * n_col + r

        def peers():
            for dz in range(2):
                for dr in range(n_col):
                    if dz or dr:
                        yield dz * n_col + dr, (zmo if dz else zm), (r + dr) % n_col

        def sums_of(i):
            if i == 0:
                return ps_mid, ar_mid
            if i <= pieces:
                return ps_edge.at[i - 1], ar_edge.at[i - 1]
            return ps.at[i - pieces - 1], ar.at[i - pieces - 1]

        def send_sums(i):
            src, slots = sums_of(i)
            for k, pz, pr in peers():
                remote(src, slots.at[me], ar_send.at[i, k], ar_recv.at[i, me], dev(pz, pr)).start()
            slots[me] = src[...]

        def scales(i):
            src, slots = sums_of(i)
            for k, pz, pr in peers():
                peer = (1 - side if k >= n_col else side) * n_col + pr
                remote(src, slots.at[peer], ar_send.at[i, k], ar_recv.at[i, peer], dev(z, r)).wait_recv()
            total = slots[0]
            for peer in range(1, 2 * n_col):
                total = total + slots[peer]
            return n / total

        def square(zq, j, slot):
            step = 64

            def body(i, total):
                rows = pl.ds(pl.multiple_of(i * step, step), step)
                value = acc[zq, rows, cols(j)]
                value = value * value
                acc[zq, rows, cols(j)] = value
                return total + jnp.sum(value.reshape(step // 8, 8, TILE), axis=0)

            total = lax.fori_loop(0, half // step, body, jnp.zeros((8, TILE), jnp.float32))
            slot[...] = jnp.sum(total, axis=0, keepdims=True)

        def expand(zq, j, slot):
            acc[zq, :, cols(j)] = jnp.dot(a[...], g[zq, :, cols(j)], preferred_element_type=jnp.float32)
            square(zq, j, slot)

        @pl.loop(0, SUBS)
        def _(s):
            send_a(2, snd.at[0], a_quarter(zm), 0, s, other)

        @pl.loop(0, pieces)
        def _(j):
            send_partner(zm, r, j)
            for s in range(SUBS):
                send_sub(1, zm, r, j, s, across)

        @pl.loop(0, SUBS)
        def _(s):
            wait_a(0, s)
            send_a(3, snd.at[1], a_quarter(zc), 0, s, other)

        @pl.loop(0, pieces * SUBS)
        def _(i):
            send_sub(0, zm, r, i // SUBS, i % SUBS, other)

        @pl.loop(0, pieces)
        def _(j):
            for s in range(SUBS):
                wait_sub(zm, r_y, j, s)
            send_partner(zm, r_y, j)

        @pl.loop(0, SUBS)
        def _(s):
            for idx in (2, 3, 1):
                wait_a(idx, s)

        @pl.loop(0, pieces)
        def _(j):
            @pl.loop(0, SUBS)
            def _(s):
                wait_sub(zmo, r, j, s)
                send_sub(1, zmo, r, j, s, across)
                wait_sub(zc, r, j, s)
                wait_sub(zmo, r_y, j, s)

                @pl.when(s == SUBS - 1)
                def _():
                    send_partner(zmo, r, j)
                    send_partner(zc, r, j)
                    send_partner(zmo, r_y, j)

                late = s // 2
                zq = zm + late * (zmo - zm)
                jq = j - late

                @pl.when(jnp.logical_and(s % 2 == 0, jq >= 0))
                def _():
                    wait_partner(zq, jq)
                    expand(zq, jq, ps_mid.at[zq - 1, :, cols(jq)])

        def finish_mid():
            scale = scales(0)
            for idx, zq in ((0, 1), (1, 2)):
                a1[:, pl.ds(zq * blk, blk)] = (acc[zq] * scale[idx]).astype(jnp.bfloat16)

        def finish_edge(j):
            scale = scales(1 + j)
            for idx, zq in ((0, 0), (1, 3)):
                a1[:, pl.ds(zq * blk + j * TILE, TILE)] = (
                    acc[zq, :, pl.ds(j * TILE, TILE)] * scale[idx]).astype(jnp.bfloat16)

        def partial(zq, k0, k_len, n0, n_len):
            rows = pl.ds(pl.multiple_of(k0, TILE), k_len)
            return jnp.dot(a1[:, rows], g[zq, rows, pl.ds(pl.multiple_of(n0, TILE), n_len)],
                           preferred_element_type=jnp.float32)

        def mid_by_mid(zq):
            @pl.loop(0, pieces)
            def _(j):
                acc[zq, :, cols(j)] = (partial(zq, blk, blk, j * TILE, TILE) + partial(zq, 2 * blk, blk, j * TILE, TILE))

        def new_columns(j):
            @pl.loop(0, 2)
            def _(i):
                zq = 3 * i
                total = partial(zq, blk, blk, j * TILE, TILE) + partial(zq, 2 * blk, blk, j * TILE, TILE)
                for k_z in (0, 3):
                    total += partial(zq, k_z * blk, (j + 1) * TILE, j * TILE, TILE)
                acc[zq, :, pl.ds(j * TILE, TILE)] = total

        def old_columns(j):
            def add(zq, n0, n_len):
                span = pl.ds(pl.multiple_of(n0, TILE), n_len)
                acc[zq, :, span] += (partial(zq, j * TILE, TILE, n0, n_len)
                                     + partial(zq, 3 * blk + j * TILE, TILE, n0, n_len))

            wide = 2 * TILE

            @pl.loop(0, 2 * blk // wide)
            def _(i):
                per = blk // wide
                add(1 + i // per, (i % per) * wide, wide)

            if j:
                @pl.loop(0, 2 * j)
                def _(i):
                    add(3 * (i // j), (i % j) * TILE, TILE)

        for i in range(AHEAD):
            send_sub(0, zc, r, i // SUBS, i % SUBS, other)

        for j in range(pieces):
            def pump(s):
                ahead = j * SUBS + s + AHEAD

                @pl.when(ahead < pieces * SUBS)
                def _():
                    send_sub(0, zc, r, ahead // SUBS, ahead % SUBS, other)

                wait_sub(zco, r, j, s)
                send_sub(1, zco, r, j, s, across)
                wait_sub(zc, r_y, j, s)
                wait_sub(zco, r_y, j, s)

            @pl.loop(0, 2)
            def _(s):
                pump(s)
                if j:
                    zq = zc + s * (zco - zc)
                    wait_partner(zq, j - 1)
                    expand(zq, j - 1, ps_edge.at[j - 1, zq // 3])
                else:
                    @pl.when(s == 0)
                    def _():
                        wait_partner(zmo, pieces - 1)
                        expand(zmo, pieces - 1, ps_mid.at[zmo - 1, :, cols(pieces - 1)])

            send_sums(j)
            pump(2)
            if j == 1:
                finish_mid()
                mid_by_mid(1)
            elif j > 1:
                finish_edge(j - 2)
                new_columns(j - 2)
            pump(3)
            send_partner(zco, r, j)
            send_partner(zc, r_y, j)
            send_partner(zco, r_y, j)
            if j == 1:
                mid_by_mid(2)
            elif j > 1:
                old_columns(j - 2)

        last = pieces - 1

        @pl.loop(0, 2)
        def _(s):
            zq = zc + s * (zco - zc)
            wait_partner(zq, last)
            expand(zq, last, ps_edge.at[last, zq // 3])

        send_sums(pieces)
        for j in (last - 1, last):
            finish_edge(j)
            new_columns(j)
            old_columns(j)

        @pl.loop(0, n_col)
        def _(zq):
            for j in range(pieces):
                square(zq, j, ps.at[0, zq, :, cols(j)])

        send_sums(pieces + 1)
        sc[...] = scales(pieces + 1)

        @pl.loop(0, n_col)
        def _(zq):
            a[:, quarter(zq)] = (acc[zq] * sc[zq]).astype(jnp.bfloat16)

        def fin_piece(ref, lead, j):
            return ref.at[lead, :, cols(j)]

        @pl.loop(0, pieces)
        def _(j):
            @pl.loop(0, 2)
            def _(i):
                zq = zco + i * (zc - zco)
                expand(zq, j, ps.at[1, zq, :, cols(j)])

                @pl.when(i == 0)
                def _():
                    remote(fin_piece(acc, zco, j), fin_piece(fin, 1, j), fin_send.at[0], fin_recv.at[2, j], other).start()

                @pl.when(i == 1)
                def _():
                    remote(fin_piece(acc, zc, j), fin_piece(fin, side, j), fin_send.at[1], fin_recv.at[1, j], corner).start()

        @pl.loop(0, 2 * pieces)
        def _(i):
            zq = zmo + (i // pieces) * (zm - zmo)
            j = i % pieces
            expand(zq, j, ps.at[1, zq, :, cols(j)])

        send_sums(pieces + 2)
        to_other = remote(acc.at[zmo], fin.at[0], fin_send.at[2], fin_recv.at[0, 0], other)
        to_other.start()
        own = pltpu.make_async_copy(acc.at[zm], m_out.at[out_rows(side), :], out_sem.at[0])
        own.start()

        @pl.loop(0, pieces)
        def _(j):
            ref = fin_piece(fin, 1, j)
            remote(ref, ref, fin_send.at[0], fin_recv.at[2, j], dev(z, r)).wait_recv()
            remote(ref, fin_piece(fin, 1 - side, j), fin_send.at[3], fin_recv.at[2, j], corner).start()

        sc[...] = scales(pieces + 2)
        scale_corner = remote(sc.at[zc], scin, sc_sem.at[0], sc_sem.at[1], corner)
        scale_corner.start()
        scale_own = pltpu.make_async_copy(sc.at[zm], s_out, out_sem.at[2])
        scale_own.start()

        remote(fin.at[0], fin.at[0], fin_send.at[0], fin_recv.at[0, 0], dev(z, r)).wait_recv()
        rest = pltpu.make_async_copy(fin.at[0], m_out.at[out_rows(1 - side), :], out_sem.at[1])
        rest.start()

        wait_a_sent(2, 0)
        wait_a_sent(3, 0)
        wait_sent(0, zm, r)
        wait_sent(0, zc, r)
        wait_sent(1, zm, r)
        wait_sent(1, zmo, r)
        wait_sent(1, zco, r)
        for zq in range(n_col):
            for yq in range(2):
                wait_sent(2, zq, 2 * yq + c)
        for i in range(pieces + 3):
            src, slots = sums_of(i)
            for k, pz, pr in peers():
                remote(src, slots.at[me], ar_send.at[i, k], ar_recv.at[i, me], dev(pz, pr)).wait_send()
        remote(acc.at[zco], fin.at[1], fin_send.at[0], fin_recv.at[0, 0], other).wait_send()
        remote(acc.at[zc], fin.at[side], fin_send.at[1], fin_recv.at[0, 0], corner).wait_send()
        to_other.wait_send()
        remote(fin.at[1], fin.at[1], fin_send.at[3], fin_recv.at[0, 0], corner).wait_send()
        scale_corner.wait_send()
        own.wait()
        rest.wait()
        scale_own.wait()


def solution(mesh):
    num_cols = mesh.shape["col"]
    num_rows = mesh.shape["row"]
    block_spec = P(("graph", "row"), "col")

    def device_step(init_blk, graph_blk):
        blk = init_blk.shape[0]
        n = blk * num_rows
        half = blk // 2
        pieces = blk // TILE
        cores = 2 * num_rows
        any_spec = pl.BlockSpec(memory_space=pl.ANY)
        squares, scale = pl.pallas_call(
            mcl_kernel,
            out_shape=(jax.ShapeDtypeStruct((blk, blk), jnp.float32), jax.ShapeDtypeStruct((1, blk), jnp.float32)),
            in_specs=[any_spec, any_spec],
            out_specs=(any_spec, any_spec),
            scratch_shapes=[
                pltpu.VMEM((num_cols, n, blk), jnp.bfloat16),
                pltpu.VMEM((half, n), jnp.bfloat16),
                pltpu.VMEM((half, n), jnp.bfloat16),
                pltpu.VMEM((2, half, blk), jnp.bfloat16),
                pltpu.VMEM((num_cols, half, blk), jnp.float32),
                pltpu.VMEM((2, half, blk), jnp.float32),
                pltpu.VMEM((2, 1, blk), jnp.float32),
                pltpu.VMEM((cores, 2, 1, blk), jnp.float32),
                pltpu.VMEM((pieces, 2, 1, TILE), jnp.float32),
                pltpu.VMEM((pieces, cores, 2, 1, TILE), jnp.float32),
                pltpu.VMEM((2, num_cols, 1, blk), jnp.float32),
                pltpu.VMEM((2, cores, num_cols, 1, blk), jnp.float32),
                pltpu.VMEM((num_cols, 1, blk), jnp.float32),
                pltpu.VMEM((1, blk), jnp.float32),
                pltpu.SemaphoreType.DMA((4,)),
                pltpu.SemaphoreType.DMA((num_cols, 2, pieces, SUBS)),
                pltpu.SemaphoreType.DMA((num_cols, 2, pieces)),
                pltpu.SemaphoreType.DMA((4, SUBS)),
                pltpu.SemaphoreType.DMA((4, num_cols, 3)),
                pltpu.SemaphoreType.DMA((4,)),
                pltpu.SemaphoreType.DMA((pieces + 3, cores)),
                pltpu.SemaphoreType.DMA((pieces + 3, cores)),
                pltpu.SemaphoreType.DMA((3, pieces)),
                pltpu.SemaphoreType.DMA((2,)),
                pltpu.SemaphoreType.DMA((3,)),
            ],
            compiler_params=pltpu.CompilerParams(
                collective_id=0, has_side_effects=True, vmem_limit_bytes=67_000_000),
        )(init_blk, graph_blk)
        return squares * scale

    return jax.shard_map(device_step, mesh=mesh, in_specs=(block_spec, block_spec), out_specs=block_spec, check_vma=False)
```

```python
import jax
import jax.numpy as jnp
from jax import lax
from jax.experimental import pallas as pl
from jax.experimental.pallas import tpu as pltpu
from jax.sharding import PartitionSpec as P

SUBS = 4
TILE = 256
AHEAD = 3
LAG = 3
MESH = pl.DeviceIdType.MESH


def mcl_kernel(a_hbm, g_hbm, m_out, s_out, g, a, a1, snd, acc, fin, ps_mid, ar_mid, ps_edge, ar_edge, ps, ar, sc, scin,
               load_sem, rg, rp, ra, send_sem, fin_send, ar_send, ar_recv, fin_recv, sc_sem, out_sem):
    n_col = g.shape[0]
    blk = g.shape[2]
    n = g.shape[1]
    half = blk // 2
    pieces = blk // TILE
    rows_s = blk // SUBS
    rows_a = half // SUBS

    z = lax.axis_index("col")
    r = lax.axis_index("row")
    y = r // 2
    c = r % 2
    side = z // 2
    middle = jnp.logical_or(z == 1, z == 2)
    zm = 1 + side
    zc = 3 * side
    zmo = 2 - side
    zco = 3 - 3 * side
    r_y = 2 * (1 - y) + c
    r_p = 2 * y + 1 - c

    def dev(zq, rq):
        return {"col": zq, "row": rq}

    def remote(src, dst, ssem, rsem, d):
        return pltpu.make_async_remote_copy(
            src_ref=src, dst_ref=dst, send_sem=ssem, recv_sem=rsem, device_id=d, device_id_type=MESH)

    def cols(j):
        return pl.ds(pl.multiple_of(j * TILE, TILE), TILE)

    def g_sub(zq, rq, j, s):
        return g.at[zq, pl.ds(pl.multiple_of(rq * blk + s * rows_s, rows_s), rows_s), cols(j)]

    def g_piece(zq, rq, j):
        return g.at[zq, pl.ds(pl.multiple_of(rq * blk, blk), blk), cols(j)]

    def g_block(zq, rq):
        return g.at[zq, pl.ds(pl.multiple_of(rq * blk, blk), blk), :]

    def send_sub(link, zq, rq, j, s, d):
        ref = g_sub(zq, rq, j, s)
        remote(ref, ref, send_sem.at[link, zq, rq // 2], rg.at[zq, rq // 2, j, s], d).start()

    def wait_sub(zq, rq, j, s):
        ref = g_sub(zq, rq, j, s)
        remote(ref, ref, send_sem.at[0, 0, 0], rg.at[zq, rq // 2, j, s], dev(z, r)).wait_recv()

    def send_partner(zq, rq, j):
        ref = g_piece(zq, rq, j)
        remote(ref, ref, send_sem.at[2, zq, rq // 2], rp.at[zq, rq // 2, j], dev(zm, r_p)).start()

    def wait_partner(zq, j):
        for yq in range(2):
            ref = g_piece(zq, 2 * yq + 1 - c, j)
            remote(ref, ref, send_sem.at[0, 0, 0], rp.at[zq, yq, j], dev(z, r)).wait_recv()

    def wait_sent(link, zq, rq):
        block = g_block(zq, rq)
        remote(block, block, send_sem.at[link, zq, rq // 2], rg.at[0, 0, 0, 0], dev(z, r)).wait_send()

    def quarter(zq):
        return pl.ds(pl.multiple_of(zq * blk, blk), blk)

    def a_sub(s):
        return pl.ds(pl.multiple_of(s * rows_a, rows_a), rows_a)

    def send_a(idx, src, dst, link, s, d):
        remote(src.at[a_sub(s), :], dst.at[a_sub(s), :], send_sem.at[link, idx, 2], ra.at[idx, s], d).start()

    def wait_a(idx, s):
        ref = snd.at[1, a_sub(s), :]
        remote(ref, ref, send_sem.at[0, 0, 2], ra.at[idx, s], dev(z, r)).wait_recv()

    def wait_a_sent(idx, link):
        remote(snd.at[1], snd.at[1], send_sem.at[link, idx, 2], ra.at[0, 0], dev(z, r)).wait_send()

    barrier = pltpu.get_barrier_semaphore()

    @pl.when(middle)
    def _():
        for dz in range(2):
            for dr in range(n_col):
                peer_z = zm if dz == 0 else zmo
                if dz == 0 and dr == 0:
                    peer_z = zc
                pl.semaphore_signal(barrier, inc=1, device_id=dev(peer_z, (r + dr) % n_col), device_id_type=MESH)

    @pl.when(jnp.logical_not(middle))
    def _():
        pl.semaphore_signal(barrier, inc=1, device_id=dev(zm, r), device_id_type=MESH)
        pl.semaphore_signal(barrier, inc=1, device_id=dev(zc, r_y), device_id_type=MESH)

    loads = []
    for h in range(2):
        loads.append(pltpu.make_async_copy(a_hbm.at[pl.ds(h * half, half), :], acc.at[h], load_sem.at[h]))
    for h in range(2):
        loads.append(pltpu.make_async_copy(g_hbm.at[pl.ds(h * half, half), :], acc.at[2 + h], load_sem.at[2 + h]))
    for load in loads:
        load.start()
    for h in range(2):
        loads[h].wait()
    snd[0] = acc[1 - side].astype(jnp.bfloat16)
    a[:, quarter(z)] = acc[side].astype(jnp.bfloat16)
    for h in range(2):
        loads[2 + h].wait()
        g[z, pl.ds(pl.multiple_of(r * blk + h * half, half), half), :] = acc[2 + h].astype(jnp.bfloat16)

    def a_quarter(zq):
        return a.at[:, quarter(zq)]

    def out_rows(h):
        return pl.ds(pl.multiple_of(h * half, half), half)

    @pl.when(jnp.logical_not(middle))
    def _():
        pl.semaphore_wait(barrier, 2)
        inner = dev(zm, r)

        @pl.loop(0, SUBS)
        def _(s):
            send_a(0, snd.at[0], snd.at[1], 3, s, inner)

        @pl.loop(0, SUBS)
        def _(s):
            send_a(1, a_quarter(z), a_quarter(z), 3, s, inner)

        @pl.loop(0, pieces * SUBS)
        def _(i):
            send_sub(1, z, r, i // SUBS, i % SUBS, dev(zc, r_y))
            send_sub(3, z, r, i // SUBS, i % SUBS, inner)

        @pl.loop(0, pieces * SUBS)
        def _(i):
            wait_sub(z, r_y, i // SUBS, i % SUBS)
            send_sub(3, z, r_y, i // SUBS, i % SUBS, inner)

        wait_a_sent(0, 3)
        wait_a_sent(1, 3)
        wait_sent(3, z, r)
        wait_sent(1, z, r)
        wait_sent(3, z, r_y)

        for kind, h in ((1, side), (2, 1 - side)):
            @pl.loop(0, pieces)
            def _(j):
                ref = fin.at[h, :, cols(j)]
                remote(ref, ref, fin_send.at[0], fin_recv.at[kind, j], dev(z, r)).wait_recv()
                pltpu.make_async_copy(ref, m_out.at[out_rows(h), cols(j)], out_sem.at[kind - 1]).start()

        remote(scin, scin, sc_sem.at[0], sc_sem.at[1], dev(z, r)).wait_recv()
        scale_copy = pltpu.make_async_copy(scin, s_out, out_sem.at[2])
        scale_copy.start()
        for kind, h in ((1, side), (2, 1 - side)):
            pltpu.make_async_copy(fin.at[h], m_out.at[out_rows(h), :], out_sem.at[kind - 1]).wait()
        scale_copy.wait()

    @pl.when(middle)
    def _():
        pl.semaphore_wait(barrier, 2 * n_col)
        other = dev(zmo, r)
        across = dev(zm, r_y)
        corner = dev(zc, r)
        me = side * n_col + r

        def peers():
            for dz in range(2):
                for dr in range(n_col):
                    if dz or dr:
                        yield dz * n_col + dr, (zmo if dz else zm), (r + dr) % n_col

        def sums_of(i):
            if i == 0:
                return ps_mid, ar_mid
            if i <= pieces:
                return ps_edge.at[i - 1], ar_edge.at[i - 1]
            return ps.at[i - pieces - 1], ar.at[i - pieces - 1]

        def send_sums(i):
            src, slots = sums_of(i)
            for k, pz, pr in peers():
                remote(src, slots.at[me], ar_send.at[i, k], ar_recv.at[i, me], dev(pz, pr)).start()
            slots[me] = src[...]

        def scales(i):
            src, slots = sums_of(i)
            for k, pz, pr in peers():
                peer = (1 - side if k >= n_col else side) * n_col + pr
                remote(src, slots.at[peer], ar_send.at[i, k], ar_recv.at[i, peer], dev(z, r)).wait_recv()
            total = slots[0]
            for peer in range(1, 2 * n_col):
                total = total + slots[peer]
            return n / total

        def square(zq, j, slot):
            step = 64

            def body(i, total):
                rows = pl.ds(pl.multiple_of(i * step, step), step)
                value = acc[zq, rows, cols(j)]
                value = value * value
                acc[zq, rows, cols(j)] = value
                return total + jnp.sum(value.reshape(step // 8, 8, TILE), axis=0)

            total = lax.fori_loop(0, half // step, body, jnp.zeros((8, TILE), jnp.float32))
            slot[...] = jnp.sum(total, axis=0, keepdims=True)

        def expand(zq, j, slot):
            acc[zq, :, cols(j)] = jnp.dot(a[...], g[zq, :, cols(j)], preferred_element_type=jnp.float32)
            square(zq, j, slot)

        @pl.loop(0, SUBS)
        def _(s):
            send_a(2, snd.at[0], a_quarter(zm), 0, s, other)

        @pl.loop(0, pieces)
        def _(j):
            send_partner(zm, r, j)
            for s in range(SUBS):
                send_sub(1, zm, r, j, s, across)

        @pl.loop(0, SUBS)
        def _(s):
            wait_a(0, s)
            send_a(3, snd.at[1], a_quarter(zc), 0, s, other)

        @pl.loop(0, pieces * SUBS)
        def _(i):
            send_sub(0, zm, r, i // SUBS, i % SUBS, other)

        @pl.loop(0, pieces)
        def _(j):
            for s in range(SUBS):
                wait_sub(zm, r_y, j, s)
            send_partner(zm, r_y, j)

        @pl.loop(0, SUBS)
        def _(s):
            for idx in (2, 3, 1):
                wait_a(idx, s)

        def finish_mid():
            scale = scales(0)
            for idx, zq in ((0, 1), (1, 2)):
                a1[:, pl.ds(zq * blk, blk)] = (acc[zq] * scale[idx]).astype(jnp.bfloat16)

        def finish_edge(j):
            scale = scales(1 + j)
            for idx, zq in ((0, 0), (1, 3)):
                a1[:, pl.ds(zq * blk + j * TILE, TILE)] = (
                    acc[zq, :, pl.ds(j * TILE, TILE)] * scale[idx]).astype(jnp.bfloat16)

        def partial(zq, k0, k_len, n0, n_len):
            rows = pl.ds(pl.multiple_of(k0, TILE), k_len)
            return jnp.dot(a1[:, rows], g[zq, rows, pl.ds(pl.multiple_of(n0, TILE), n_len)],
                           preferred_element_type=jnp.float32)

        def mid_by_mid(zq):
            @pl.loop(0, pieces)
            def _(j):
                acc[zq, :, cols(j)] = (partial(zq, blk, blk, j * TILE, TILE) + partial(zq, 2 * blk, blk, j * TILE, TILE))

        def new_columns(j):
            @pl.loop(0, 2)
            def _(i):
                zq = 3 * i
                total = partial(zq, blk, blk, j * TILE, TILE) + partial(zq, 2 * blk, blk, j * TILE, TILE)
                for k_z in (0, 3):
                    total += partial(zq, k_z * blk, (j + 1) * TILE, j * TILE, TILE)
                acc[zq, :, pl.ds(j * TILE, TILE)] = total

        def old_columns(j):
            def add(zq, n0, n_len):
                span = pl.ds(pl.multiple_of(n0, TILE), n_len)
                acc[zq, :, span] += (partial(zq, j * TILE, TILE, n0, n_len)
                                     + partial(zq, 3 * blk + j * TILE, TILE, n0, n_len))

            wide = 2 * TILE

            @pl.loop(0, 2 * blk // wide)
            def _(i):
                per = blk // wide
                add(1 + i // per, (i % per) * wide, wide)

            if j:
                @pl.loop(0, 2 * j)
                def _(i):
                    add(3 * (i // j), (i % j) * TILE, TILE)

        n_slices = pieces * SUBS

        def from_other(q):
            return zmo + (q // pieces) * (zco - zmo)

        def pump(i):
            q, s = i // SUBS, i % SUBS
            j = q % pieces
            z_m = from_other(q)
            r_e = r + (q // pieces) * (r_y - r)
            ahead = i + AHEAD - n_slices

            @pl.when(jnp.logical_and(ahead >= 0, ahead < n_slices))
            def _():
                send_sub(0, zc, r, ahead // SUBS, ahead % SUBS, other)

            wait_sub(z_m, r, j, s)
            send_sub(1, z_m, r, j, s, across)
            wait_sub(zc, r_e, j, s)

            @pl.when(s == SUBS - 1)
            def _():
                send_partner(z_m, r, j)
                send_partner(zc, r_e, j)

            @pl.when(i >= LAG)
            def _():
                pump_across(i - LAG)

        def pump_across(i):
            q, s = i // SUBS, i % SUBS
            wait_sub(from_other(q), r_y, q % pieces, s)

            @pl.when(s == SUBS - 1)
            def _():
                send_partner(from_other(q), r_y, q % pieces)

        @pl.loop(0, pieces + 1)
        def _(q):
            @pl.loop(0, SUBS)
            def _(s):
                pump(q * SUBS + s)
                first = q == 0
                zq = jnp.where(first, zm, zmo)
                jq = jnp.where(first, s, q - 1)

                @pl.when(jnp.logical_or(first, s == SUBS - 1))
                def _():
                    wait_partner(zq, jq)
                    expand(zq, jq, ps_mid.at[zq - 1, :, cols(jq)])

        send_sums(0)

        def edge_step(j, second, third):
            @pl.loop(0, SUBS)
            def _(s):
                pump((pieces + 1 + j) * SUBS + s)

                @pl.when(jnp.logical_or(s == 0, s == SUBS - 1))
                def _():
                    zq = jnp.where(s == 0, zc, zco)
                    wait_partner(zq, j)
                    expand(zq, j, ps_edge.at[j, zq // 3])

                @pl.when(s == 1)
                def _():
                    second()

                @pl.when(s == 2)
                def _():
                    third()

            send_sums(1 + j)

        def mid_start():
            finish_mid()
            mid_by_mid(1)

        def edge_start(j):
            finish_edge(j)
            new_columns(j)

        edge_step(0, lambda: None, mid_start)
        edge_step(1, lambda: mid_by_mid(2), lambda: None)
        edge_step(2, lambda: edge_start(0), lambda: old_columns(0))

        last = pieces - 1
        edge_start(last - 2)
        old_columns(last - 2)
        for i in range(2 * n_slices - LAG, 2 * n_slices):
            pump_across(i)
        edge_start(last - 1)

        @pl.loop(0, 2)
        def _(s):
            zq = zc + s * (zco - zc)
            wait_partner(zq, last)
            expand(zq, last, ps_edge.at[last, zq // 3])

        send_sums(pieces)
        old_columns(last - 1)
        edge_start(last)
        old_columns(last)

        @pl.loop(0, n_col)
        def _(zq):
            for j in range(pieces):
                square(zq, j, ps.at[0, zq, :, cols(j)])

        send_sums(pieces + 1)
        sc[...] = scales(pieces + 1)

        @pl.loop(0, n_col)
        def _(zq):
            a[:, quarter(zq)] = (acc[zq] * sc[zq]).astype(jnp.bfloat16)

        def fin_piece(ref, lead, j):
            return ref.at[lead, :, cols(j)]

        @pl.loop(0, pieces)
        def _(j):
            @pl.loop(0, 2)
            def _(i):
                zq = zco + i * (zc - zco)
                expand(zq, j, ps.at[1, zq, :, cols(j)])

                @pl.when(i == 0)
                def _():
                    remote(fin_piece(acc, zco, j), fin_piece(fin, 1, j), fin_send.at[0], fin_recv.at[2, j], other).start()

                @pl.when(i == 1)
                def _():
                    remote(fin_piece(acc, zc, j), fin_piece(fin, side, j), fin_send.at[1], fin_recv.at[1, j], corner).start()

        @pl.loop(0, 2 * pieces)
        def _(i):
            zq = zmo + (i // pieces) * (zm - zmo)
            j = i % pieces
            expand(zq, j, ps.at[1, zq, :, cols(j)])

        send_sums(pieces + 2)
        to_other = remote(acc.at[zmo], fin.at[0], fin_send.at[2], fin_recv.at[0, 0], other)
        to_other.start()
        own = pltpu.make_async_copy(acc.at[zm], m_out.at[out_rows(side), :], out_sem.at[0])
        own.start()

        @pl.loop(0, pieces)
        def _(j):
            ref = fin_piece(fin, 1, j)
            remote(ref, ref, fin_send.at[0], fin_recv.at[2, j], dev(z, r)).wait_recv()
            remote(ref, fin_piece(fin, 1 - side, j), fin_send.at[3], fin_recv.at[2, j], corner).start()

        sc[...] = scales(pieces + 2)
        scale_corner = remote(sc.at[zc], scin, sc_sem.at[0], sc_sem.at[1], corner)
        scale_corner.start()
        scale_own = pltpu.make_async_copy(sc.at[zm], s_out, out_sem.at[2])
        scale_own.start()

        remote(fin.at[0], fin.at[0], fin_send.at[0], fin_recv.at[0, 0], dev(z, r)).wait_recv()
        rest = pltpu.make_async_copy(fin.at[0], m_out.at[out_rows(1 - side), :], out_sem.at[1])
        rest.start()

        wait_a_sent(2, 0)
        wait_a_sent(3, 0)
        wait_sent(0, zm, r)
        wait_sent(0, zc, r)
        wait_sent(1, zm, r)
        wait_sent(1, zmo, r)
        wait_sent(1, zco, r)
        for zq in range(n_col):
            for yq in range(2):
                wait_sent(2, zq, 2 * yq + c)
        for i in range(pieces + 3):
            src, slots = sums_of(i)
            for k, pz, pr in peers():
                remote(src, slots.at[me], ar_send.at[i, k], ar_recv.at[i, me], dev(pz, pr)).wait_send()
        remote(acc.at[zco], fin.at[1], fin_send.at[0], fin_recv.at[0, 0], other).wait_send()
        remote(acc.at[zc], fin.at[side], fin_send.at[1], fin_recv.at[0, 0], corner).wait_send()
        to_other.wait_send()
        remote(fin.at[1], fin.at[1], fin_send.at[3], fin_recv.at[0, 0], corner).wait_send()
        scale_corner.wait_send()
        own.wait()
        rest.wait()
        scale_own.wait()


def solution(mesh):
    num_cols = mesh.shape["col"]
    num_rows = mesh.shape["row"]
    block_spec = P(("graph", "row"), "col")

    def device_step(init_blk, graph_blk):
        blk = init_blk.shape[0]
        n = blk * num_rows
        half = blk // 2
        pieces = blk // TILE
        cores = 2 * num_rows
        any_spec = pl.BlockSpec(memory_space=pl.ANY)
        squares, scale = pl.pallas_call(
            mcl_kernel,
            out_shape=(jax.ShapeDtypeStruct((blk, blk), jnp.float32), jax.ShapeDtypeStruct((1, blk), jnp.float32)),
            in_specs=[any_spec, any_spec],
            out_specs=(any_spec, any_spec),
            scratch_shapes=[
                pltpu.VMEM((num_cols, n, blk), jnp.bfloat16),
                pltpu.VMEM((half, n), jnp.bfloat16),
                pltpu.VMEM((half, n), jnp.bfloat16),
                pltpu.VMEM((2, half, blk), jnp.bfloat16),
                pltpu.VMEM((num_cols, half, blk), jnp.float32),
                pltpu.VMEM((2, half, blk), jnp.float32),
                pltpu.VMEM((2, 1, blk), jnp.float32),
                pltpu.VMEM((cores, 2, 1, blk), jnp.float32),
                pltpu.VMEM((pieces, 2, 1, TILE), jnp.float32),
                pltpu.VMEM((pieces, cores, 2, 1, TILE), jnp.float32),
                pltpu.VMEM((2, num_cols, 1, blk), jnp.float32),
                pltpu.VMEM((2, cores, num_cols, 1, blk), jnp.float32),
                pltpu.VMEM((num_cols, 1, blk), jnp.float32),
                pltpu.VMEM((1, blk), jnp.float32),
                pltpu.SemaphoreType.DMA((4,)),
                pltpu.SemaphoreType.DMA((num_cols, 2, pieces, SUBS)),
                pltpu.SemaphoreType.DMA((num_cols, 2, pieces)),
                pltpu.SemaphoreType.DMA((4, SUBS)),
                pltpu.SemaphoreType.DMA((4, num_cols, 3)),
                pltpu.SemaphoreType.DMA((4,)),
                pltpu.SemaphoreType.DMA((pieces + 3, cores)),
                pltpu.SemaphoreType.DMA((pieces + 3, cores)),
                pltpu.SemaphoreType.DMA((3, pieces)),
                pltpu.SemaphoreType.DMA((2,)),
                pltpu.SemaphoreType.DMA((3,)),
            ],
            compiler_params=pltpu.CompilerParams(
                collective_id=0, has_side_effects=True, vmem_limit_bytes=67_000_000),
        )(init_blk, graph_blk)
        return squares * scale

    return jax.shard_map(device_step, mesh=mesh, in_specs=(block_spec, block_spec), out_specs=block_spec, check_vma=False)
```

```python
import jax
import jax.numpy as jnp
from jax import lax
from jax.experimental import pallas as pl
from jax.experimental.pallas import tpu as pltpu
from jax.sharding import PartitionSpec as P

SUBS = 4
TILE = 256
AHEAD = 2
LAG = 3
MESH = pl.DeviceIdType.MESH


def mcl_kernel(a_hbm, g_hbm, m_out, s_out, g, a, a1, snd, acc, fin, ps_mid, ar_mid, ps_edge, ar_edge, ps, ar, sc,
               load_sem, rm, re, ry, rp, ra_relay, ra, send_sem, fin_send, ar_send, ar_recv, fin_recv, sc_sem):
    n_col = g.shape[0]
    blk = g.shape[2]
    n = g.shape[1]
    half = blk // 2
    pieces = blk // TILE
    rows_s = blk // SUBS
    rows_a = half // SUBS

    z = lax.axis_index("col")
    r = lax.axis_index("row")
    y = r // 2
    c = r % 2
    side = z // 2
    middle = jnp.logical_or(z == 1, z == 2)
    zm = 1 + side
    zc = 3 * side
    zmo = 2 - side
    zco = 3 - 3 * side
    r_y = 2 * (1 - y) + c
    r_p = 2 * y + 1 - c

    def dev(zq, rq):
        return {"col": zq, "row": rq}

    def remote(src, dst, ssem, rsem, d):
        return pltpu.make_async_remote_copy(
            src_ref=src, dst_ref=dst, send_sem=ssem, recv_sem=rsem, device_id=d, device_id_type=MESH)

    def cols(j):
        return pl.ds(pl.multiple_of(j * TILE, TILE), TILE)

    def g_sub(zq, rq, j, s):
        return g.at[zq, pl.ds(pl.multiple_of(rq * blk + s * rows_s, rows_s), rows_s), cols(j)]

    def g_piece(zq, rq, j):
        return g.at[zq, pl.ds(pl.multiple_of(rq * blk, blk), blk), cols(j)]

    def g_block(zq, rq):
        return g.at[zq, pl.ds(pl.multiple_of(rq * blk, blk), blk), :]

    def copy_to(ref, ssem, rsem, d):
        remote(ref, ref, ssem, rsem, d).start()

    def wait_for(ref, rsem):
        remote(ref, ref, send_sem.at[0], rsem, dev(z, r)).wait_recv()

    def wait_sent(ref, ssem):
        remote(ref, ref, ssem, re.at[0, 0], dev(z, r)).wait_send()

    def send_partner(zq, rq, j):
        copy_to(g_piece(zq, rq, j), send_sem.at[4 + zq], rp.at[zq, j], dev(zm, r_p))

    def wait_partner(zq, j):
        wait_for(g.at[zq, pl.ds(0, 2 * blk), cols(j)], rp.at[zq, j])

    def quarter(zq):
        return pl.ds(pl.multiple_of(zq * blk, blk), blk)

    def a_quarter(zq):
        return a.at[:, quarter(zq)]

    def a_sub(s):
        return pl.ds(pl.multiple_of(s * rows_a, rows_a), rows_a)

    def out_rows(h):
        return pl.ds(pl.multiple_of(h * half, half), half)

    barrier = pltpu.get_barrier_semaphore()

    @pl.when(middle)
    def _():
        for dz in range(2):
            for dr in range(n_col):
                peer_z = zm if dz == 0 else zmo
                if dz == 0 and dr == 0:
                    peer_z = zc
                pl.semaphore_signal(barrier, inc=1, device_id=dev(peer_z, (r + dr) % n_col), device_id_type=MESH)

    @pl.when(jnp.logical_not(middle))
    def _():
        pl.semaphore_signal(barrier, inc=1, device_id=dev(zm, r), device_id_type=MESH)
        pl.semaphore_signal(barrier, inc=1, device_id=dev(zc, r_y), device_id_type=MESH)

    def load(src, h, slot):
        return pltpu.make_async_copy(src.at[out_rows(h), :], acc.at[slot], load_sem.at[slot])

    loads = (load(a_hbm, 1 - side, 0), load(g_hbm, 0, 1), load(g_hbm, 1, 2), load(a_hbm, side, 3))
    for copy in loads:
        copy.start()
    loads[0].wait()
    snd[0] = acc[0].astype(jnp.bfloat16)
    pl.semaphore_wait(barrier, jnp.where(middle, 2 * n_col, 2))

    @pl.when(middle)
    def _():
        remote(snd.at[0], a_quarter(zm), send_sem.at[3], ra.at[1], dev(zmo, r)).start()

    @pl.when(jnp.logical_not(middle))
    def _():
        @pl.loop(0, SUBS)
        def _(s):
            remote(snd.at[0, a_sub(s), :], snd.at[1, a_sub(s), :], send_sem.at[3], ra_relay.at[s], dev(zm, r)).start()

    for h in range(2):
        loads[1 + h].wait()
        g[z, pl.ds(pl.multiple_of(r * blk + h * half, half), half), :] = acc[1 + h].astype(jnp.bfloat16)

    @pl.when(jnp.logical_not(middle))
    def _():
        inner = dev(zm, r)

        @pl.loop(0, pieces)
        def _(j):
            copy_to(g_piece(z, r, j), send_sem.at[1], ry.at[0, j], dev(zc, r_y))

        loads[3].wait()
        a[:, quarter(z)] = acc[3].astype(jnp.bfloat16)
        remote(a_quarter(z), a_quarter(z), send_sem.at[3], ra.at[0], inner).start()

        @pl.loop(0, pieces)
        def _(j):
            copy_to(g_piece(z, r, j), send_sem.at[2], re.at[0, j], inner)

        @pl.loop(0, pieces)
        def _(j):
            wait_for(g_piece(z, r_y, j), ry.at[0, j])
            copy_to(g_piece(z, r_y, j), send_sem.at[2], re.at[1, j], inner)

        wait_sent(snd, send_sem.at[3])
        wait_sent(g_block(z, r), send_sem.at[1])
        wait_sent(g.at[0, pl.ds(0, 2 * blk), :], send_sem.at[2])

        for kind, h in ((1, side), (2, 1 - side)):
            @pl.loop(0, pieces)
            def _(j):
                wait_for(m_out.at[out_rows(h), cols(j)], fin_recv.at[kind, j])

        wait_for(s_out, sc_sem.at[1])

    @pl.when(middle)
    def _():
        other = dev(zmo, r)
        across = dev(zm, r_y)
        corner = dev(zc, r)
        me = side * n_col + r

        def peers():
            for dz in range(2):
                for dr in range(n_col):
                    if dz or dr:
                        yield (zmo if dz else zm), (r + dr) % n_col

        def sums_of(i):
            if i == 0:
                return ps_mid, ar_mid
            if i <= pieces:
                return ps_edge.at[i - 1], ar_edge.at[i - 1]
            return ps.at[i - pieces - 1], ar.at[i - pieces - 1]

        def send_sums(i):
            src, slots = sums_of(i)
            for pz, pr in peers():
                remote(src, slots.at[me], ar_send.at[i], ar_recv.at[i], dev(pz, pr)).start()
            slots[me] = src[...]

        def peer_slots(i):
            return sums_of(i)[1].at[pl.ds(0, 2 * n_col - 1)]

        def scales(i):
            src, slots = sums_of(i)
            wait_for(peer_slots(i), ar_recv.at[i])
            total = slots[0]
            for peer in range(1, 2 * n_col):
                total = total + slots[peer]
            return n / total

        def square(zq, j, slot):
            step = 64

            def body(i, total):
                rows = pl.ds(pl.multiple_of(i * step, step), step)
                value = acc[zq, rows, cols(j)]
                value = value * value
                acc[zq, rows, cols(j)] = value
                return total + jnp.sum(value.reshape(step // 8, 8, TILE), axis=0)

            total = lax.fori_loop(0, half // step, body, jnp.zeros((8, TILE), jnp.float32))
            slot[...] = jnp.sum(total, axis=0, keepdims=True)

        def expand(zq, j, slot):
            acc[zq, :, cols(j)] = jnp.dot(a[...], g[zq, :, cols(j)], preferred_element_type=jnp.float32)
            square(zq, j, slot)

        @pl.loop(0, pieces)
        def _(j):
            copy_to(g_piece(zm, r, j), send_sem.at[1], ry.at[0, j], across)
            send_partner(zm, r, j)

        loads[3].wait()
        a[:, quarter(zm)] = acc[3].astype(jnp.bfloat16)

        @pl.loop(0, SUBS)
        def _(s):
            wait_for(snd.at[1, a_sub(s), :], ra_relay.at[s])
            remote(snd.at[1, a_sub(s), :], a.at[a_sub(s), quarter(zc)], send_sem.at[3], ra.at[2], other).start()

        @pl.loop(0, pieces * SUBS)
        def _(i):
            copy_to(g_sub(zm, r, i // SUBS, i % SUBS), send_sem.at[0], rm.at[0, i // SUBS, i % SUBS], other)

        @pl.loop(0, pieces)
        def _(j):
            wait_for(g_piece(zm, r_y, j), ry.at[0, j])
            send_partner(zm, r_y, j)

        for idx, zq in ((1, zmo), (2, zco), (0, zc)):
            wait_for(a_quarter(zq), ra.at[idx])

        def finish_mid():
            scale = scales(0)
            for idx, zq in ((0, 1), (1, 2)):
                a1[:, pl.ds(zq * blk, blk)] = (acc[zq] * scale[idx]).astype(jnp.bfloat16)

        def finish_edge(j):
            scale = scales(1 + j)
            for idx, zq in ((0, 0), (1, 3)):
                a1[:, pl.ds(zq * blk + j * TILE, TILE)] = (
                    acc[zq, :, pl.ds(j * TILE, TILE)] * scale[idx]).astype(jnp.bfloat16)

        def partial(zq, k0, k_len, n0, n_len):
            rows = pl.ds(pl.multiple_of(k0, TILE), k_len)
            return jnp.dot(a1[:, rows], g[zq, rows, pl.ds(pl.multiple_of(n0, TILE), n_len)],
                           preferred_element_type=jnp.float32)

        def mid_by_mid(zq):
            @pl.loop(0, pieces)
            def _(j):
                acc[zq, :, cols(j)] = (partial(zq, blk, blk, j * TILE, TILE) + partial(zq, 2 * blk, blk, j * TILE, TILE))

        def new_columns(j):
            @pl.loop(0, 2)
            def _(i):
                zq = 3 * i
                total = partial(zq, blk, blk, j * TILE, TILE) + partial(zq, 2 * blk, blk, j * TILE, TILE)
                for k_z in (0, 3):
                    total += partial(zq, k_z * blk, (j + 1) * TILE, j * TILE, TILE)
                acc[zq, :, pl.ds(j * TILE, TILE)] = total

        def old_columns(j):
            def add(zq, n0, n_len):
                span = pl.ds(pl.multiple_of(n0, TILE), n_len)
                acc[zq, :, span] += (partial(zq, j * TILE, TILE, n0, n_len)
                                     + partial(zq, 3 * blk + j * TILE, TILE, n0, n_len))

            wide = 2 * TILE

            @pl.loop(0, 2 * blk // wide)
            def _(i):
                per = blk // wide
                add(1 + i // per, (i % per) * wide, wide)

            if j:
                @pl.loop(0, 2 * j)
                def _(i):
                    add(3 * (i // j), (i % j) * TILE, TILE)

        n_slices = pieces * SUBS

        def from_other(q):
            return zmo + (q // pieces) * (zco - zmo)

        def pump(i):
            q, s = i // SUBS, i % SUBS
            late, j = q // pieces, q % pieces
            z_m = from_other(q)
            ahead = i + AHEAD - n_slices

            @pl.when(jnp.logical_and(ahead >= 0, ahead < n_slices))
            def _():
                ref = g_sub(zc, r, ahead // SUBS, ahead % SUBS)
                copy_to(ref, send_sem.at[0], rm.at[1, ahead // SUBS, ahead % SUBS], other)

            ref = g_sub(z_m, r, j, s)
            wait_for(ref, rm.at[late, j, s])
            copy_to(ref, send_sem.at[1], ry.at[1 + late, j], across)

            @pl.when(s == SUBS - 1)
            def _():
                r_e = r + late * (r_y - r)
                send_partner(z_m, r, j)
                wait_for(g_piece(zc, r_e, j), re.at[late, j])
                send_partner(zc, r_e, j)

            @pl.when(jnp.logical_and(i >= LAG, (i - LAG) % SUBS == SUBS - 1))
            def _():
                piece_across((i - LAG) // SUBS)

        def piece_across(q):
            late, j = q // pieces, q % pieces
            wait_for(g_piece(from_other(q), r_y, j), ry.at[1 + late, j])
            send_partner(from_other(q), r_y, j)

        @pl.loop(0, pieces + 1)
        def _(q):
            @pl.loop(0, SUBS)
            def _(s):
                pump(q * SUBS + s)
                first = q == 0
                zq = jnp.where(first, zm, zmo)
                jq = jnp.where(first, s, q - 1)

                @pl.when(jnp.logical_or(first, s == SUBS - 1))
                def _():
                    wait_partner(zq, jq)
                    expand(zq, jq, ps_mid.at[zq - 1, :, cols(jq)])

        send_sums(0)

        def edge_step(j, second, third, fourth):
            @pl.loop(0, SUBS)
            def _(s):
                pump((pieces + 1 + j) * SUBS + s)

                @pl.when(jnp.logical_or(s == 0, s == SUBS - 1))
                def _():
                    zq = jnp.where(s == 0, zc, zco)
                    wait_partner(zq, j)
                    expand(zq, j, ps_edge.at[j, zq // 3])

                @pl.when(s == 1)
                def _():
                    second()

                @pl.when(s == 2)
                def _():
                    third()

            send_sums(1 + j)
            fourth()

        def mid_start():
            finish_mid()
            mid_by_mid(1)

        def edge_start(j):
            finish_edge(j)
            new_columns(j)

        def idle():
            pass

        edge_step(0, idle, mid_start, idle)
        edge_step(1, lambda: mid_by_mid(2), lambda: edge_start(0), idle)
        edge_step(2, lambda: old_columns(0), lambda: edge_start(1), lambda: old_columns(1))

        last = pieces - 1

        def last_piece(zq):
            wait_partner(zq, last)
            expand(zq, last, ps_edge.at[last, zq // 3])

        last_piece(zc)
        piece_across(2 * pieces - 1)
        edge_start(last - 1)
        last_piece(zco)
        send_sums(pieces)
        old_columns(last - 1)
        edge_start(last)
        old_columns(last)

        @pl.loop(0, n_col)
        def _(zq):
            for j in range(pieces):
                square(zq, j, ps.at[0, zq, :, cols(j)])

        send_sums(pieces + 1)
        sc[...] = scales(pieces + 1)

        @pl.loop(0, n_col)
        def _(zq):
            a[:, quarter(zq)] = (acc[zq] * sc[zq]).astype(jnp.bfloat16)

        @pl.loop(0, pieces)
        def _(j):
            @pl.loop(0, 2)
            def _(i):
                zq = zco + i * (zc - zco)
                expand(zq, j, ps.at[1, zq, :, cols(j)])
                done = acc.at[zq, :, cols(j)]

                @pl.when(i == 0)
                def _():
                    remote(done, fin.at[:, cols(j)], fin_send.at[0], fin_recv.at[2, j], other).start()

                @pl.when(i == 1)
                def _():
                    remote(done, m_out.at[out_rows(side), cols(j)], fin_send.at[1], fin_recv.at[1, j], corner).start()

        @pl.loop(0, 2 * pieces)
        def _(i):
            zq = zmo + (i // pieces) * (zm - zmo)
            j = i % pieces
            expand(zq, j, ps.at[1, zq, :, cols(j)])

        send_sums(pieces + 2)
        remote(acc.at[zmo], m_out.at[out_rows(side), :], fin_send.at[2], fin_recv.at[0, 0], other).start()
        m_out[out_rows(side), :] = acc[zm]

        @pl.loop(0, pieces)
        def _(j):
            ref = fin.at[:, cols(j)]
            wait_for(ref, fin_recv.at[2, j])
            remote(ref, m_out.at[out_rows(1 - side), cols(j)], fin_send.at[3], fin_recv.at[2, j], corner).start()

        sc[...] = scales(pieces + 2)
        remote(sc.at[zc], s_out, sc_sem.at[0], sc_sem.at[1], corner).start()
        s_out[...] = sc[zm]

        wait_sent(snd, send_sem.at[3])
        wait_sent(g.at[0, pl.ds(0, 2 * blk), :], send_sem.at[0])
        wait_sent(g.at[0, pl.ds(0, 3 * blk), :], send_sem.at[1])
        for zq in range(n_col):
            wait_sent(g.at[0, pl.ds(0, 2 * blk), :], send_sem.at[4 + zq])
        for i in range(pieces + 3):
            wait_sent(peer_slots(i), ar_send.at[i])
        for i in range(4):
            wait_sent(acc.at[0], fin_send.at[i])
        wait_sent(sc.at[0], sc_sem.at[0])
        wait_for(m_out.at[out_rows(1 - side), :], fin_recv.at[0, 0])


def solution(mesh):
    num_cols = mesh.shape["col"]
    num_rows = mesh.shape["row"]
    block_spec = P(("graph", "row"), "col")

    def device_step(init_blk, graph_blk):
        blk = init_blk.shape[0]
        n = blk * num_rows
        half = blk // 2
        pieces = blk // TILE
        cores = 2 * num_rows
        any_spec = pl.BlockSpec(memory_space=pl.ANY)
        vmem_spec = pl.BlockSpec(memory_space=pltpu.VMEM)
        squares, scale = pl.pallas_call(
            mcl_kernel,
            out_shape=(pltpu.VMEM((blk, blk), jnp.float32), pltpu.VMEM((1, blk), jnp.float32)),
            in_specs=[any_spec, any_spec],
            out_specs=(vmem_spec, vmem_spec),
            scratch_shapes=[
                pltpu.VMEM((num_cols, n, blk), jnp.bfloat16),
                pltpu.VMEM((half, n), jnp.bfloat16),
                pltpu.VMEM((half, n), jnp.bfloat16),
                pltpu.VMEM((2, half, blk), jnp.bfloat16),
                pltpu.VMEM((num_cols, half, blk), jnp.float32),
                pltpu.VMEM((half, blk), jnp.float32),
                pltpu.VMEM((2, 1, blk), jnp.float32),
                pltpu.VMEM((cores, 2, 1, blk), jnp.float32),
                pltpu.VMEM((pieces, 2, 1, TILE), jnp.float32),
                pltpu.VMEM((pieces, cores, 2, 1, TILE), jnp.float32),
                pltpu.VMEM((2, num_cols, 1, blk), jnp.float32),
                pltpu.VMEM((2, cores, num_cols, 1, blk), jnp.float32),
                pltpu.VMEM((num_cols, 1, blk), jnp.float32),
                pltpu.SemaphoreType.DMA((4,)),
                pltpu.SemaphoreType.DMA((2, pieces, SUBS)),
                pltpu.SemaphoreType.DMA((2, pieces)),
                pltpu.SemaphoreType.DMA((3, pieces)),
                pltpu.SemaphoreType.DMA((num_cols, pieces)),
                pltpu.SemaphoreType.DMA((SUBS,)),
                pltpu.SemaphoreType.DMA((3,)),
                pltpu.SemaphoreType.DMA((4 + num_cols,)),
                pltpu.SemaphoreType.DMA((4,)),
                pltpu.SemaphoreType.DMA((pieces + 3,)),
                pltpu.SemaphoreType.DMA((pieces + 3,)),
                pltpu.SemaphoreType.DMA((3, pieces)),
                pltpu.SemaphoreType.DMA((2,)),
            ],
            compiler_params=pltpu.CompilerParams(
                collective_id=0, has_side_effects=True, vmem_limit_bytes=60_000_000),
        )(init_blk, graph_blk)
        return squares * scale

    return jax.shard_map(device_step, mesh=mesh, in_specs=(block_spec, block_spec), out_specs=block_spec, check_vma=False)
```

```python
import jax
import jax.numpy as jnp
from jax import lax
from jax.experimental import pallas as pl
from jax.experimental.pallas import tpu as pltpu
from jax.sharding import PartitionSpec as P

SUBS = 4
TILE = 256
AHEAD = 2
LAG = 3
MESH = pl.DeviceIdType.MESH


def mcl_kernel(a_hbm, g_hbm, m_out, s_out, g, a, a1, snd, acc, fin, ps_mid, ar_mid, ps_edge, ar_edge, ps, ar, sc,
               load_sem, rm, re, ry, rp, ra_relay, ra, send_sem, fin_send, ar_send, ar_recv, fin_recv, sc_sem):
    n_col = g.shape[0]
    blk = g.shape[2]
    n = g.shape[1]
    half = blk // 2
    pieces = blk // TILE
    rows_s = blk // SUBS
    rows_a = half // SUBS

    z = lax.axis_index("col")
    r = lax.axis_index("row")
    y = r // 2
    c = r % 2
    side = z // 2
    middle = jnp.logical_or(z == 1, z == 2)
    zm = 1 + side
    zc = 3 * side
    zmo = 2 - side
    zco = 3 - 3 * side
    r_y = 2 * (1 - y) + c
    r_p = 2 * y + 1 - c

    def dev(zq, rq):
        return {"col": zq, "row": rq}

    def remote(src, dst, ssem, rsem, d):
        return pltpu.make_async_remote_copy(
            src_ref=src, dst_ref=dst, send_sem=ssem, recv_sem=rsem, device_id=d, device_id_type=MESH)

    def cols(j):
        return pl.ds(pl.multiple_of(j * TILE, TILE), TILE)

    def g_sub(zq, rq, j, s):
        return g.at[zq, pl.ds(pl.multiple_of(rq * blk + s * rows_s, rows_s), rows_s), cols(j)]

    def g_piece(zq, rq, j):
        return g.at[zq, pl.ds(pl.multiple_of(rq * blk, blk), blk), cols(j)]

    def g_block(zq, rq):
        return g.at[zq, pl.ds(pl.multiple_of(rq * blk, blk), blk), :]

    def copy_to(ref, ssem, rsem, d):
        remote(ref, ref, ssem, rsem, d).start()

    def wait_for(ref, rsem):
        remote(ref, ref, send_sem.at[0], rsem, dev(z, r)).wait_recv()

    def wait_sent(ref, ssem):
        remote(ref, ref, ssem, re.at[0, 0], dev(z, r)).wait_send()

    def send_partner(zq, rq, j):
        copy_to(g_piece(zq, rq, j), send_sem.at[4 + zq], rp.at[zq, j], dev(zm, r_p))

    def wait_partner(zq, j):
        wait_for(g.at[zq, pl.ds(0, 2 * blk), cols(j)], rp.at[zq, j])

    def quarter(zq):
        return pl.ds(pl.multiple_of(zq * blk, blk), blk)

    def a_quarter(zq):
        return a.at[:, quarter(zq)]

    def a_sub(s):
        return pl.ds(pl.multiple_of(s * rows_a, rows_a), rows_a)

    def out_rows(h):
        return pl.ds(pl.multiple_of(h * half, half), half)

    barrier = pltpu.get_barrier_semaphore()

    @pl.when(middle)
    def _():
        for dz in range(2):
            for dr in range(n_col):
                peer_z = zm if dz == 0 else zmo
                if dz == 0 and dr == 0:
                    peer_z = zc
                pl.semaphore_signal(barrier, inc=1, device_id=dev(peer_z, (r + dr) % n_col), device_id_type=MESH)

    @pl.when(jnp.logical_not(middle))
    def _():
        pl.semaphore_signal(barrier, inc=1, device_id=dev(zm, r), device_id_type=MESH)
        pl.semaphore_signal(barrier, inc=1, device_id=dev(zc, r_y), device_id_type=MESH)

    def load(src, h, slot):
        return pltpu.make_async_copy(src.at[out_rows(h), :], acc.at[slot], load_sem.at[slot])

    loads = (load(a_hbm, 1 - side, 0), load(g_hbm, 0, 1), load(g_hbm, 1, 2), load(a_hbm, side, 3))
    for copy in loads:
        copy.start()
    loads[0].wait()
    snd[0] = acc[0].astype(jnp.bfloat16)
    pl.semaphore_wait(barrier, jnp.where(middle, 2 * n_col, 2))

    @pl.when(middle)
    def _():
        remote(snd.at[0], a_quarter(zm), send_sem.at[3], ra.at[1], dev(zmo, r)).start()

    @pl.when(jnp.logical_not(middle))
    def _():
        @pl.loop(0, SUBS)
        def _(s):
            remote(snd.at[0, a_sub(s), :], snd.at[1, a_sub(s), :], send_sem.at[3], ra_relay.at[s], dev(zm, r)).start()

    for h in range(2):
        loads[1 + h].wait()
        g[z, pl.ds(pl.multiple_of(r * blk + h * half, half), half), :] = acc[1 + h].astype(jnp.bfloat16)

    @pl.when(jnp.logical_not(middle))
    def _():
        inner = dev(zm, r)

        @pl.loop(0, pieces)
        def _(j):
            copy_to(g_piece(z, r, j), send_sem.at[1], ry.at[0, j], dev(zc, r_y))

        loads[3].wait()
        a[:, quarter(z)] = acc[3].astype(jnp.bfloat16)
        remote(a_quarter(z), a_quarter(z), send_sem.at[3], ra.at[0], inner).start()

        @pl.loop(0, pieces)
        def _(j):
            copy_to(g_piece(z, r, j), send_sem.at[2], re.at[0, j], inner)

        @pl.loop(0, pieces)
        def _(j):
            wait_for(g_piece(z, r_y, j), ry.at[0, j])
            copy_to(g_piece(z, r_y, j), send_sem.at[2], re.at[1, j], inner)

        wait_sent(snd, send_sem.at[3])
        wait_sent(g_block(z, r), send_sem.at[1])
        wait_sent(g.at[0, pl.ds(0, 2 * blk), :], send_sem.at[2])

        for kind, h in ((1, side), (2, 1 - side)):
            @pl.loop(0, pieces)
            def _(j):
                wait_for(m_out.at[out_rows(h), cols(j)], fin_recv.at[kind, j])

        wait_for(s_out, sc_sem.at[1])

    @pl.when(middle)
    def _():
        other = dev(zmo, r)
        across = dev(zm, r_y)
        corner = dev(zc, r)
        me = side * n_col + r

        def peers():
            for dz in range(2):
                for dr in range(n_col):
                    if dz or dr:
                        yield (zmo if dz else zm), (r + dr) % n_col

        exchanges = [(ps_mid.at[0], ar_mid.at[0])]
        exchanges += [(ps_edge.at[j], ar_edge.at[j]) for j in range(pieces)]
        exchanges += [(ps_mid.at[1], ar_mid.at[1]), (ps_mid.at[2], ar_mid.at[2]), (ps, ar)]
        second_mid, second_edge, third = pieces + 1, pieces + 2, pieces + 3

        def sums_of(i):
            return exchanges[i]

        def send_sums(i):
            src, slots = sums_of(i)
            for pz, pr in peers():
                remote(src, slots.at[me], ar_send.at[i], ar_recv.at[i], dev(pz, pr)).start()
            slots[me] = src[...]

        def peer_slots(i):
            return sums_of(i)[1].at[pl.ds(0, 2 * n_col - 1)]

        def scales(i):
            src, slots = sums_of(i)
            wait_for(peer_slots(i), ar_recv.at[i])
            total = slots[0]
            for peer in range(1, 2 * n_col):
                total = total + slots[peer]
            return n / total

        def square(value, zq, span, slot):
            value = value * value
            acc[zq, :, span] = value
            slot[...] = jnp.sum(value, axis=0, keepdims=True)

        def expand(zq, j, slot):
            square(jnp.dot(a[...], g[zq, :, cols(j)], preferred_element_type=jnp.float32), zq, cols(j), slot)

        @pl.loop(0, pieces)
        def _(j):
            copy_to(g_piece(zm, r, j), send_sem.at[1], ry.at[0, j], across)
            send_partner(zm, r, j)

        loads[3].wait()
        a[:, quarter(zm)] = acc[3].astype(jnp.bfloat16)

        @pl.loop(0, SUBS)
        def _(s):
            wait_for(snd.at[1, a_sub(s), :], ra_relay.at[s])
            remote(snd.at[1, a_sub(s), :], a.at[a_sub(s), quarter(zc)], send_sem.at[3], ra.at[2], other).start()

        @pl.loop(0, pieces * SUBS)
        def _(i):
            copy_to(g_sub(zm, r, i // SUBS, i % SUBS), send_sem.at[0], rm.at[0, i // SUBS, i % SUBS], other)

        @pl.loop(0, pieces)
        def _(j):
            wait_for(g_piece(zm, r_y, j), ry.at[0, j])
            send_partner(zm, r_y, j)

        for idx, zq in ((1, zmo), (2, zco), (0, zc)):
            wait_for(a_quarter(zq), ra.at[idx])

        def finish_mid():
            scale = scales(0)
            for idx, zq in ((0, 1), (1, 2)):
                a1[:, pl.ds(zq * blk, blk)] = (acc[zq] * scale[idx]).astype(jnp.bfloat16)

        def finish_edge(j):
            scale = scales(1 + j)
            for idx, zq in ((0, 0), (1, 3)):
                a1[:, pl.ds(zq * blk + j * TILE, TILE)] = (
                    acc[zq, :, pl.ds(j * TILE, TILE)] * scale[idx]).astype(jnp.bfloat16)

        def partial(rows, zq, k0, k_len, n0, n_len):
            k = pl.ds(pl.multiple_of(k0, TILE), k_len)
            return jnp.dot(rows[:, k], g[zq, k, pl.ds(pl.multiple_of(n0, TILE), n_len)],
                           preferred_element_type=jnp.float32)

        def two_quarters(rows, zq, k_len, n0, *k_z):
            first, second = (partial(rows, zq, k * blk, k_len, n0, TILE) for k in k_z)
            return first + second

        def mid_by_mid(zq):
            @pl.loop(0, pieces)
            def _(j):
                acc[zq, :, cols(j)] = two_quarters(a1, zq, blk, j * TILE, 1, 2)

        def new_columns(j):
            @pl.loop(0, 2)
            def _(i):
                zq = 3 * i
                span = pl.ds(j * TILE, TILE)
                total = (two_quarters(a1, zq, blk, j * TILE, 1, 2)
                         + two_quarters(a1, zq, (j + 1) * TILE, j * TILE, 0, 3))
                if j == pieces - 1:
                    square(total, zq, span, ps_mid.at[2, i, :, span])
                else:
                    acc[zq, :, span] = total

        def old_columns(j, zq, width, slot):
            span = pl.ds(0, width)
            total = (acc[zq, :, span] + partial(a1, zq, j * TILE, TILE, 0, width)
                     + partial(a1, zq, 3 * blk + j * TILE, TILE, 0, width))
            if j == pieces - 1:
                square(total, zq, span, slot.at[:, span])
            else:
                acc[zq, :, span] = total

        def old_mid(j):
            @pl.loop(0, 2)
            def _(i):
                old_columns(j, 1 + i, blk, ps_mid.at[1, i])

        def old_edge(j):
            if j:
                @pl.loop(0, 2)
                def _(i):
                    old_columns(j, 3 * i, j * TILE, ps_mid.at[2, i])

        n_slices = pieces * SUBS

        def from_other(q):
            return zmo + (q // pieces) * (zco - zmo)

        def pump(i):
            q, s = i // SUBS, i % SUBS
            late, j = q // pieces, q % pieces
            z_m = from_other(q)
            ahead = i + AHEAD - n_slices

            @pl.when(jnp.logical_and(ahead >= 0, ahead < n_slices))
            def _():
                ref = g_sub(zc, r, ahead // SUBS, ahead % SUBS)
                copy_to(ref, send_sem.at[0], rm.at[1, ahead // SUBS, ahead % SUBS], other)

            ref = g_sub(z_m, r, j, s)
            wait_for(ref, rm.at[late, j, s])
            copy_to(ref, send_sem.at[1], ry.at[1 + late, j], across)

            @pl.when(s == SUBS - 1)
            def _():
                r_e = r + late * (r_y - r)
                send_partner(z_m, r, j)
                wait_for(g_piece(zc, r_e, j), re.at[late, j])
                send_partner(zc, r_e, j)

            @pl.when(jnp.logical_and(i >= LAG, (i - LAG) % SUBS == SUBS - 1))
            def _():
                piece_across((i - LAG) // SUBS)

        def piece_across(q):
            late, j = q // pieces, q % pieces
            wait_for(g_piece(from_other(q), r_y, j), ry.at[1 + late, j])
            send_partner(from_other(q), r_y, j)

        @pl.loop(0, pieces + 1)
        def _(q):
            @pl.loop(0, SUBS)
            def _(s):
                pump(q * SUBS + s)
                first = q == 0
                zq = jnp.where(first, zm, zmo)
                jq = jnp.where(first, s, q - 1)

                @pl.when(jnp.logical_or(first, s == SUBS - 1))
                def _():
                    wait_partner(zq, jq)
                    expand(zq, jq, ps_mid.at[0, zq - 1, :, cols(jq)])

        send_sums(0)

        def edge_step(j, second, third, fourth):
            @pl.loop(0, SUBS)
            def _(s):
                pump((pieces + 1 + j) * SUBS + s)

                @pl.when(jnp.logical_or(s == 0, s == SUBS - 1))
                def _():
                    zq = jnp.where(s == 0, zc, zco)
                    wait_partner(zq, j)
                    expand(zq, j, ps_edge.at[j, zq // 3])

                @pl.when(s == 1)
                def _():
                    second()

                @pl.when(s == 2)
                def _():
                    third()

            send_sums(1 + j)
            fourth()

        def mid_start():
            finish_mid()
            mid_by_mid(1)

        def edge_start(j):
            finish_edge(j)
            new_columns(j)

        def old(j):
            old_mid(j)
            old_edge(j)

        def idle():
            pass

        def second_piece():
            edge_start(1)
            old(1)

        edge_step(0, idle, mid_start, idle)
        edge_step(1, lambda: mid_by_mid(2), lambda: edge_start(0), lambda: old(0))
        edge_step(2, idle, second_piece, idle)

        last = pieces - 1

        def last_piece(zq):
            wait_partner(zq, last)
            expand(zq, last, ps_edge.at[last, zq // 3])

        last_piece(zc)
        piece_across(2 * pieces - 1)
        edge_start(last - 1)
        last_piece(zco)
        send_sums(pieces)
        old(last - 1)
        finish_edge(last)
        old_mid(last)
        send_sums(second_mid)
        new_columns(last)
        old_edge(last)
        send_sums(second_edge)

        def finish_second(i, *quarters):
            scale = scales(i)
            for idx, zq in enumerate(quarters):
                a[:, quarter(zq)] = (acc[zq] * scale[idx]).astype(jnp.bfloat16)

        finish_second(second_mid, 1, 2)

        @pl.loop(0, 2)
        def _(i):
            acc[zm, :, cols(i)] = two_quarters(a, zc + i * (zco - zc), blk, 0, 1, 2)

        finish_second(second_edge, 0, 3)

        def send_result(i, zq, j):
            done = acc.at[zq, :, cols(j)]

            @pl.when(i == 0)
            def _():
                remote(done, m_out.at[out_rows(side), cols(j)], fin_send.at[1], fin_recv.at[1, j], corner).start()

            @pl.when(i == 1)
            def _():
                remote(done, fin.at[:, cols(j)], fin_send.at[0], fin_recv.at[2, j], other).start()

        @pl.loop(0, 2)
        def _(i):
            zq = zc + i * (zco - zc)
            square(acc[zm, :, cols(i)] + two_quarters(a, zq, blk, 0, 0, 3), zq, cols(0), ps.at[zq, :, cols(0)])
            send_result(i, zq, 0)

        @pl.loop(1, pieces)
        def _(j):
            @pl.loop(0, 2)
            def _(i):
                zq = zc + i * (zco - zc)
                expand(zq, j, ps.at[zq, :, cols(j)])
                send_result(i, zq, j)

        @pl.loop(0, 2 * pieces)
        def _(i):
            zq = zmo + (i // pieces) * (zm - zmo)
            j = i % pieces
            expand(zq, j, ps.at[zq, :, cols(j)])

        send_sums(third)
        remote(acc.at[zmo], m_out.at[out_rows(side), :], fin_send.at[2], fin_recv.at[0, 0], other).start()
        m_out[out_rows(side), :] = acc[zm]

        @pl.loop(0, pieces)
        def _(j):
            ref = fin.at[:, cols(j)]
            wait_for(ref, fin_recv.at[2, j])
            remote(ref, m_out.at[out_rows(1 - side), cols(j)], fin_send.at[3], fin_recv.at[2, j], corner).start()

        sc[...] = scales(third)
        remote(sc.at[zc], s_out, sc_sem.at[0], sc_sem.at[1], corner).start()
        s_out[...] = sc[zm]

        wait_sent(snd, send_sem.at[3])
        wait_sent(g.at[0, pl.ds(0, 2 * blk), :], send_sem.at[0])
        wait_sent(g.at[0, pl.ds(0, 3 * blk), :], send_sem.at[1])
        for zq in range(n_col):
            wait_sent(g.at[0, pl.ds(0, 2 * blk), :], send_sem.at[4 + zq])
        for i in range(len(exchanges)):
            wait_sent(peer_slots(i), ar_send.at[i])
        for i in range(4):
            wait_sent(acc.at[0], fin_send.at[i])
        wait_sent(sc.at[0], sc_sem.at[0])
        wait_for(m_out.at[out_rows(1 - side), :], fin_recv.at[0, 0])


def solution(mesh):
    num_cols = mesh.shape["col"]
    num_rows = mesh.shape["row"]
    block_spec = P(("graph", "row"), "col")

    def device_step(init_blk, graph_blk):
        blk = init_blk.shape[0]
        n = blk * num_rows
        half = blk // 2
        pieces = blk // TILE
        cores = 2 * num_rows
        any_spec = pl.BlockSpec(memory_space=pl.ANY)
        vmem_spec = pl.BlockSpec(memory_space=pltpu.VMEM)
        squares, scale = pl.pallas_call(
            mcl_kernel,
            out_shape=(pltpu.VMEM((blk, blk), jnp.float32), pltpu.VMEM((1, blk), jnp.float32)),
            in_specs=[any_spec, any_spec],
            out_specs=(vmem_spec, vmem_spec),
            scratch_shapes=[
                pltpu.VMEM((num_cols, n, blk), jnp.bfloat16),
                pltpu.VMEM((half, n), jnp.bfloat16),
                pltpu.VMEM((half, n), jnp.bfloat16),
                pltpu.VMEM((2, half, blk), jnp.bfloat16),
                pltpu.VMEM((num_cols, half, blk), jnp.float32),
                pltpu.VMEM((half, blk), jnp.float32),
                pltpu.VMEM((3, 2, 1, blk), jnp.float32),
                pltpu.VMEM((3, cores, 2, 1, blk), jnp.float32),
                pltpu.VMEM((pieces, 2, 1, TILE), jnp.float32),
                pltpu.VMEM((pieces, cores, 2, 1, TILE), jnp.float32),
                pltpu.VMEM((num_cols, 1, blk), jnp.float32),
                pltpu.VMEM((cores, num_cols, 1, blk), jnp.float32),
                pltpu.VMEM((num_cols, 1, blk), jnp.float32),
                pltpu.SemaphoreType.DMA((4,)),
                pltpu.SemaphoreType.DMA((2, pieces, SUBS)),
                pltpu.SemaphoreType.DMA((2, pieces)),
                pltpu.SemaphoreType.DMA((3, pieces)),
                pltpu.SemaphoreType.DMA((num_cols, pieces)),
                pltpu.SemaphoreType.DMA((SUBS,)),
                pltpu.SemaphoreType.DMA((3,)),
                pltpu.SemaphoreType.DMA((4 + num_cols,)),
                pltpu.SemaphoreType.DMA((4,)),
                pltpu.SemaphoreType.DMA((pieces + 4,)),
                pltpu.SemaphoreType.DMA((pieces + 4,)),
                pltpu.SemaphoreType.DMA((3, pieces)),
                pltpu.SemaphoreType.DMA((2,)),
            ],
            compiler_params=pltpu.CompilerParams(
                collective_id=0, has_side_effects=True, vmem_limit_bytes=60_000_000),
        )(init_blk, graph_blk)
        return squares * scale

    return jax.shard_map(device_step, mesh=mesh, in_specs=(block_spec, block_spec), out_specs=block_spec, check_vma=False)
```

```python
import jax
import jax.numpy as jnp
from jax import lax
from jax.experimental import pallas as pl
from jax.experimental.pallas import tpu as pltpu
from jax.sharding import PartitionSpec as P

SUBS = 4
TILE = 256
AHEAD = 2
LAG = 2
MESH = pl.DeviceIdType.MESH


def mcl_kernel(a_hbm, g_hbm, m_out, s_out, g, a, a1, snd, acc, fin, ps_mid, ar_mid, ps_edge, ar_edge, ps, ar, sc,
               load_sem, rm, re, ry, rp, ra_relay, ra, send_sem, fin_send, ar_send, ar_recv, fin_recv, sc_sem):
    n_col = g.shape[0]
    blk = g.shape[2]
    n = g.shape[1]
    half = blk // 2
    pieces = blk // TILE
    rows_s = blk // SUBS
    rows_a = half // SUBS

    z = lax.axis_index("col")
    r = lax.axis_index("row")
    y = r // 2
    c = r % 2
    side = z // 2
    middle = jnp.logical_or(z == 1, z == 2)
    zm = 1 + side
    zc = 3 * side
    zmo = 2 - side
    zco = 3 - 3 * side
    r_y = 2 * (1 - y) + c
    r_p = 2 * y + 1 - c

    def dev(zq, rq):
        return {"col": zq, "row": rq}

    def remote(src, dst, ssem, rsem, d):
        return pltpu.make_async_remote_copy(
            src_ref=src, dst_ref=dst, send_sem=ssem, recv_sem=rsem, device_id=d, device_id_type=MESH)

    def cols(j):
        return pl.ds(pl.multiple_of(j * TILE, TILE), TILE)

    def g_sub(zq, rq, j, s):
        return g.at[zq, pl.ds(pl.multiple_of(rq * blk + s * rows_s, rows_s), rows_s), cols(j)]

    def g_piece(zq, rq, j):
        return g.at[zq, pl.ds(pl.multiple_of(rq * blk, blk), blk), cols(j)]

    def g_block(zq, rq):
        return g.at[zq, pl.ds(pl.multiple_of(rq * blk, blk), blk), :]

    def copy_to(ref, ssem, rsem, d):
        remote(ref, ref, ssem, rsem, d).start()

    def wait_for(ref, rsem):
        remote(ref, ref, send_sem.at[0], rsem, dev(z, r)).wait_recv()

    def wait_sent(ref, ssem):
        remote(ref, ref, ssem, re.at[0, 0], dev(z, r)).wait_send()

    def send_partner(zq, rq, j):
        copy_to(g_piece(zq, rq, j), send_sem.at[4 + zq], rp.at[zq, j], dev(zm, r_p))

    def wait_partner(zq, j):
        wait_for(g.at[zq, pl.ds(0, 2 * blk), cols(j)], rp.at[zq, j])

    def quarter(zq):
        return pl.ds(pl.multiple_of(zq * blk, blk), blk)

    def a_quarter(zq):
        return a.at[:, quarter(zq)]

    def a_sub(s):
        return pl.ds(pl.multiple_of(s * rows_a, rows_a), rows_a)

    def out_rows(h):
        return pl.ds(pl.multiple_of(h * half, half), half)

    barrier = pltpu.get_barrier_semaphore()

    @pl.when(middle)
    def _():
        for dz in range(2):
            for dr in range(n_col):
                peer_z = zm if dz == 0 else zmo
                if dz == 0 and dr == 0:
                    peer_z = zc
                pl.semaphore_signal(barrier, inc=1, device_id=dev(peer_z, (r + dr) % n_col), device_id_type=MESH)

    @pl.when(jnp.logical_not(middle))
    def _():
        pl.semaphore_signal(barrier, inc=1, device_id=dev(zm, r), device_id_type=MESH)
        pl.semaphore_signal(barrier, inc=1, device_id=dev(zc, r_y), device_id_type=MESH)

    def load(src, h, slot):
        return pltpu.make_async_copy(src.at[out_rows(h), :], acc.at[slot], load_sem.at[slot])

    loads = (load(a_hbm, 1 - side, 0), load(g_hbm, 0, 1), load(g_hbm, 1, 2), load(a_hbm, side, 3))
    for copy in loads:
        copy.start()
    loads[0].wait()
    snd[0] = acc[0].astype(jnp.bfloat16)
    pl.semaphore_wait(barrier, jnp.where(middle, 2 * n_col, 2))

    @pl.when(middle)
    def _():
        remote(snd.at[0], a_quarter(zm), send_sem.at[3], ra.at[1], dev(zmo, r)).start()

    @pl.when(jnp.logical_not(middle))
    def _():
        @pl.loop(0, SUBS)
        def _(s):
            remote(snd.at[0, a_sub(s), :], snd.at[1, a_sub(s), :], send_sem.at[3], ra_relay.at[s], dev(zm, r)).start()

    for h in range(2):
        loads[1 + h].wait()
        g[z, pl.ds(pl.multiple_of(r * blk + h * half, half), half), :] = acc[1 + h].astype(jnp.bfloat16)

    @pl.when(jnp.logical_not(middle))
    def _():
        inner = dev(zm, r)

        @pl.loop(0, pieces)
        def _(j):
            copy_to(g_piece(z, r, j), send_sem.at[1], ry.at[0, j], dev(zc, r_y))

        loads[3].wait()
        a[:, quarter(z)] = acc[3].astype(jnp.bfloat16)
        remote(a_quarter(z), a_quarter(z), send_sem.at[3], ra.at[0], inner).start()

        @pl.loop(0, pieces)
        def _(j):
            copy_to(g_piece(z, r, j), send_sem.at[2], re.at[0, j], inner)

        @pl.loop(0, pieces)
        def _(j):
            wait_for(g_piece(z, r_y, j), ry.at[0, j])
            copy_to(g_piece(z, r_y, j), send_sem.at[2], re.at[1, j], inner)

        wait_sent(snd, send_sem.at[3])
        wait_sent(g_block(z, r), send_sem.at[1])
        wait_sent(g.at[0, pl.ds(0, 2 * blk), :], send_sem.at[2])

        for kind, h in ((1, side), (2, 1 - side)):
            @pl.loop(0, pieces)
            def _(j):
                wait_for(m_out.at[out_rows(h), cols(j)], fin_recv.at[kind, j])

        wait_for(s_out, sc_sem.at[1])

    @pl.when(middle)
    def _():
        other = dev(zmo, r)
        across = dev(zm, r_y)
        corner = dev(zc, r)
        me = side * n_col + r

        def peers():
            for dz in range(2):
                for dr in range(n_col):
                    if dz or dr:
                        yield (zmo if dz else zm), (r + dr) % n_col

        exchanges = [(ps_mid.at[0], ar_mid.at[0])]
        exchanges += [(ps_edge.at[j], ar_edge.at[j]) for j in range(pieces)]
        exchanges += [(ps_mid.at[1], ar_mid.at[1]), (ps_mid.at[2], ar_mid.at[2]), (ps, ar)]
        second_mid, second_edge, third = pieces + 1, pieces + 2, pieces + 3

        def sums_of(i):
            return exchanges[i]

        def send_sums(i):
            src, slots = sums_of(i)
            for pz, pr in peers():
                remote(src, slots.at[me], ar_send.at[i], ar_recv.at[i], dev(pz, pr)).start()
            slots[me] = src[...]

        def peer_slots(i):
            return sums_of(i)[1].at[pl.ds(0, 2 * n_col - 1)]

        def scales(i):
            src, slots = sums_of(i)
            wait_for(peer_slots(i), ar_recv.at[i])
            total = slots[0]
            for peer in range(1, 2 * n_col):
                total = total + slots[peer]
            return n / total

        def square(value, zq, span, slot):
            value = value * value
            acc[zq, :, span] = value
            slot[...] = jnp.sum(value, axis=0, keepdims=True)

        def expand(zq, j, slot):
            square(jnp.dot(a[...], g[zq, :, cols(j)], preferred_element_type=jnp.float32), zq, cols(j), slot)

        @pl.loop(0, pieces)
        def _(j):
            copy_to(g_piece(zm, r, j), send_sem.at[1], ry.at[0, j], across)
            send_partner(zm, r, j)

        loads[3].wait()
        a[:, quarter(zm)] = acc[3].astype(jnp.bfloat16)

        @pl.loop(0, SUBS)
        def _(s):
            wait_for(snd.at[1, a_sub(s), :], ra_relay.at[s])
            remote(snd.at[1, a_sub(s), :], a.at[a_sub(s), quarter(zc)], send_sem.at[3], ra.at[2], other).start()

        @pl.loop(0, pieces * SUBS)
        def _(i):
            copy_to(g_sub(zm, r, i // SUBS, i % SUBS), send_sem.at[0], rm.at[0, i // SUBS, i % SUBS], other)

        @pl.loop(0, pieces)
        def _(j):
            wait_for(g_piece(zm, r_y, j), ry.at[0, j])
            send_partner(zm, r_y, j)

        for idx, zq in ((1, zmo), (2, zco), (0, zc)):
            wait_for(a_quarter(zq), ra.at[idx])

        def finish_mid():
            scale = scales(0)
            for idx, zq in ((0, 1), (1, 2)):
                a1[:, pl.ds(zq * blk, blk)] = (acc[zq] * scale[idx]).astype(jnp.bfloat16)

        def finish_edge(j):
            scale = scales(1 + j)
            for idx, zq in ((0, 0), (1, 3)):
                a1[:, pl.ds(zq * blk + j * TILE, TILE)] = (
                    acc[zq, :, pl.ds(j * TILE, TILE)] * scale[idx]).astype(jnp.bfloat16)

        def partial(rows, zq, k0, k_len, n0, n_len):
            k = pl.ds(pl.multiple_of(k0, TILE), k_len)
            return jnp.dot(rows[:, k], g[zq, k, pl.ds(pl.multiple_of(n0, TILE), n_len)],
                           preferred_element_type=jnp.float32)

        def two_quarters(rows, zq, k_len, n0, *k_z):
            first, second = (partial(rows, zq, k * blk, k_len, n0, TILE) for k in k_z)
            return first + second

        def mid_by_mid(zq):
            @pl.loop(0, pieces)
            def _(j):
                acc[zq, :, cols(j)] = two_quarters(a1, zq, blk, j * TILE, 1, 2)

        def new_columns(j):
            @pl.loop(0, 2)
            def _(i):
                zq = 3 * i
                acc[zq, :, pl.ds(j * TILE, TILE)] = (two_quarters(a1, zq, blk, j * TILE, 1, 2)
                                                     + two_quarters(a1, zq, (j + 1) * TILE, j * TILE, 0, 3))

        def last_new_columns(j):
            @pl.loop(0, 2)
            def _(i):
                zq = 3 * i
                fin[:, cols(i)] = (two_quarters(a1, zq, blk, j * TILE, 1, 2)
                                   + two_quarters(a1, zq, j * TILE, j * TILE, 0, 3))

        def piece_update(j, zq, n0, width):
            return partial(a1, zq, j * TILE, TILE, n0, width) + partial(a1, zq, 3 * blk + j * TILE, TILE, n0, width)

        def old_columns(j, zq, width, slot):
            span = pl.ds(0, width)
            total = acc[zq, :, span] + piece_update(j, zq, 0, width)
            if j == pieces - 1:
                square(total, zq, span, slot.at[:, span])
            else:
                acc[zq, :, span] = total

        def old_mid(j):
            @pl.loop(0, 2)
            def _(i):
                old_columns(j, 1 + i, blk, ps_mid.at[1, i])

        def old_edge(j):
            if j:
                @pl.loop(0, 2)
                def _(i):
                    old_columns(j, 3 * i, j * TILE, ps_mid.at[2, i])
            if j == pieces - 1:
                @pl.loop(0, 2)
                def _(i):
                    span = pl.ds(j * TILE, TILE)
                    square(fin[:, cols(i)] + piece_update(j, 3 * i, j * TILE, TILE), 3 * i, span, ps_mid.at[2, i, :, span])

        n_slices = pieces * SUBS

        def from_other(q):
            return zmo + (q // pieces) * (zco - zmo)

        def pump(i):
            q, s = i // SUBS, i % SUBS
            late, j = q // pieces, q % pieces
            z_m = from_other(q)
            ahead = i + AHEAD - n_slices

            @pl.when(jnp.logical_and(ahead >= 0, ahead < n_slices))
            def _():
                ref = g_sub(zc, r, ahead // SUBS, ahead % SUBS)
                copy_to(ref, send_sem.at[0], rm.at[1, ahead // SUBS, ahead % SUBS], other)

            ref = g_sub(z_m, r, j, s)
            wait_for(ref, rm.at[late, j, s])
            copy_to(ref, send_sem.at[1], ry.at[1 + late, j], across)

            @pl.when(s == SUBS - 1)
            def _():
                r_e = r + late * (r_y - r)
                send_partner(z_m, r, j)
                wait_for(g_piece(zc, r_e, j), re.at[late, j])
                send_partner(zc, r_e, j)

            @pl.when(jnp.logical_and(i >= LAG, (i - LAG) % SUBS == SUBS - 1))
            def _():
                piece_across((i - LAG) // SUBS)

        def piece_across(q):
            late, j = q // pieces, q % pieces
            wait_for(g_piece(from_other(q), r_y, j), ry.at[1 + late, j])
            send_partner(from_other(q), r_y, j)

        @pl.loop(0, pieces + 1)
        def _(q):
            @pl.loop(0, SUBS)
            def _(s):
                pump(q * SUBS + s)
                first = q == 0
                zq = jnp.where(first, zm, zmo)
                jq = jnp.where(first, s, q - 1)

                @pl.when(jnp.logical_or(first, s == SUBS - 1))
                def _():
                    wait_partner(zq, jq)
                    expand(zq, jq, ps_mid.at[0, zq - 1, :, cols(jq)])

        send_sums(0)

        def edge_step(j, tasks):
            @pl.loop(0, SUBS)
            def _(s):
                pump((pieces + 1 + j) * SUBS + s)

                @pl.when(s % 2 == 0)
                def _():
                    zq = jnp.where(s == 0, zc, zco)
                    wait_partner(zq, j)
                    expand(zq, j, ps_edge.at[j, zq // 3])

                @pl.when(s == 2)
                def _():
                    send_sums(1 + j)

                for at, task in tasks.items():
                    pl.when(s == at)(task)

        def mid_start():
            finish_mid()
            mid_by_mid(1)

        def edge_start(j):
            finish_edge(j)
            new_columns(j)

        def old(j):
            old_mid(j)
            old_edge(j)

        def first_piece():
            edge_start(0)
            old(0)

        edge_step(0, {3: mid_start})
        edge_step(1, {1: lambda: mid_by_mid(2), 3: first_piece})
        edge_step(2, {1: lambda: edge_start(1), 2: lambda: old(1)})

        last = pieces - 1

        def last_piece(zq):
            wait_partner(zq, last)
            expand(zq, last, ps_edge.at[last, zq // 3])

        last_piece(zc)
        edge_start(last - 1)
        piece_across(2 * pieces - 1)
        old_mid(last - 1)
        last_piece(zco)
        send_sums(pieces)
        old_edge(last - 1)
        last_new_columns(last)
        finish_edge(last)
        old_mid(last)
        send_sums(second_mid)
        old_edge(last)
        send_sums(second_edge)

        def finish_second(i, *quarters):
            scale = scales(i)
            for idx, zq in enumerate(quarters):
                a[:, quarter(zq)] = (acc[zq] * scale[idx]).astype(jnp.bfloat16)

        finish_second(second_mid, 1, 2)

        @pl.loop(0, 2)
        def _(i):
            acc[zm, :, cols(i)] = two_quarters(a, zc + i * (zco - zc), blk, 0, 1, 2)

        finish_second(second_edge, 0, 3)

        def send_result(i, zq, j):
            done = acc.at[zq, :, cols(j)]

            @pl.when(i == 0)
            def _():
                remote(done, m_out.at[out_rows(side), cols(j)], fin_send.at[1], fin_recv.at[1, j], corner).start()

            @pl.when(i == 1)
            def _():
                remote(done, fin.at[:, cols(j)], fin_send.at[0], fin_recv.at[2, j], other).start()

        @pl.loop(0, 2)
        def _(i):
            zq = zc + i * (zco - zc)
            square(acc[zm, :, cols(i)] + two_quarters(a, zq, blk, 0, 0, 3), zq, cols(0), ps.at[zq, :, cols(0)])
            send_result(i, zq, 0)

        @pl.loop(1, pieces)
        def _(j):
            @pl.loop(0, 2)
            def _(i):
                zq = zc + i * (zco - zc)
                expand(zq, j, ps.at[zq, :, cols(j)])
                send_result(i, zq, j)

        @pl.loop(0, 2 * pieces)
        def _(i):
            zq = zmo + (i // pieces) * (zm - zmo)
            j = i % pieces
            expand(zq, j, ps.at[zq, :, cols(j)])

        send_sums(third)
        remote(acc.at[zmo], m_out.at[out_rows(side), :], fin_send.at[2], fin_recv.at[0, 0], other).start()
        m_out[out_rows(side), :] = acc[zm]

        @pl.loop(0, pieces)
        def _(j):
            ref = fin.at[:, cols(j)]
            wait_for(ref, fin_recv.at[2, j])
            remote(ref, m_out.at[out_rows(1 - side), cols(j)], fin_send.at[3], fin_recv.at[2, j], corner).start()

        sc[...] = scales(third)
        remote(sc.at[zc], s_out, sc_sem.at[0], sc_sem.at[1], corner).start()
        s_out[...] = sc[zm]

        wait_sent(snd, send_sem.at[3])
        wait_sent(g.at[0, pl.ds(0, 2 * blk), :], send_sem.at[0])
        wait_sent(g.at[0, pl.ds(0, 3 * blk), :], send_sem.at[1])
        for zq in range(n_col):
            wait_sent(g.at[0, pl.ds(0, 2 * blk), :], send_sem.at[4 + zq])
        for i in range(len(exchanges)):
            wait_sent(peer_slots(i), ar_send.at[i])
        for i in range(4):
            wait_sent(acc.at[0], fin_send.at[i])
        wait_sent(sc.at[0], sc_sem.at[0])
        wait_for(m_out.at[out_rows(1 - side), :], fin_recv.at[0, 0])


def solution(mesh):
    num_cols = mesh.shape["col"]
    num_rows = mesh.shape["row"]
    block_spec = P(("graph", "row"), "col")

    def device_step(init_blk, graph_blk):
        blk = init_blk.shape[0]
        n = blk * num_rows
        half = blk // 2
        pieces = blk // TILE
        cores = 2 * num_rows
        any_spec = pl.BlockSpec(memory_space=pl.ANY)
        vmem_spec = pl.BlockSpec(memory_space=pltpu.VMEM)
        squares, scale = pl.pallas_call(
            mcl_kernel,
            out_shape=(pltpu.VMEM((blk, blk), jnp.float32), pltpu.VMEM((1, blk), jnp.float32)),
            in_specs=[any_spec, any_spec],
            out_specs=(vmem_spec, vmem_spec),
            scratch_shapes=[
                pltpu.VMEM((num_cols, n, blk), jnp.bfloat16),
                pltpu.VMEM((half, n), jnp.bfloat16),
                pltpu.VMEM((half, n), jnp.bfloat16),
                pltpu.VMEM((2, half, blk), jnp.bfloat16),
                pltpu.VMEM((num_cols, half, blk), jnp.float32),
                pltpu.VMEM((half, blk), jnp.float32),
                pltpu.VMEM((3, 2, 1, blk), jnp.float32),
                pltpu.VMEM((3, cores, 2, 1, blk), jnp.float32),
                pltpu.VMEM((pieces, 2, 1, TILE), jnp.float32),
                pltpu.VMEM((pieces, cores, 2, 1, TILE), jnp.float32),
                pltpu.VMEM((num_cols, 1, blk), jnp.float32),
                pltpu.VMEM((cores, num_cols, 1, blk), jnp.float32),
                pltpu.VMEM((num_cols, 1, blk), jnp.float32),
                pltpu.SemaphoreType.DMA((4,)),
                pltpu.SemaphoreType.DMA((2, pieces, SUBS)),
                pltpu.SemaphoreType.DMA((2, pieces)),
                pltpu.SemaphoreType.DMA((3, pieces)),
                pltpu.SemaphoreType.DMA((num_cols, pieces)),
                pltpu.SemaphoreType.DMA((SUBS,)),
                pltpu.SemaphoreType.DMA((3,)),
                pltpu.SemaphoreType.DMA((4 + num_cols,)),
                pltpu.SemaphoreType.DMA((4,)),
                pltpu.SemaphoreType.DMA((pieces + 4,)),
                pltpu.SemaphoreType.DMA((pieces + 4,)),
                pltpu.SemaphoreType.DMA((3, pieces)),
                pltpu.SemaphoreType.DMA((2,)),
            ],
            compiler_params=pltpu.CompilerParams(
                collective_id=0, has_side_effects=True, vmem_limit_bytes=60_000_000),
        )(init_blk, graph_blk)
        return squares * scale

    return jax.shard_map(device_step, mesh=mesh, in_specs=(block_spec, block_spec), out_specs=block_spec, check_vma=False)
```

```python
import jax
import jax.numpy as jnp
from jax import lax
from jax.experimental import pallas as pl
from jax.experimental.pallas import tpu as pltpu
from jax.sharding import PartitionSpec as P

SUBS = 4
TILE = 256
AHEAD = 3
LAG = 2
MESH = pl.DeviceIdType.MESH


def mcl_kernel(a_hbm, g_hbm, m_out, s_out, g, a, a1, snd, acc, fin, ps_mid, ar_mid, ps_edge, ar_edge, ps, ar, sc,
               load_sem, rm, re, ry, rp, ra_relay, ra, send_sem, fin_send, ar_send, ar_recv, fin_recv, sc_sem):
    n_col = g.shape[0]
    blk = g.shape[2]
    n = g.shape[1]
    half = blk // 2
    pieces = blk // TILE
    rows_s = blk // SUBS
    rows_a = half // SUBS

    z = lax.axis_index("col")
    r = lax.axis_index("row")
    y = r // 2
    c = r % 2
    side = z // 2
    middle = jnp.logical_or(z == 1, z == 2)
    zm = 1 + side
    zc = 3 * side
    zmo = 2 - side
    zco = 3 - 3 * side
    r_y = 2 * (1 - y) + c
    r_p = 2 * y + 1 - c

    def dev(zq, rq):
        return {"col": zq, "row": rq}

    def remote(src, dst, ssem, rsem, d):
        return pltpu.make_async_remote_copy(
            src_ref=src, dst_ref=dst, send_sem=ssem, recv_sem=rsem, device_id=d, device_id_type=MESH)

    def cols(j):
        return pl.ds(pl.multiple_of(j * TILE, TILE), TILE)

    def g_sub(zq, rq, j, s):
        return g.at[zq, pl.ds(pl.multiple_of(rq * blk + s * rows_s, rows_s), rows_s), cols(j)]

    def g_piece(zq, rq, j):
        return g.at[zq, pl.ds(pl.multiple_of(rq * blk, blk), blk), cols(j)]

    def g_block(zq, rq):
        return g.at[zq, pl.ds(pl.multiple_of(rq * blk, blk), blk), :]

    def copy_to(ref, ssem, rsem, d):
        remote(ref, ref, ssem, rsem, d).start()

    def wait_for(ref, rsem):
        remote(ref, ref, send_sem.at[0], rsem, dev(z, r)).wait_recv()

    def wait_sent(ref, ssem):
        remote(ref, ref, ssem, re.at[0, 0], dev(z, r)).wait_send()

    def send_partner(zq, rq, j):
        copy_to(g_piece(zq, rq, j), send_sem.at[4 + zq], rp.at[zq, j], dev(zm, r_p))

    def wait_partner(zq, j):
        wait_for(g.at[zq, pl.ds(0, 2 * blk), cols(j)], rp.at[zq, j])

    def quarter(zq):
        return pl.ds(pl.multiple_of(zq * blk, blk), blk)

    def a_quarter(zq):
        return a.at[:, quarter(zq)]

    def a_sub(s):
        return pl.ds(pl.multiple_of(s * rows_a, rows_a), rows_a)

    def out_rows(h):
        return pl.ds(pl.multiple_of(h * half, half), half)

    barrier = pltpu.get_barrier_semaphore()

    @pl.when(middle)
    def _():
        for dz in range(2):
            for dr in range(n_col):
                peer_z = zm if dz == 0 else zmo
                if dz == 0 and dr == 0:
                    peer_z = zc
                pl.semaphore_signal(barrier, inc=1, device_id=dev(peer_z, (r + dr) % n_col), device_id_type=MESH)

    @pl.when(jnp.logical_not(middle))
    def _():
        pl.semaphore_signal(barrier, inc=1, device_id=dev(zm, r), device_id_type=MESH)
        pl.semaphore_signal(barrier, inc=1, device_id=dev(zc, r_y), device_id_type=MESH)

    def load(src, h, slot):
        return pltpu.make_async_copy(src.at[out_rows(h), :], acc.at[slot], load_sem.at[slot])

    loads = (load(a_hbm, 1 - side, 0), load(g_hbm, 0, 1), load(g_hbm, 1, 2), load(a_hbm, side, 3))
    for copy in loads:
        copy.start()
    loads[0].wait()
    snd[0] = acc[0].astype(jnp.bfloat16)
    pl.semaphore_wait(barrier, jnp.where(middle, 2 * n_col, 2))

    @pl.when(middle)
    def _():
        remote(snd.at[0], a_quarter(zm), send_sem.at[3], ra.at[1], dev(zmo, r)).start()

    @pl.when(jnp.logical_not(middle))
    def _():
        @pl.loop(0, SUBS)
        def _(s):
            remote(snd.at[0, a_sub(s), :], snd.at[1, a_sub(s), :], send_sem.at[3], ra_relay.at[s], dev(zm, r)).start()

    for h in range(2):
        loads[1 + h].wait()
        g[z, pl.ds(pl.multiple_of(r * blk + h * half, half), half), :] = acc[1 + h].astype(jnp.bfloat16)

    @pl.when(jnp.logical_not(middle))
    def _():
        inner = dev(zm, r)

        @pl.loop(0, pieces)
        def _(j):
            copy_to(g_piece(z, r, j), send_sem.at[1], ry.at[0, j], dev(zc, r_y))

        loads[3].wait()
        a[:, quarter(z)] = acc[3].astype(jnp.bfloat16)
        remote(a_quarter(z), a_quarter(z), send_sem.at[3], ra.at[0], inner).start()

        @pl.loop(0, pieces)
        def _(j):
            copy_to(g_piece(z, r, j), send_sem.at[2], re.at[0, j], inner)

        @pl.loop(0, pieces)
        def _(j):
            wait_for(g_piece(z, r_y, j), ry.at[0, j])
            copy_to(g_piece(z, r_y, j), send_sem.at[2], re.at[1, j], inner)

        wait_sent(snd, send_sem.at[3])
        wait_sent(g_block(z, r), send_sem.at[1])
        wait_sent(g.at[0, pl.ds(0, 2 * blk), :], send_sem.at[2])

        for kind, h in ((1, side), (2, 1 - side)):
            @pl.loop(0, pieces)
            def _(j):
                wait_for(m_out.at[out_rows(h), cols(j)], fin_recv.at[kind, j])

        wait_for(s_out, sc_sem.at[1])

    @pl.when(middle)
    def _():
        other = dev(zmo, r)
        across = dev(zm, r_y)
        corner = dev(zc, r)
        me = side * n_col + r

        def peers():
            for dz in range(2):
                for dr in range(n_col):
                    if dz or dr:
                        yield (zmo if dz else zm), (r + dr) % n_col

        exchanges = [(ps_mid.at[0], ar_mid.at[0])]
        exchanges += [(ps_edge.at[j], ar_edge.at[j]) for j in range(pieces)]
        exchanges += [(ps_mid.at[1], ar_mid.at[1]), (ps_mid.at[2], ar_mid.at[2]), (ps, ar)]
        second_mid, second_edge, third = pieces + 1, pieces + 2, pieces + 3

        def sums_of(i):
            return exchanges[i]

        def send_sums(i):
            src, slots = sums_of(i)
            for pz, pr in peers():
                remote(src, slots.at[me], ar_send.at[i], ar_recv.at[i], dev(pz, pr)).start()
            slots[me] = src[...]

        def peer_slots(i):
            return sums_of(i)[1].at[pl.ds(0, 2 * n_col - 1)]

        def scales(i):
            src, slots = sums_of(i)
            wait_for(peer_slots(i), ar_recv.at[i])
            total = slots[0]
            for peer in range(1, 2 * n_col):
                total = total + slots[peer]
            return n / total

        def square(value, zq, span, slot):
            value = value * value
            acc[zq, :, span] = value
            slot[...] = jnp.sum(value, axis=0, keepdims=True)

        def expand(zq, j, slot):
            square(jnp.dot(a[...], g[zq, :, cols(j)], preferred_element_type=jnp.float32), zq, cols(j), slot)

        @pl.loop(0, pieces)
        def _(j):
            copy_to(g_piece(zm, r, j), send_sem.at[1], ry.at[0, j], across)
            send_partner(zm, r, j)

        loads[3].wait()
        a[:, quarter(zm)] = acc[3].astype(jnp.bfloat16)

        @pl.loop(0, SUBS)
        def _(s):
            wait_for(snd.at[1, a_sub(s), :], ra_relay.at[s])
            remote(snd.at[1, a_sub(s), :], a.at[a_sub(s), quarter(zc)], send_sem.at[3], ra.at[2], other).start()

        @pl.loop(0, pieces * SUBS)
        def _(i):
            copy_to(g_sub(zm, r, i // SUBS, i % SUBS), send_sem.at[0], rm.at[0, i // SUBS, i % SUBS], other)

        @pl.loop(0, pieces)
        def _(j):
            wait_for(g_piece(zm, r_y, j), ry.at[0, j])
            send_partner(zm, r_y, j)

        for idx, zq in ((1, zmo), (2, zco), (0, zc)):
            wait_for(a_quarter(zq), ra.at[idx])

        def finish_mid():
            scale = scales(0)
            for idx, zq in ((0, 1), (1, 2)):
                a1[:, pl.ds(zq * blk, blk)] = (acc[zq] * scale[idx]).astype(jnp.bfloat16)

        def finish_edge(j):
            scale = scales(1 + j)
            for idx, zq in ((0, 0), (1, 3)):
                a1[:, pl.ds(zq * blk + j * TILE, TILE)] = (
                    acc[zq, :, pl.ds(j * TILE, TILE)] * scale[idx]).astype(jnp.bfloat16)

        def partial(rows, zq, k0, k_len, n0, n_len):
            k = pl.ds(pl.multiple_of(k0, TILE), k_len)
            return jnp.dot(rows[:, k], g[zq, k, pl.ds(pl.multiple_of(n0, TILE), n_len)],
                           preferred_element_type=jnp.float32)

        def two_quarters(rows, zq, k_len, n0, *k_z):
            first, second = (partial(rows, zq, k * blk, k_len, n0, TILE) for k in k_z)
            return first + second

        def mid_by_mid(zq):
            @pl.loop(0, pieces)
            def _(j):
                acc[zq, :, cols(j)] = two_quarters(a1, zq, blk, j * TILE, 1, 2)

        def new_columns(j):
            @pl.loop(0, 2)
            def _(i):
                zq = 3 * i
                if j == pieces - 2:
                    pl.when(i == 1)(lambda: piece_across(2 * pieces - 1))
                acc[zq, :, pl.ds(j * TILE, TILE)] = (two_quarters(a1, zq, blk, j * TILE, 1, 2)
                                                     + two_quarters(a1, zq, (j + 1) * TILE, j * TILE, 0, 3))

        def last_new_columns(j):
            @pl.loop(0, 2)
            def _(i):
                zq = 3 * i
                fin[:, cols(i)] = (two_quarters(a1, zq, blk, j * TILE, 1, 2)
                                   + two_quarters(a1, zq, j * TILE, j * TILE, 0, 3))

        def piece_update(j, zq, n0, width):
            return partial(a1, zq, j * TILE, TILE, n0, width) + partial(a1, zq, 3 * blk + j * TILE, TILE, n0, width)

        def old_columns(j, zq, width, slot):
            span = pl.ds(0, width)
            total = acc[zq, :, span] + piece_update(j, zq, 0, width)
            if j == pieces - 1:
                square(total, zq, span, slot.at[:, span])
            else:
                acc[zq, :, span] = total

        def old_mid(j):
            @pl.loop(0, 2)
            def _(i):
                old_columns(j, 1 + i, blk, ps_mid.at[1, i])

        def old_edge(j):
            if j:
                @pl.loop(0, 2)
                def _(i):
                    old_columns(j, 3 * i, j * TILE, ps_mid.at[2, i])
            if j == pieces - 1:
                @pl.loop(0, 2)
                def _(i):
                    span = pl.ds(j * TILE, TILE)
                    square(fin[:, cols(i)] + piece_update(j, 3 * i, j * TILE, TILE), 3 * i, span, ps_mid.at[2, i, :, span])

        n_slices = pieces * SUBS

        def from_other(q):
            return zmo + (q // pieces) * (zco - zmo)

        def pump(i):
            q, s = i // SUBS, i % SUBS
            late, j = q // pieces, q % pieces
            z_m = from_other(q)
            ahead = i + AHEAD - n_slices

            @pl.when(jnp.logical_and(ahead >= 0, ahead < n_slices))
            def _():
                ref = g_sub(zc, r, ahead // SUBS, ahead % SUBS)
                copy_to(ref, send_sem.at[0], rm.at[1, ahead // SUBS, ahead % SUBS], other)

            ref = g_sub(z_m, r, j, s)
            wait_for(ref, rm.at[late, j, s])
            copy_to(ref, send_sem.at[1], ry.at[1 + late, j], across)

            @pl.when(s == SUBS - 1)
            def _():
                r_e = r + late * (r_y - r)
                send_partner(z_m, r, j)
                wait_for(g_piece(zc, r_e, j), re.at[late, j])
                send_partner(zc, r_e, j)

            @pl.when(jnp.logical_and(i >= LAG, (i - LAG) % SUBS == SUBS - 1))
            def _():
                piece_across((i - LAG) // SUBS)

        def piece_across(q):
            late, j = q // pieces, q % pieces
            wait_for(g_piece(from_other(q), r_y, j), ry.at[1 + late, j])
            send_partner(from_other(q), r_y, j)

        @pl.loop(0, pieces + 1)
        def _(q):
            @pl.loop(0, SUBS)
            def _(s):
                pump(q * SUBS + s)
                first = q == 0
                zq = jnp.where(first, zm, zmo)
                jq = jnp.where(first, s, q - 1)

                @pl.when(jnp.logical_or(first, s == SUBS - 1))
                def _():
                    wait_partner(zq, jq)
                    expand(zq, jq, ps_mid.at[0, zq - 1, :, cols(jq)])

        send_sums(0)

        def edge_step(j, tasks):
            @pl.loop(0, SUBS)
            def _(s):
                pump((pieces + 1 + j) * SUBS + s)

                @pl.when(s % 2 == 0)
                def _():
                    zq = jnp.where(s == 0, zc, zco)
                    wait_partner(zq, j)
                    expand(zq, j, ps_edge.at[j, zq // 3])

                @pl.when(s == 2)
                def _():
                    send_sums(1 + j)

                for at, task in tasks.items():
                    pl.when(s == at)(task)

        def mid_start():
            finish_mid()
            mid_by_mid(1)

        def edge_start(j):
            finish_edge(j)
            new_columns(j)

        def old(j):
            old_mid(j)
            old_edge(j)

        def first_piece():
            edge_start(0)
            old(0)

        edge_step(0, {3: mid_start})
        edge_step(1, {1: lambda: mid_by_mid(2), 3: first_piece})
        edge_step(2, {1: lambda: edge_start(1)})
        old(1)

        last = pieces - 1

        def last_piece(zq):
            wait_partner(zq, last)
            expand(zq, last, ps_edge.at[last, zq // 3])

        last_piece(zc)
        edge_start(last - 1)
        old_mid(last - 1)
        last_piece(zco)
        send_sums(pieces)
        old_edge(last - 1)
        last_new_columns(last)
        finish_edge(last)
        old_mid(last)
        send_sums(second_mid)
        old_edge(last)
        send_sums(second_edge)

        def finish_second(i, *quarters):
            scale = scales(i)
            for idx, zq in enumerate(quarters):
                a[:, quarter(zq)] = (acc[zq] * scale[idx]).astype(jnp.bfloat16)

        finish_second(second_mid, 1, 2)

        @pl.loop(0, 2)
        def _(i):
            acc[zm, :, cols(i)] = two_quarters(a, zc + i * (zco - zc), blk, 0, 1, 2)

        finish_second(second_edge, 0, 3)

        def send_result(i, zq, j):
            done = acc.at[zq, :, cols(j)]

            @pl.when(i == 0)
            def _():
                remote(done, m_out.at[out_rows(side), cols(j)], fin_send.at[1], fin_recv.at[1, j], corner).start()

            @pl.when(i == 1)
            def _():
                remote(done, fin.at[:, cols(j)], fin_send.at[0], fin_recv.at[2, j], other).start()

        @pl.loop(0, 2)
        def _(i):
            zq = zc + i * (zco - zc)
            square(acc[zm, :, cols(i)] + two_quarters(a, zq, blk, 0, 0, 3), zq, cols(0), ps.at[zq, :, cols(0)])
            send_result(i, zq, 0)

        @pl.loop(1, pieces)
        def _(j):
            @pl.loop(0, 2)
            def _(i):
                zq = zc + i * (zco - zc)
                expand(zq, j, ps.at[zq, :, cols(j)])
                send_result(i, zq, j)

        @pl.loop(0, 2 * pieces)
        def _(i):
            zq = zmo + (i // pieces) * (zm - zmo)
            j = i % pieces
            expand(zq, j, ps.at[zq, :, cols(j)])

        send_sums(third)
        remote(acc.at[zmo], m_out.at[out_rows(side), :], fin_send.at[2], fin_recv.at[0, 0], other).start()
        m_out[out_rows(side), :] = acc[zm]

        @pl.loop(0, pieces)
        def _(j):
            ref = fin.at[:, cols(j)]
            wait_for(ref, fin_recv.at[2, j])
            remote(ref, m_out.at[out_rows(1 - side), cols(j)], fin_send.at[3], fin_recv.at[2, j], corner).start()

        sc[...] = scales(third)
        remote(sc.at[zc], s_out, sc_sem.at[0], sc_sem.at[1], corner).start()
        s_out[...] = sc[zm]

        wait_sent(snd, send_sem.at[3])
        wait_sent(g.at[0, pl.ds(0, 2 * blk), :], send_sem.at[0])
        wait_sent(g.at[0, pl.ds(0, 3 * blk), :], send_sem.at[1])
        for zq in range(n_col):
            wait_sent(g.at[0, pl.ds(0, 2 * blk), :], send_sem.at[4 + zq])
        for i in range(len(exchanges)):
            wait_sent(peer_slots(i), ar_send.at[i])
        for i in range(4):
            wait_sent(acc.at[0], fin_send.at[i])
        wait_sent(sc.at[0], sc_sem.at[0])
        wait_for(m_out.at[out_rows(1 - side), :], fin_recv.at[0, 0])


def solution(mesh):
    num_cols = mesh.shape["col"]
    num_rows = mesh.shape["row"]
    block_spec = P(("graph", "row"), "col")

    def device_step(init_blk, graph_blk):
        blk = init_blk.shape[0]
        n = blk * num_rows
        half = blk // 2
        pieces = blk // TILE
        cores = 2 * num_rows
        any_spec = pl.BlockSpec(memory_space=pl.ANY)
        vmem_spec = pl.BlockSpec(memory_space=pltpu.VMEM)
        squares, scale = pl.pallas_call(
            mcl_kernel,
            out_shape=(pltpu.VMEM((blk, blk), jnp.float32), pltpu.VMEM((1, blk), jnp.float32)),
            in_specs=[any_spec, any_spec],
            out_specs=(vmem_spec, vmem_spec),
            scratch_shapes=[
                pltpu.VMEM((num_cols, n, blk), jnp.bfloat16),
                pltpu.VMEM((half, n), jnp.bfloat16),
                pltpu.VMEM((half, n), jnp.bfloat16),
                pltpu.VMEM((2, half, blk), jnp.bfloat16),
                pltpu.VMEM((num_cols, half, blk), jnp.float32),
                pltpu.VMEM((half, blk), jnp.float32),
                pltpu.VMEM((3, 2, 1, blk), jnp.float32),
                pltpu.VMEM((3, cores, 2, 1, blk), jnp.float32),
                pltpu.VMEM((pieces, 2, 1, TILE), jnp.float32),
                pltpu.VMEM((pieces, cores, 2, 1, TILE), jnp.float32),
                pltpu.VMEM((num_cols, 1, blk), jnp.float32),
                pltpu.VMEM((cores, num_cols, 1, blk), jnp.float32),
                pltpu.VMEM((num_cols, 1, blk), jnp.float32),
                pltpu.SemaphoreType.DMA((4,)),
                pltpu.SemaphoreType.DMA((2, pieces, SUBS)),
                pltpu.SemaphoreType.DMA((2, pieces)),
                pltpu.SemaphoreType.DMA((3, pieces)),
                pltpu.SemaphoreType.DMA((num_cols, pieces)),
                pltpu.SemaphoreType.DMA((SUBS,)),
                pltpu.SemaphoreType.DMA((3,)),
                pltpu.SemaphoreType.DMA((4 + num_cols,)),
                pltpu.SemaphoreType.DMA((4,)),
                pltpu.SemaphoreType.DMA((pieces + 4,)),
                pltpu.SemaphoreType.DMA((pieces + 4,)),
                pltpu.SemaphoreType.DMA((3, pieces)),
                pltpu.SemaphoreType.DMA((2,)),
            ],
            compiler_params=pltpu.CompilerParams(
                collective_id=0, has_side_effects=True, vmem_limit_bytes=60_000_000),
        )(init_blk, graph_blk)
        return squares * scale

    return jax.shard_map(device_step, mesh=mesh, in_specs=(block_spec, block_spec), out_specs=block_spec, check_vma=False)
```

```python
import jax
import jax.numpy as jnp
from jax import lax
from jax.experimental import pallas as pl
from jax.experimental.pallas import tpu as pltpu
from jax.sharding import PartitionSpec as P

SUBS = 8
TILE = 256
AHEAD = 6
LAG = 4
MESH = pl.DeviceIdType.MESH


def mcl_kernel(a_hbm, g_hbm, m_out, s_out, g, a, a1, snd, acc, fin, ps_mid, ar_mid, ps_edge, ar_edge, ps, ar, sc,
               load_sem, rm, re, ry, rp, ra_relay, ra, send_sem, fin_send, ar_send, ar_recv, fin_recv, sc_sem):
    n_col = g.shape[0]
    blk = g.shape[2]
    n = g.shape[1]
    half = blk // 2
    pieces = blk // TILE
    rows_s = blk // SUBS
    rows_a = half // SUBS
    turn = SUBS // 4

    z = lax.axis_index("col")
    r = lax.axis_index("row")
    y = r // 2
    c = r % 2
    side = z // 2
    middle = jnp.logical_or(z == 1, z == 2)
    zm = 1 + side
    zc = 3 * side
    zmo = 2 - side
    zco = 3 - 3 * side
    r_y = 2 * (1 - y) + c
    r_p = 2 * y + 1 - c

    def dev(zq, rq):
        return {"col": zq, "row": rq}

    def remote(src, dst, ssem, rsem, d):
        return pltpu.make_async_remote_copy(
            src_ref=src, dst_ref=dst, send_sem=ssem, recv_sem=rsem, device_id=d, device_id_type=MESH)

    def cols(j):
        return pl.ds(pl.multiple_of(j * TILE, TILE), TILE)

    def g_sub(zq, rq, j, s):
        return g.at[zq, pl.ds(pl.multiple_of(rq * blk + s * rows_s, rows_s), rows_s), cols(j)]

    def g_piece(zq, rq, j):
        return g.at[zq, pl.ds(pl.multiple_of(rq * blk, blk), blk), cols(j)]

    def g_block(zq, rq):
        return g.at[zq, pl.ds(pl.multiple_of(rq * blk, blk), blk), :]

    def copy_to(ref, ssem, rsem, d):
        remote(ref, ref, ssem, rsem, d).start()

    def wait_for(ref, rsem):
        remote(ref, ref, send_sem.at[0], rsem, dev(z, r)).wait_recv()

    def wait_sent(ref, ssem):
        remote(ref, ref, ssem, re.at[0, 0], dev(z, r)).wait_send()

    def send_partner(zq, rq, j):
        copy_to(g_piece(zq, rq, j), send_sem.at[4 + zq], rp.at[zq, j], dev(zm, r_p))

    def wait_partner(zq, j):
        wait_for(g.at[zq, pl.ds(0, 2 * blk), cols(j)], rp.at[zq, j])

    def quarter(zq):
        return pl.ds(pl.multiple_of(zq * blk, blk), blk)

    def a_quarter(zq):
        return a.at[:, quarter(zq)]

    def a_sub(s):
        return pl.ds(pl.multiple_of(s * rows_a, rows_a), rows_a)

    def out_rows(h):
        return pl.ds(pl.multiple_of(h * half, half), half)

    barrier = pltpu.get_barrier_semaphore()

    @pl.when(middle)
    def _():
        for dz in range(2):
            for dr in range(n_col):
                peer_z = zm if dz == 0 else zmo
                if dz == 0 and dr == 0:
                    peer_z = zc
                pl.semaphore_signal(barrier, inc=1, device_id=dev(peer_z, (r + dr) % n_col), device_id_type=MESH)

    @pl.when(jnp.logical_not(middle))
    def _():
        pl.semaphore_signal(barrier, inc=1, device_id=dev(zm, r), device_id_type=MESH)
        pl.semaphore_signal(barrier, inc=1, device_id=dev(zc, r_y), device_id_type=MESH)

    def load(src, h, slot):
        return pltpu.make_async_copy(src.at[out_rows(h), :], acc.at[slot], load_sem.at[slot])

    loads = (load(a_hbm, 1 - side, 0), load(g_hbm, 0, 1), load(g_hbm, 1, 2), load(a_hbm, side, 3))
    for copy in loads:
        copy.start()
    loads[0].wait()
    snd[0] = acc[0].astype(jnp.bfloat16)
    pl.semaphore_wait(barrier, jnp.where(middle, 2 * n_col, 2))

    @pl.when(middle)
    def _():
        remote(snd.at[0], a_quarter(zm), send_sem.at[3], ra.at[1], dev(zmo, r)).start()

    @pl.when(jnp.logical_not(middle))
    def _():
        @pl.loop(0, SUBS)
        def _(s):
            remote(snd.at[0, a_sub(s), :], snd.at[1, a_sub(s), :], send_sem.at[3], ra_relay.at[s], dev(zm, r)).start()

    for h in range(2):
        loads[1 + h].wait()
        g[z, pl.ds(pl.multiple_of(r * blk + h * half, half), half), :] = acc[1 + h].astype(jnp.bfloat16)

    @pl.when(jnp.logical_not(middle))
    def _():
        inner = dev(zm, r)

        @pl.loop(0, pieces)
        def _(j):
            copy_to(g_piece(z, r, j), send_sem.at[1], ry.at[0, j], dev(zc, r_y))

        loads[3].wait()
        a[:, quarter(z)] = acc[3].astype(jnp.bfloat16)
        remote(a_quarter(z), a_quarter(z), send_sem.at[3], ra.at[0], inner).start()

        @pl.loop(0, pieces)
        def _(j):
            copy_to(g_piece(z, r, j), send_sem.at[2], re.at[0, j], inner)

        @pl.loop(0, pieces)
        def _(j):
            wait_for(g_piece(z, r_y, j), ry.at[0, j])
            copy_to(g_piece(z, r_y, j), send_sem.at[2], re.at[1, j], inner)

        wait_sent(snd, send_sem.at[3])
        wait_sent(g_block(z, r), send_sem.at[1])
        wait_sent(g.at[0, pl.ds(0, 2 * blk), :], send_sem.at[2])

        for kind, h in ((1, side), (2, 1 - side)):
            @pl.loop(0, pieces)
            def _(j):
                wait_for(m_out.at[out_rows(h), cols(j)], fin_recv.at[kind, j])

        wait_for(s_out, sc_sem.at[1])

    @pl.when(middle)
    def _():
        other = dev(zmo, r)
        across = dev(zm, r_y)
        corner = dev(zc, r)
        me = side * n_col + r

        def peers():
            for dz in range(2):
                for dr in range(n_col):
                    if dz or dr:
                        yield (zmo if dz else zm), (r + dr) % n_col

        exchanges = [(ps_mid.at[0], ar_mid.at[0])]
        exchanges += [(ps_edge.at[j], ar_edge.at[j]) for j in range(pieces)]
        exchanges += [(ps_mid.at[1], ar_mid.at[1]), (ps_mid.at[2], ar_mid.at[2]), (ps, ar)]
        second_mid, second_edge, third = pieces + 1, pieces + 2, pieces + 3

        def sums_of(i):
            return exchanges[i]

        def send_sums(i):
            src, slots = sums_of(i)
            for pz, pr in peers():
                remote(src, slots.at[me], ar_send.at[i], ar_recv.at[i], dev(pz, pr)).start()
            slots[me] = src[...]

        def peer_slots(i):
            return sums_of(i)[1].at[pl.ds(0, 2 * n_col - 1)]

        def scales(i):
            src, slots = sums_of(i)
            wait_for(peer_slots(i), ar_recv.at[i])
            total = slots[0]
            for peer in range(1, 2 * n_col):
                total = total + slots[peer]
            return n / total

        def square(value, zq, span, slot):
            value = value * value
            acc[zq, :, span] = value
            slot[...] = jnp.sum(value, axis=0, keepdims=True)

        def expand(zq, j, slot):
            square(jnp.dot(a[...], g[zq, :, cols(j)], preferred_element_type=jnp.float32), zq, cols(j), slot)

        @pl.loop(0, pieces)
        def _(j):
            copy_to(g_piece(zm, r, j), send_sem.at[1], ry.at[0, j], across)
            send_partner(zm, r, j)

        loads[3].wait()
        a[:, quarter(zm)] = acc[3].astype(jnp.bfloat16)

        @pl.loop(0, SUBS)
        def _(s):
            wait_for(snd.at[1, a_sub(s), :], ra_relay.at[s])
            remote(snd.at[1, a_sub(s), :], a.at[a_sub(s), quarter(zc)], send_sem.at[3], ra.at[2], other).start()

        @pl.loop(0, pieces * SUBS)
        def _(i):
            copy_to(g_sub(zm, r, i // SUBS, i % SUBS), send_sem.at[0], rm.at[0, i // SUBS, i % SUBS], other)

        @pl.loop(0, pieces)
        def _(j):
            wait_for(g_piece(zm, r_y, j), ry.at[0, j])
            send_partner(zm, r_y, j)

        for idx, zq in ((1, zmo), (2, zco), (0, zc)):
            wait_for(a_quarter(zq), ra.at[idx])

        def finish_mid():
            scale = scales(0)
            for idx, zq in ((0, 1), (1, 2)):
                a1[:, pl.ds(zq * blk, blk)] = (acc[zq] * scale[idx]).astype(jnp.bfloat16)

        def finish_edge(j):
            scale = scales(1 + j)
            for idx, zq in ((0, 0), (1, 3)):
                a1[:, pl.ds(zq * blk + j * TILE, TILE)] = (
                    acc[zq, :, pl.ds(j * TILE, TILE)] * scale[idx]).astype(jnp.bfloat16)

        def partial(rows, zq, k0, k_len, n0, n_len):
            k = pl.ds(pl.multiple_of(k0, TILE), k_len)
            return jnp.dot(rows[:, k], g[zq, k, pl.ds(pl.multiple_of(n0, TILE), n_len)],
                           preferred_element_type=jnp.float32)

        def two_quarters(rows, zq, k_len, n0, *k_z):
            first, second = (partial(rows, zq, k * blk, k_len, n0, TILE) for k in k_z)
            return first + second

        def mid_by_mid(zq):
            @pl.loop(0, pieces)
            def _(j):
                acc[zq, :, cols(j)] = two_quarters(a1, zq, blk, j * TILE, 1, 2)

        def new_columns(j):
            @pl.loop(0, 2)
            def _(i):
                zq = 3 * i
                if j == pieces - 2:
                    pl.when(i == 1)(lambda: piece_across(2 * pieces - 1))
                acc[zq, :, pl.ds(j * TILE, TILE)] = (two_quarters(a1, zq, blk, j * TILE, 1, 2)
                                                     + two_quarters(a1, zq, (j + 1) * TILE, j * TILE, 0, 3))

        def last_new_columns(j):
            @pl.loop(0, 2)
            def _(i):
                zq = 3 * i
                fin[:, cols(i)] = (two_quarters(a1, zq, blk, j * TILE, 1, 2)
                                   + two_quarters(a1, zq, j * TILE, j * TILE, 0, 3))

        def piece_update(j, zq, n0, width):
            return partial(a1, zq, j * TILE, TILE, n0, width) + partial(a1, zq, 3 * blk + j * TILE, TILE, n0, width)

        def old_columns(j, zq, width, slot):
            span = pl.ds(0, width)
            total = acc[zq, :, span] + piece_update(j, zq, 0, width)
            if j == pieces - 1:
                square(total, zq, span, slot.at[:, span])
            else:
                acc[zq, :, span] = total

        def old_mid(j):
            @pl.loop(0, 2)
            def _(i):
                old_columns(j, 1 + i, blk, ps_mid.at[1, i])

        def old_edge(j):
            if j:
                @pl.loop(0, 2)
                def _(i):
                    old_columns(j, 3 * i, j * TILE, ps_mid.at[2, i])
            if j == pieces - 1:
                @pl.loop(0, 2)
                def _(i):
                    span = pl.ds(j * TILE, TILE)
                    square(fin[:, cols(i)] + piece_update(j, 3 * i, j * TILE, TILE), 3 * i, span, ps_mid.at[2, i, :, span])

        n_slices = pieces * SUBS

        def from_other(q):
            return zmo + (q // pieces) * (zco - zmo)

        def pump(i):
            q, s = i // SUBS, i % SUBS
            late, j = q // pieces, q % pieces
            z_m = from_other(q)
            ahead = i + AHEAD - n_slices

            @pl.when(jnp.logical_and(ahead >= 0, ahead < n_slices))
            def _():
                ref = g_sub(zc, r, ahead // SUBS, ahead % SUBS)
                copy_to(ref, send_sem.at[0], rm.at[1, ahead // SUBS, ahead % SUBS], other)

            ref = g_sub(z_m, r, j, s)
            wait_for(ref, rm.at[late, j, s])
            copy_to(ref, send_sem.at[1], ry.at[1 + late, j], across)

            @pl.when(s == SUBS - 1)
            def _():
                r_e = r + late * (r_y - r)
                send_partner(z_m, r, j)
                wait_for(g_piece(zc, r_e, j), re.at[late, j])
                send_partner(zc, r_e, j)

            @pl.when(jnp.logical_and(i >= LAG, (i - LAG) % SUBS == SUBS - 1))
            def _():
                piece_across((i - LAG) // SUBS)

        def piece_across(q):
            late, j = q // pieces, q % pieces
            wait_for(g_piece(from_other(q), r_y, j), ry.at[1 + late, j])
            send_partner(from_other(q), r_y, j)

        @pl.loop(0, pieces + 1)
        def _(q):
            @pl.loop(0, SUBS)
            def _(s):
                pump(q * SUBS + s)
                first = q == 0
                zq = jnp.where(first, zm, zmo)
                jq = jnp.where(first, s // turn, q - 1)

                @pl.when(jnp.logical_or(jnp.logical_and(first, s % turn == turn - 1), s == SUBS - 1))
                def _():
                    wait_partner(zq, jq)
                    expand(zq, jq, ps_mid.at[0, zq - 1, :, cols(jq)])

        send_sums(0)

        def edge_step(j, tasks):
            @pl.loop(0, SUBS)
            def _(s):
                pump((pieces + 1 + j) * SUBS + s)

                @pl.when(s % (2 * turn) == turn - 1)
                def _():
                    zq = jnp.where(s == turn - 1, zc, zco)
                    wait_partner(zq, j)
                    expand(zq, j, ps_edge.at[j, zq // 3])

                @pl.when(s == 3 * turn - 1)
                def _():
                    send_sums(1 + j)

                for at, task in tasks.items():
                    pl.when(s == (at + 1) * turn - 1)(task)

        def mid_start():
            finish_mid()
            mid_by_mid(1)

        def edge_start(j):
            finish_edge(j)
            new_columns(j)

        def old(j):
            old_mid(j)
            old_edge(j)

        def first_piece():
            edge_start(0)
            old(0)

        edge_step(0, {3: mid_start})
        edge_step(1, {1: lambda: mid_by_mid(2), 3: first_piece})
        edge_step(2, {1: lambda: edge_start(1)})
        old(1)

        last = pieces - 1

        def last_piece(zq):
            wait_partner(zq, last)
            expand(zq, last, ps_edge.at[last, zq // 3])

        last_piece(zc)
        edge_start(last - 1)
        old_mid(last - 1)
        last_piece(zco)
        send_sums(pieces)
        old_edge(last - 1)
        last_new_columns(last)
        finish_edge(last)
        old_mid(last)
        send_sums(second_mid)
        old_edge(last)
        send_sums(second_edge)

        def finish_second(i, *quarters):
            scale = scales(i)
            for idx, zq in enumerate(quarters):
                a[:, quarter(zq)] = (acc[zq] * scale[idx]).astype(jnp.bfloat16)

        finish_second(second_mid, 1, 2)

        @pl.loop(0, 2)
        def _(i):
            acc[zm, :, cols(i)] = two_quarters(a, zc + i * (zco - zc), blk, 0, 1, 2)

        finish_second(second_edge, 0, 3)

        def send_result(i, zq, j):
            done = acc.at[zq, :, cols(j)]

            @pl.when(i == 0)
            def _():
                remote(done, m_out.at[out_rows(side), cols(j)], fin_send.at[1], fin_recv.at[1, j], corner).start()

            @pl.when(i == 1)
            def _():
                remote(done, fin.at[:, cols(j)], fin_send.at[0], fin_recv.at[2, j], other).start()

        @pl.loop(0, 2)
        def _(i):
            zq = zc + i * (zco - zc)
            square(acc[zm, :, cols(i)] + two_quarters(a, zq, blk, 0, 0, 3), zq, cols(0), ps.at[zq, :, cols(0)])
            send_result(i, zq, 0)

        @pl.loop(1, pieces)
        def _(j):
            @pl.loop(0, 2)
            def _(i):
                zq = zc + i * (zco - zc)
                expand(zq, j, ps.at[zq, :, cols(j)])
                send_result(i, zq, j)

        @pl.loop(0, 2 * pieces)
        def _(i):
            zq = zmo + (i // pieces) * (zm - zmo)
            j = i % pieces
            expand(zq, j, ps.at[zq, :, cols(j)])

        send_sums(third)
        remote(acc.at[zmo], m_out.at[out_rows(side), :], fin_send.at[2], fin_recv.at[0, 0], other).start()
        m_out[out_rows(side), :] = acc[zm]

        @pl.loop(0, pieces)
        def _(j):
            ref = fin.at[:, cols(j)]
            wait_for(ref, fin_recv.at[2, j])
            remote(ref, m_out.at[out_rows(1 - side), cols(j)], fin_send.at[3], fin_recv.at[2, j], corner).start()

        sc[...] = scales(third)
        remote(sc.at[zc], s_out, sc_sem.at[0], sc_sem.at[1], corner).start()
        s_out[...] = sc[zm]

        wait_sent(snd, send_sem.at[3])
        wait_sent(g.at[0, pl.ds(0, 2 * blk), :], send_sem.at[0])
        wait_sent(g.at[0, pl.ds(0, 3 * blk), :], send_sem.at[1])
        for zq in range(n_col):
            wait_sent(g.at[0, pl.ds(0, 2 * blk), :], send_sem.at[4 + zq])
        for i in range(len(exchanges)):
            wait_sent(peer_slots(i), ar_send.at[i])
        for i in range(4):
            wait_sent(acc.at[0], fin_send.at[i])
        wait_sent(sc.at[0], sc_sem.at[0])
        wait_for(m_out.at[out_rows(1 - side), :], fin_recv.at[0, 0])


def solution(mesh):
    num_cols = mesh.shape["col"]
    num_rows = mesh.shape["row"]
    block_spec = P(("graph", "row"), "col")

    def device_step(init_blk, graph_blk):
        blk = init_blk.shape[0]
        n = blk * num_rows
        half = blk // 2
        pieces = blk // TILE
        cores = 2 * num_rows
        any_spec = pl.BlockSpec(memory_space=pl.ANY)
        vmem_spec = pl.BlockSpec(memory_space=pltpu.VMEM)
        squares, scale = pl.pallas_call(
            mcl_kernel,
            out_shape=(pltpu.VMEM((blk, blk), jnp.float32), pltpu.VMEM((1, blk), jnp.float32)),
            in_specs=[any_spec, any_spec],
            out_specs=(vmem_spec, vmem_spec),
            scratch_shapes=[
                pltpu.VMEM((num_cols, n, blk), jnp.bfloat16),
                pltpu.VMEM((half, n), jnp.bfloat16),
                pltpu.VMEM((half, n), jnp.bfloat16),
                pltpu.VMEM((2, half, blk), jnp.bfloat16),
                pltpu.VMEM((num_cols, half, blk), jnp.float32),
                pltpu.VMEM((half, blk), jnp.float32),
                pltpu.VMEM((3, 2, 1, blk), jnp.float32),
                pltpu.VMEM((3, cores, 2, 1, blk), jnp.float32),
                pltpu.VMEM((pieces, 2, 1, TILE), jnp.float32),
                pltpu.VMEM((pieces, cores, 2, 1, TILE), jnp.float32),
                pltpu.VMEM((num_cols, 1, blk), jnp.float32),
                pltpu.VMEM((cores, num_cols, 1, blk), jnp.float32),
                pltpu.VMEM((num_cols, 1, blk), jnp.float32),
                pltpu.SemaphoreType.DMA((4,)),
                pltpu.SemaphoreType.DMA((2, pieces, SUBS)),
                pltpu.SemaphoreType.DMA((2, pieces)),
                pltpu.SemaphoreType.DMA((3, pieces)),
                pltpu.SemaphoreType.DMA((num_cols, pieces)),
                pltpu.SemaphoreType.DMA((SUBS,)),
                pltpu.SemaphoreType.DMA((3,)),
                pltpu.SemaphoreType.DMA((4 + num_cols,)),
                pltpu.SemaphoreType.DMA((4,)),
                pltpu.SemaphoreType.DMA((pieces + 4,)),
                pltpu.SemaphoreType.DMA((pieces + 4,)),
                pltpu.SemaphoreType.DMA((3, pieces)),
                pltpu.SemaphoreType.DMA((2,)),
            ],
            compiler_params=pltpu.CompilerParams(
                collective_id=0, has_side_effects=True, vmem_limit_bytes=60_000_000),
        )(init_blk, graph_blk)
        return squares * scale

    return jax.shard_map(device_step, mesh=mesh, in_specs=(block_spec, block_spec), out_specs=block_spec, check_vma=False)
```

```python
import jax
import jax.numpy as jnp
from jax import lax
from jax.experimental import pallas as pl
from jax.experimental.pallas import tpu as pltpu
from jax.sharding import PartitionSpec as P

SUBS = 4
TILE = 256
AHEAD = 3
LAG = 2
MESH = pl.DeviceIdType.MESH


def mcl_kernel(a_hbm, g_hbm, m_out, s_out, g, a, a1, snd, acc, fin, ps_mid, ar_mid, ps_edge, ar_edge, ps, ar, sc,
               load_sem, rm, re, ry, rp, ra_relay, ra, send_sem, fin_send, ar_send, ar_recv, fin_recv, sc_sem):
    n_col = g.shape[0]
    blk = g.shape[2]
    n = g.shape[1]
    half = blk // 2
    pieces = blk // TILE
    rows_s = blk // SUBS
    rows_a = half // SUBS
    turn = SUBS // 4

    z = lax.axis_index("col")
    r = lax.axis_index("row")
    y = r // 2
    c = r % 2
    side = z // 2
    middle = jnp.logical_or(z == 1, z == 2)
    zm = 1 + side
    zc = 3 * side
    zmo = 2 - side
    zco = 3 - 3 * side
    r_y = 2 * (1 - y) + c
    r_p = 2 * y + 1 - c

    def dev(zq, rq):
        return {"col": zq, "row": rq}

    def remote(src, dst, ssem, rsem, d):
        return pltpu.make_async_remote_copy(
            src_ref=src, dst_ref=dst, send_sem=ssem, recv_sem=rsem, device_id=d, device_id_type=MESH)

    def cols(j):
        return pl.ds(pl.multiple_of(j * TILE, TILE), TILE)

    def g_sub(zq, rq, j, s):
        return g.at[zq, pl.ds(pl.multiple_of(rq * blk + s * rows_s, rows_s), rows_s), cols(j)]

    def g_piece(zq, rq, j):
        return g.at[zq, pl.ds(pl.multiple_of(rq * blk, blk), blk), cols(j)]

    def g_block(zq, rq):
        return g.at[zq, pl.ds(pl.multiple_of(rq * blk, blk), blk), :]

    def copy_to(ref, ssem, rsem, d):
        remote(ref, ref, ssem, rsem, d).start()

    def wait_for(ref, rsem):
        remote(ref, ref, send_sem.at[0], rsem, dev(z, r)).wait_recv()

    def wait_sent(ref, ssem):
        remote(ref, ref, ssem, re.at[0, 0], dev(z, r)).wait_send()

    def send_partner(zq, rq, j):
        copy_to(g_piece(zq, rq, j), send_sem.at[4 + zq], rp.at[zq, j], dev(zm, r_p))

    def wait_partner(zq, j):
        wait_for(g.at[zq, pl.ds(0, 2 * blk), cols(j)], rp.at[zq, j])

    def quarter(zq):
        return pl.ds(pl.multiple_of(zq * blk, blk), blk)

    def a_quarter(zq):
        return a.at[:, quarter(zq)]

    def a_sub(s):
        return pl.ds(pl.multiple_of(s * rows_a, rows_a), rows_a)

    def out_rows(h):
        return pl.ds(pl.multiple_of(h * half, half), half)

    barrier = pltpu.get_barrier_semaphore()

    @pl.when(middle)
    def _():
        for dz in range(2):
            for dr in range(n_col):
                peer_z = zm if dz == 0 else zmo
                if dz == 0 and dr == 0:
                    peer_z = zc
                pl.semaphore_signal(barrier, inc=1, device_id=dev(peer_z, (r + dr) % n_col), device_id_type=MESH)

    @pl.when(jnp.logical_not(middle))
    def _():
        pl.semaphore_signal(barrier, inc=1, device_id=dev(zm, r), device_id_type=MESH)
        pl.semaphore_signal(barrier, inc=1, device_id=dev(zc, r_y), device_id_type=MESH)

    def load(src, h, slot):
        return pltpu.make_async_copy(src.at[out_rows(h), :], acc.at[slot], load_sem.at[slot])

    loads = (load(a_hbm, 1 - side, 0), load(g_hbm, 0, 1), load(g_hbm, 1, 2), load(a_hbm, side, 3))
    loads[0].start()
    loads[0].wait()
    for copy in loads[1:]:
        copy.start()
    snd[0] = acc[0].astype(jnp.bfloat16)
    pl.semaphore_wait(barrier, jnp.where(middle, 2 * n_col, 2))

    @pl.when(middle)
    def _():
        remote(snd.at[0], a_quarter(zm), send_sem.at[3], ra.at[1], dev(zmo, r)).start()

    @pl.when(jnp.logical_not(middle))
    def _():
        @pl.loop(0, SUBS)
        def _(s):
            remote(snd.at[0, a_sub(s), :], snd.at[1, a_sub(s), :], send_sem.at[3], ra_relay.at[s], dev(zm, r)).start()

    for h in range(2):
        loads[1 + h].wait()
        g[z, pl.ds(pl.multiple_of(r * blk + h * half, half), half), :] = acc[1 + h].astype(jnp.bfloat16)

    @pl.when(jnp.logical_not(middle))
    def _():
        inner = dev(zm, r)

        @pl.loop(0, pieces)
        def _(j):
            copy_to(g_piece(z, r, j), send_sem.at[1], ry.at[0, j], dev(zc, r_y))

        loads[3].wait()
        a[:, quarter(z)] = acc[3].astype(jnp.bfloat16)
        remote(a_quarter(z), a_quarter(z), send_sem.at[3], ra.at[0], inner).start()

        @pl.loop(0, pieces)
        def _(j):
            copy_to(g_piece(z, r, j), send_sem.at[2], re.at[0, j], inner)

        @pl.loop(0, pieces)
        def _(j):
            wait_for(g_piece(z, r_y, j), ry.at[0, j])
            copy_to(g_piece(z, r_y, j), send_sem.at[2], re.at[1, j], inner)

        wait_sent(snd, send_sem.at[3])
        wait_sent(g_block(z, r), send_sem.at[1])
        wait_sent(g.at[0, pl.ds(0, 2 * blk), :], send_sem.at[2])

        for kind, h in ((1, side), (2, 1 - side)):
            @pl.loop(0, pieces)
            def _(j):
                wait_for(m_out.at[out_rows(h), cols(j)], fin_recv.at[kind, j])

        wait_for(s_out, sc_sem.at[1])

    @pl.when(middle)
    def _():
        other = dev(zmo, r)
        across = dev(zm, r_y)
        corner = dev(zc, r)
        me = side * n_col + r

        def peers():
            for dz in range(2):
                for dr in range(n_col):
                    if dz or dr:
                        yield (zmo if dz else zm), (r + dr) % n_col

        exchanges = [(ps_mid.at[0], ar_mid.at[0])]
        exchanges += [(ps_edge.at[j], ar_edge.at[j]) for j in range(pieces)]
        exchanges += [(ps_mid.at[1], ar_mid.at[1]), (ps_mid.at[2], ar_mid.at[2]), (ps, ar)]
        second_mid, second_edge, third = pieces + 1, pieces + 2, pieces + 3

        def sums_of(i):
            return exchanges[i]

        def send_sums(i):
            src, slots = sums_of(i)
            for pz, pr in peers():
                remote(src, slots.at[me], ar_send.at[i], ar_recv.at[i], dev(pz, pr)).start()
            slots[me] = src[...]

        def peer_slots(i):
            return sums_of(i)[1].at[pl.ds(0, 2 * n_col - 1)]

        def scales(i):
            src, slots = sums_of(i)
            wait_for(peer_slots(i), ar_recv.at[i])
            total = slots[0]
            for peer in range(1, 2 * n_col):
                total = total + slots[peer]
            return n / total

        def square(value, zq, span, slot, keep=None):
            value = value * value
            if keep is None:
                acc[zq, :, span] = value
            else:
                fin[:, keep] = value
            slot[...] = jnp.sum(value, axis=0, keepdims=True)

        def expand(zq, j, slot, keep=None):
            square(jnp.dot(a[...], g[zq, :, cols(j)], preferred_element_type=jnp.float32), zq, cols(j), slot, keep)

        @pl.loop(0, pieces)
        def _(j):
            copy_to(g_piece(zm, r, j), send_sem.at[1], ry.at[0, j], across)
            send_partner(zm, r, j)

        loads[3].wait()
        a[:, quarter(zm)] = acc[3].astype(jnp.bfloat16)

        @pl.loop(0, SUBS)
        def _(s):
            wait_for(snd.at[1, a_sub(s), :], ra_relay.at[s])
            remote(snd.at[1, a_sub(s), :], a.at[a_sub(s), quarter(zc)], send_sem.at[3], ra.at[2], other).start()

        @pl.loop(0, pieces * SUBS)
        def _(i):
            copy_to(g_sub(zm, r, i // SUBS, i % SUBS), send_sem.at[0], rm.at[0, i // SUBS, i % SUBS], other)

        @pl.loop(0, pieces)
        def _(j):
            wait_for(g_piece(zm, r_y, j), ry.at[0, j])
            send_partner(zm, r_y, j)

        for idx, zq in ((1, zmo), (2, zco), (0, zc)):
            wait_for(a_quarter(zq), ra.at[idx])

        def finish_mid():
            scale = scales(0)
            for idx, zq in ((0, 1), (1, 2)):
                a1[:, pl.ds(zq * blk, blk)] = (acc[zq] * scale[idx]).astype(jnp.bfloat16)

        def finish_edge(j):
            scale = scales(1 + j)
            for idx, zq in ((0, 0), (1, 3)):
                kept = fin[:, cols(idx)] if j == pieces - 1 else acc[zq, :, pl.ds(j * TILE, TILE)]
                a1[:, pl.ds(zq * blk + j * TILE, TILE)] = (kept * scale[idx]).astype(jnp.bfloat16)

        def partial(rows, zq, k0, k_len, n0, n_len):
            k = pl.ds(pl.multiple_of(k0, TILE), k_len)
            return jnp.dot(rows[:, k], g[zq, k, pl.ds(pl.multiple_of(n0, TILE), n_len)],
                           preferred_element_type=jnp.float32)

        def two_quarters(rows, zq, k_len, n0, *k_z):
            first, second = (partial(rows, zq, k * blk, k_len, n0, TILE) for k in k_z)
            return first + second

        def mid_by_mid(zq):
            @pl.loop(0, pieces)
            def _(j):
                acc[zq, :, cols(j)] = two_quarters(a1, zq, blk, j * TILE, 1, 2)

        def new_columns(j):
            @pl.loop(0, 2)
            def _(i):
                zq = 3 * i
                if j == pieces - 2:
                    pl.when(i == 1)(lambda: piece_across(2 * pieces - 1))
                acc[zq, :, pl.ds(j * TILE, TILE)] = (two_quarters(a1, zq, blk, j * TILE, 1, 2)
                                                     + two_quarters(a1, zq, (j + 1) * TILE, j * TILE, 0, 3))

        def last_new_columns(j):
            @pl.loop(0, 2)
            def _(i):
                zq = 3 * i
                acc[zq, :, cols(j)] = (two_quarters(a1, zq, blk, j * TILE, 1, 2)
                                   + two_quarters(a1, zq, j * TILE, j * TILE, 0, 3))

        def piece_update(j, zq, n0, width):
            return partial(a1, zq, j * TILE, TILE, n0, width) + partial(a1, zq, 3 * blk + j * TILE, TILE, n0, width)

        def old_columns(j, zq, width, slot):
            span = pl.ds(0, width)
            total = acc[zq, :, span] + piece_update(j, zq, 0, width)
            if j == pieces - 1:
                square(total, zq, span, slot.at[:, span])
            else:
                acc[zq, :, span] = total

        def old_mid(j):
            @pl.loop(0, 2)
            def _(i):
                old_columns(j, 1 + i, blk, ps_mid.at[1, i])

        def old_edge(j):
            if j:
                @pl.loop(0, 2)
                def _(i):
                    old_columns(j, 3 * i, blk if j == pieces - 1 else j * TILE, ps_mid.at[2, i])

        n_slices = pieces * SUBS

        def from_other(q):
            return zmo + (q // pieces) * (zco - zmo)

        def relay_ahead(i):
            ahead = i + AHEAD - n_slices

            @pl.when(jnp.logical_and(ahead >= 0, ahead < n_slices))
            def _():
                ref = g_sub(zc, r, ahead // SUBS, ahead % SUBS)
                copy_to(ref, send_sem.at[0], rm.at[1, ahead // SUBS, ahead % SUBS], other)

        def pump(i):
            q, s = i // SUBS, i % SUBS
            late, j = q // pieces, q % pieces
            z_m = from_other(q)
            ref = g_sub(z_m, r, j, s)
            wait_for(ref, rm.at[late, j, s])
            copy_to(ref, send_sem.at[1], ry.at[1 + late, j], across)

            @pl.when(s == SUBS - 1)
            def _():
                r_e = r + late * (r_y - r)
                send_partner(z_m, r, j)
                wait_for(g_piece(zc, r_e, j), re.at[late, j])
                send_partner(zc, r_e, j)

            @pl.when(jnp.logical_and(i >= LAG, (i - LAG) % SUBS == SUBS - 1))
            def _():
                piece_across((i - LAG) // SUBS)

        def piece_across(q):
            late, j = q // pieces, q % pieces
            wait_for(g_piece(from_other(q), r_y, j), ry.at[1 + late, j])
            send_partner(from_other(q), r_y, j)

        @pl.loop(0, pieces + 1)
        def _(q):
            @pl.loop(0, SUBS)
            def _(s):
                relay_ahead(q * SUBS + s)
                pump(q * SUBS + s)
                first = q == 0
                zq = jnp.where(first, zm, zmo)
                jq = jnp.where(first, s // turn, q - 1)

                @pl.when(jnp.logical_or(jnp.logical_and(first, s % turn == turn - 1), s == SUBS - 1))
                def _():
                    wait_partner(zq, jq)
                    expand(zq, jq, ps_mid.at[0, zq - 1, :, cols(jq)])

        send_sums(0)

        def edge_step(j, tasks):
            @pl.loop(0, SUBS)
            def _(s):
                i = (pieces + 1 + j) * SUBS + s
                pl.when(s != 3 * turn - 1)(lambda: relay_ahead(i))
                pump(i)

                @pl.when(s % (2 * turn) == turn - 1)
                def _():
                    zq = jnp.where(s == turn - 1, zc, zco)
                    wait_partner(zq, j)
                    expand(zq, j, ps_edge.at[j, zq // 3])

                @pl.when(s == 3 * turn - 1)
                def _():
                    send_sums(1 + j)
                    relay_ahead(i)

                for at, task in tasks.items():
                    pl.when(s == (at + 1) * turn - 1)(task)

        def mid_start():
            finish_mid()
            mid_by_mid(1)

        def edge_start(j):
            finish_edge(j)
            new_columns(j)

        def old(j):
            old_mid(j)
            old_edge(j)

        def first_piece():
            edge_start(0)
            old(0)

        edge_step(0, {3: mid_start})
        edge_step(1, {1: lambda: mid_by_mid(2), 3: first_piece})
        edge_step(2, {1: lambda: edge_start(1)})
        old(1)

        last = pieces - 1

        def last_piece(zq):
            wait_partner(zq, last)
            expand(zq, last, ps_edge.at[last, zq // 3], cols(zq // 3))

        last_piece(zc)
        edge_start(last - 1)
        old_mid(last - 1)
        last_piece(zco)
        send_sums(pieces)
        old_edge(last - 1)
        last_new_columns(last)
        finish_edge(last)
        old_mid(last)
        send_sums(second_mid)
        old_edge(last)
        send_sums(second_edge)

        def finish_second(i, *quarters):
            scale = scales(i)
            for idx, zq in enumerate(quarters):
                a[:, quarter(zq)] = (acc[zq] * scale[idx]).astype(jnp.bfloat16)

        finish_second(second_mid, 1, 2)

        @pl.loop(0, 2)
        def _(i):
            acc[zm, :, cols(i)] = two_quarters(a, zc + i * (zco - zc), blk, 0, 1, 2)

        finish_second(second_edge, 0, 3)

        def send_result(i, zq, j):
            done = acc.at[zq, :, cols(j)]

            @pl.when(i == 0)
            def _():
                remote(done, m_out.at[out_rows(side), cols(j)], fin_send.at[1], fin_recv.at[1, j], corner).start()

            @pl.when(i == 1)
            def _():
                remote(done, fin.at[:, cols(j)], fin_send.at[0], fin_recv.at[2, j], other).start()

        @pl.loop(0, 2)
        def _(i):
            zq = zc + i * (zco - zc)
            square(acc[zm, :, cols(i)] + two_quarters(a, zq, blk, 0, 0, 3), zq, cols(0), ps.at[zq, :, cols(0)])
            send_result(i, zq, 0)

        @pl.loop(1, pieces)
        def _(j):
            @pl.loop(0, 2)
            def _(i):
                zq = zc + i * (zco - zc)
                expand(zq, j, ps.at[zq, :, cols(j)])
                send_result(i, zq, j)

        @pl.loop(0, 2 * pieces)
        def _(i):
            zq = zmo + (i // pieces) * (zm - zmo)
            j = i % pieces
            expand(zq, j, ps.at[zq, :, cols(j)])

        send_sums(third)
        remote(acc.at[zmo], m_out.at[out_rows(side), :], fin_send.at[2], fin_recv.at[0, 0], other).start()
        m_out[out_rows(side), :] = acc[zm]

        @pl.loop(0, pieces)
        def _(j):
            ref = fin.at[:, cols(j)]
            wait_for(ref, fin_recv.at[2, j])
            remote(ref, m_out.at[out_rows(1 - side), cols(j)], fin_send.at[3], fin_recv.at[2, j], corner).start()

        sc[...] = scales(third)
        remote(sc.at[zc], s_out, sc_sem.at[0], sc_sem.at[1], corner).start()
        s_out[...] = sc[zm]

        wait_sent(snd, send_sem.at[3])
        wait_sent(g.at[0, pl.ds(0, 2 * blk), :], send_sem.at[0])
        wait_sent(g.at[0, pl.ds(0, 3 * blk), :], send_sem.at[1])
        for zq in range(n_col):
            wait_sent(g.at[0, pl.ds(0, 2 * blk), :], send_sem.at[4 + zq])
        for i in range(len(exchanges)):
            wait_sent(peer_slots(i), ar_send.at[i])
        for i in range(4):
            wait_sent(acc.at[0], fin_send.at[i])
        wait_sent(sc.at[0], sc_sem.at[0])
        wait_for(m_out.at[out_rows(1 - side), :], fin_recv.at[0, 0])


def solution(mesh):
    num_cols = mesh.shape["col"]
    num_rows = mesh.shape["row"]
    block_spec = P(("graph", "row"), "col")

    def device_step(init_blk, graph_blk):
        blk = init_blk.shape[0]
        n = blk * num_rows
        half = blk // 2
        pieces = blk // TILE
        cores = 2 * num_rows
        any_spec = pl.BlockSpec(memory_space=pl.ANY)
        vmem_spec = pl.BlockSpec(memory_space=pltpu.VMEM)
        squares, scale = pl.pallas_call(
            mcl_kernel,
            out_shape=(pltpu.VMEM((blk, blk), jnp.float32), pltpu.VMEM((1, blk), jnp.float32)),
            in_specs=[any_spec, any_spec],
            out_specs=(vmem_spec, vmem_spec),
            scratch_shapes=[
                pltpu.VMEM((num_cols, n, blk), jnp.bfloat16),
                pltpu.VMEM((half, n), jnp.bfloat16),
                pltpu.VMEM((half, n), jnp.bfloat16),
                pltpu.VMEM((2, half, blk), jnp.bfloat16),
                pltpu.VMEM((num_cols, half, blk), jnp.float32),
                pltpu.VMEM((half, blk), jnp.float32),
                pltpu.VMEM((3, 2, 1, blk), jnp.float32),
                pltpu.VMEM((3, cores, 2, 1, blk), jnp.float32),
                pltpu.VMEM((pieces, 2, 1, TILE), jnp.float32),
                pltpu.VMEM((pieces, cores, 2, 1, TILE), jnp.float32),
                pltpu.VMEM((num_cols, 1, blk), jnp.float32),
                pltpu.VMEM((cores, num_cols, 1, blk), jnp.float32),
                pltpu.VMEM((num_cols, 1, blk), jnp.float32),
                pltpu.SemaphoreType.DMA((4,)),
                pltpu.SemaphoreType.DMA((2, pieces, SUBS)),
                pltpu.SemaphoreType.DMA((2, pieces)),
                pltpu.SemaphoreType.DMA((3, pieces)),
                pltpu.SemaphoreType.DMA((num_cols, pieces)),
                pltpu.SemaphoreType.DMA((SUBS,)),
                pltpu.SemaphoreType.DMA((3,)),
                pltpu.SemaphoreType.DMA((4 + num_cols,)),
                pltpu.SemaphoreType.DMA((4,)),
                pltpu.SemaphoreType.DMA((pieces + 4,)),
                pltpu.SemaphoreType.DMA((pieces + 4,)),
                pltpu.SemaphoreType.DMA((3, pieces)),
                pltpu.SemaphoreType.DMA((2,)),
            ],
            compiler_params=pltpu.CompilerParams(
                collective_id=0, has_side_effects=True, vmem_limit_bytes=60_000_000),
        )(init_blk, graph_blk)
        return squares * scale

    return jax.shard_map(device_step, mesh=mesh, in_specs=(block_spec, block_spec), out_specs=block_spec, check_vma=False)
```

```python
import jax
import jax.numpy as jnp
from jax import lax
from jax.experimental import pallas as pl
from jax.experimental.pallas import tpu as pltpu
from jax.sharding import PartitionSpec as P

SUBS = 4
TILE = 256
AHEAD = 3
LAG = 2
MESH = pl.DeviceIdType.MESH


def mcl_kernel(a_hbm, g_hbm, m_out, s_out, g, a, a1, snd, acc, fin, ps_mid, ar_mid, ps_edge, ar_edge, ps, ar, sc,
               load_sem, rm, re, ry, rp, ra_relay, ra, send_sem, fin_send, ar_send, ar_recv, fin_recv, sc_sem):
    n_col = g.shape[0]
    blk = g.shape[2]
    n = g.shape[1]
    half = blk // 2
    pieces = blk // TILE
    rows_s = blk // SUBS
    rows_a = half // SUBS
    turn = SUBS // 4

    z = lax.axis_index("col")
    r = lax.axis_index("row")
    y = r // 2
    c = r % 2
    side = z // 2
    middle = jnp.logical_or(z == 1, z == 2)
    zm = 1 + side
    zc = 3 * side
    zmo = 2 - side
    zco = 3 - 3 * side
    r_y = 2 * (1 - y) + c
    r_p = 2 * y + 1 - c

    def dev(zq, rq):
        return {"col": zq, "row": rq}

    def remote(src, dst, ssem, rsem, d):
        return pltpu.make_async_remote_copy(
            src_ref=src, dst_ref=dst, send_sem=ssem, recv_sem=rsem, device_id=d, device_id_type=MESH)

    def cols(j):
        return pl.ds(pl.multiple_of(j * TILE, TILE), TILE)

    def g_sub(zq, rq, j, s):
        return g.at[zq, pl.ds(pl.multiple_of(rq * blk + s * rows_s, rows_s), rows_s), cols(j)]

    def g_piece(zq, rq, j):
        return g.at[zq, pl.ds(pl.multiple_of(rq * blk, blk), blk), cols(j)]

    def g_block(zq, rq):
        return g.at[zq, pl.ds(pl.multiple_of(rq * blk, blk), blk), :]

    def copy_to(ref, ssem, rsem, d):
        remote(ref, ref, ssem, rsem, d).start()

    def wait_for(ref, rsem):
        remote(ref, ref, send_sem.at[0], rsem, dev(z, r)).wait_recv()

    def wait_sent(ref, ssem):
        remote(ref, ref, ssem, re.at[0, 0], dev(z, r)).wait_send()

    def send_partner(zq, rq, j):
        copy_to(g_piece(zq, rq, j), send_sem.at[4 + zq], rp.at[zq, j], dev(zm, r_p))

    def wait_partner(zq, j):
        wait_for(g.at[zq, pl.ds(0, 2 * blk), cols(j)], rp.at[zq, j])

    def quarter(zq):
        return pl.ds(pl.multiple_of(zq * blk, blk), blk)

    def a_quarter(zq):
        return a.at[:, quarter(zq)]

    def a_sub(s):
        return pl.ds(pl.multiple_of(s * rows_a, rows_a), rows_a)

    def out_rows(h):
        return pl.ds(pl.multiple_of(h * half, half), half)

    barrier = pltpu.get_barrier_semaphore()

    @pl.when(middle)
    def _():
        for dz in range(2):
            for dr in range(n_col):
                peer_z = zm if dz == 0 else zmo
                if dz == 0 and dr == 0:
                    peer_z = zc
                pl.semaphore_signal(barrier, inc=1, device_id=dev(peer_z, (r + dr) % n_col), device_id_type=MESH)

    @pl.when(jnp.logical_not(middle))
    def _():
        pl.semaphore_signal(barrier, inc=1, device_id=dev(zm, r), device_id_type=MESH)
        pl.semaphore_signal(barrier, inc=1, device_id=dev(zc, r_y), device_id_type=MESH)

    def load(src, h, slot):
        return pltpu.make_async_copy(src.at[out_rows(h), :], acc.at[slot], load_sem.at[slot])

    loads = (load(a_hbm, 1 - side, 0), load(g_hbm, 0, 1), load(g_hbm, 1, 2), load(a_hbm, side, 3))
    for copy in loads:
        copy.start()
    loads[0].wait()
    snd[0] = acc[0].astype(jnp.bfloat16)
    pl.semaphore_wait(barrier, jnp.where(middle, 2 * n_col, 2))

    @pl.when(middle)
    def _():
        remote(snd.at[0], a_quarter(zm), send_sem.at[3], ra.at[1], dev(zmo, r)).start()

    @pl.when(jnp.logical_not(middle))
    def _():
        @pl.loop(0, SUBS)
        def _(s):
            remote(snd.at[0, a_sub(s), :], snd.at[1, a_sub(s), :], send_sem.at[3], ra_relay.at[s], dev(zm, r)).start()

    for h in range(2):
        loads[1 + h].wait()
        g[z, pl.ds(pl.multiple_of(r * blk + h * half, half), half), :] = acc[1 + h].astype(jnp.bfloat16)

    @pl.when(jnp.logical_not(middle))
    def _():
        inner = dev(zm, r)

        @pl.loop(0, pieces)
        def _(j):
            copy_to(g_piece(z, r, j), send_sem.at[1], ry.at[0, j], dev(zc, r_y))

        loads[3].wait()
        a[:, quarter(z)] = acc[3].astype(jnp.bfloat16)
        remote(a_quarter(z), a_quarter(z), send_sem.at[3], ra.at[0], inner).start()

        @pl.loop(0, pieces)
        def _(j):
            copy_to(g_piece(z, r, j), send_sem.at[2], re.at[0, j], inner)

        @pl.loop(0, pieces)
        def _(j):
            wait_for(g_piece(z, r_y, j), ry.at[0, j])
            copy_to(g_piece(z, r_y, j), send_sem.at[2], re.at[1, j], inner)

        wait_sent(snd, send_sem.at[3])
        wait_sent(g_block(z, r), send_sem.at[1])
        wait_sent(g.at[0, pl.ds(0, 2 * blk), :], send_sem.at[2])

        for kind, h in ((1, side), (2, 1 - side)):
            @pl.loop(0, pieces)
            def _(j):
                wait_for(m_out.at[out_rows(h), cols(j)], fin_recv.at[kind, j])

        wait_for(s_out, sc_sem.at[1])

    @pl.when(middle)
    def _():
        other = dev(zmo, r)
        across = dev(zm, r_y)
        corner = dev(zc, r)
        me = side * n_col + r

        def peers():
            for dz in range(2):
                for dr in range(n_col):
                    if dz or dr:
                        yield dz == 0, (zmo if dz else zm), (r + dr) % n_col

        exchanges = [(ps_mid.at[0], ar_mid.at[0])]
        exchanges += [(ps_edge.at[j], ar_edge.at[j]) for j in range(pieces)]
        exchanges += [(ps_mid.at[1], ar_mid.at[1]), (ps_mid.at[2], ar_mid.at[2]), (ps, ar)]
        second_mid, second_edge, third = pieces + 1, pieces + 2, pieces + 3

        def sums_of(i):
            return exchanges[i]

        def send_sums(i):
            src, slots = sums_of(i)
            for same, pz, pr in peers():
                part = src.at[side if same else 1 - side] if i == third else src
                remote(part, slots.at[me], ar_send.at[i], ar_recv.at[i], dev(pz, pr)).start()
            slots[me] = src[side] if i == third else src[...]

        def peer_slots(i):
            return sums_of(i)[1].at[pl.ds(0, 2 * n_col - 1)]

        def scales(i):
            src, slots = sums_of(i)
            wait_for(peer_slots(i), ar_recv.at[i])
            total = slots[0]
            for peer in range(1, 2 * n_col):
                total = total + slots[peer]
            return n / total

        def square(value, zq, span, slot, keep=None):
            value = value * value
            if keep is None:
                acc[zq, :, span] = value
            else:
                fin[:, keep] = value
            slot[...] = jnp.sum(value, axis=0, keepdims=True)

        def expand(zq, j, slot, keep=None):
            square(jnp.dot(a[...], g[zq, :, cols(j)], preferred_element_type=jnp.float32), zq, cols(j), slot, keep)

        @pl.loop(0, pieces)
        def _(j):
            copy_to(g_piece(zm, r, j), send_sem.at[1], ry.at[0, j], across)
            send_partner(zm, r, j)

        loads[3].wait()
        a[:, quarter(zm)] = acc[3].astype(jnp.bfloat16)

        @pl.loop(0, SUBS)
        def _(s):
            wait_for(snd.at[1, a_sub(s), :], ra_relay.at[s])
            remote(snd.at[1, a_sub(s), :], a.at[a_sub(s), quarter(zc)], send_sem.at[3], ra.at[2], other).start()

        @pl.loop(0, pieces * SUBS)
        def _(i):
            copy_to(g_sub(zm, r, i // SUBS, i % SUBS), send_sem.at[0], rm.at[0, i // SUBS, i % SUBS], other)

        @pl.loop(0, pieces)
        def _(j):
            wait_for(g_piece(zm, r_y, j), ry.at[0, j])
            send_partner(zm, r_y, j)

        for idx, zq in ((1, zmo), (2, zco), (0, zc)):
            wait_for(a_quarter(zq), ra.at[idx])

        def finish_mid():
            scale = scales(0)
            for idx, zq in ((0, 1), (1, 2)):
                a1[:, pl.ds(zq * blk, blk)] = (acc[zq] * scale[idx]).astype(jnp.bfloat16)

        def finish_edge(j):
            scale = scales(1 + j)
            for idx, zq in ((0, 0), (1, 3)):
                kept = fin[:, cols(idx)] if j == pieces - 1 else acc[zq, :, pl.ds(j * TILE, TILE)]
                a1[:, pl.ds(zq * blk + j * TILE, TILE)] = (kept * scale[idx]).astype(jnp.bfloat16)

        def partial(rows, zq, k0, k_len, n0, n_len):
            k = pl.ds(pl.multiple_of(k0, TILE), k_len)
            return jnp.dot(rows[:, k], g[zq, k, pl.ds(pl.multiple_of(n0, TILE), n_len)],
                           preferred_element_type=jnp.float32)

        def two_quarters(rows, zq, k_len, n0, *k_z):
            first, second = (partial(rows, zq, k * blk, k_len, n0, TILE) for k in k_z)
            return first + second

        def mid_by_mid(zq):
            @pl.loop(0, pieces)
            def _(j):
                acc[zq, :, cols(j)] = two_quarters(a1, zq, blk, j * TILE, 1, 2)

        def new_columns(j):
            @pl.loop(0, 2)
            def _(i):
                zq = 3 * i
                acc[zq, :, pl.ds(j * TILE, TILE)] = (two_quarters(a1, zq, blk, j * TILE, 1, 2)
                                                     + two_quarters(a1, zq, (j + 1) * TILE, j * TILE, 0, 3))

        def last_new_columns(j):
            @pl.loop(0, 2)
            def _(i):
                zq = 3 * i
                acc[zq, :, cols(j)] = (two_quarters(a1, zq, blk, j * TILE, 1, 2)
                                   + two_quarters(a1, zq, j * TILE, j * TILE, 0, 3))

        def piece_update(j, zq, n0, width):
            return partial(a1, zq, j * TILE, TILE, n0, width) + partial(a1, zq, 3 * blk + j * TILE, TILE, n0, width)

        def old_columns(j, zq, width, slot):
            span = pl.ds(0, width)
            total = acc[zq, :, span] + piece_update(j, zq, 0, width)
            if j == pieces - 1:
                square(total, zq, span, slot.at[:, span])
            else:
                acc[zq, :, span] = total

        def old_mid(j):
            @pl.loop(0, 2)
            def _(i):
                old_columns(j, 1 + i, blk, ps_mid.at[1, i])

        def old_edge(j):
            if j:
                @pl.loop(0, 2)
                def _(i):
                    old_columns(j, 3 * i, blk if j == pieces - 1 else j * TILE, ps_mid.at[2, i])

        n_slices = pieces * SUBS

        def from_other(q):
            return zmo + (q // pieces) * (zco - zmo)

        def relay_ahead(i):
            ahead = i + AHEAD - n_slices

            @pl.when(jnp.logical_and(ahead >= 0, ahead < n_slices))
            def _():
                ref = g_sub(zc, r, ahead // SUBS, ahead % SUBS)
                copy_to(ref, send_sem.at[0], rm.at[1, ahead // SUBS, ahead % SUBS], other)

        def pump(i):
            q, s = i // SUBS, i % SUBS
            late, j = q // pieces, q % pieces
            z_m = from_other(q)
            ref = g_sub(z_m, r, j, s)
            wait_for(ref, rm.at[late, j, s])
            copy_to(ref, send_sem.at[1], ry.at[1 + late, j], across)

            @pl.when(s == SUBS - 1)
            def _():
                r_e = r + late * (r_y - r)
                send_partner(z_m, r, j)
                wait_for(g_piece(zc, r_e, j), re.at[late, j])
                send_partner(zc, r_e, j)

            @pl.when(jnp.logical_and(i >= LAG, (i - LAG) % SUBS == SUBS - 1))
            def _():
                piece_across((i - LAG) // SUBS)

        def piece_across(q):
            late, j = q // pieces, q % pieces
            wait_for(g_piece(from_other(q), r_y, j), ry.at[1 + late, j])
            send_partner(from_other(q), r_y, j)

        @pl.loop(0, pieces + 1)
        def _(q):
            @pl.loop(0, SUBS)
            def _(s):
                relay_ahead(q * SUBS + s)
                pump(q * SUBS + s)
                first = q == 0
                zq = jnp.where(first, zm, zmo)
                jq = jnp.where(first, s // turn, q - 1)

                @pl.when(jnp.logical_or(jnp.logical_and(first, s % turn == turn - 1), s == SUBS - 1))
                def _():
                    wait_partner(zq, jq)
                    expand(zq, jq, ps_mid.at[0, zq - 1, :, cols(jq)])

        send_sums(0)

        def edge_step(j, tasks):
            @pl.loop(0, SUBS)
            def _(s):
                i = (pieces + 1 + j) * SUBS + s
                pl.when(s != 3 * turn - 1)(lambda: relay_ahead(i))
                pump(i)

                @pl.when(s % (2 * turn) == turn - 1)
                def _():
                    zq = jnp.where(s == turn - 1, zc, zco)
                    wait_partner(zq, j)
                    expand(zq, j, ps_edge.at[j, zq // 3])

                @pl.when(s == 3 * turn - 1)
                def _():
                    send_sums(1 + j)
                    relay_ahead(i)

                for at, task in tasks.items():
                    pl.when(s == (at + 1) * turn - 1)(task)

        def mid_start():
            finish_mid()
            mid_by_mid(1)

        def edge_start(j):
            finish_edge(j)
            new_columns(j)

        def old(j):
            old_mid(j)
            old_edge(j)

        def first_piece():
            edge_start(0)
            old(0)

        edge_step(0, {3: mid_start})
        edge_step(1, {1: lambda: mid_by_mid(2), 3: first_piece})
        edge_step(2, {1: lambda: edge_start(1)})
        old(1)

        last = pieces - 1

        def last_piece(zq):
            wait_partner(zq, last)
            expand(zq, last, ps_edge.at[last, zq // 3], cols(zq // 3))

        last_piece(zc)
        edge_start(last - 1)
        piece_across(2 * pieces - 1)
        old_mid(last - 1)
        last_piece(zco)
        send_sums(pieces)
        old_edge(last - 1)
        last_new_columns(last)
        finish_edge(last)
        old_mid(last)
        send_sums(second_mid)
        old_edge(last)
        send_sums(second_edge)

        def finish_second(i, *quarters):
            scale = scales(i)
            for idx, zq in enumerate(quarters):
                a[:, quarter(zq)] = (acc[zq] * scale[idx]).astype(jnp.bfloat16)

        finish_second(second_mid, 1, 2)

        @pl.loop(0, 2)
        def _(i):
            acc[zm, :, cols(i)] = two_quarters(a, zc + i * (zco - zc), blk, 0, 1, 2)

        finish_second(second_edge, 0, 3)

        def last_sums(zq, j):
            return ps.at[zq // 2, jnp.where(zq % 3 == 0, 1, 0), :, cols(j)]

        def send_result(i, zq, j):
            done = acc.at[zq, :, cols(j)]

            @pl.when(i == 0)
            def _():
                remote(done, m_out.at[out_rows(side), cols(j)], fin_send.at[1], fin_recv.at[1, j], corner).start()

            @pl.when(i == 1)
            def _():
                remote(done, fin.at[:, cols(j)], fin_send.at[0], fin_recv.at[2, j], other).start()

        @pl.loop(0, 2)
        def _(i):
            zq = zc + i * (zco - zc)
            square(acc[zm, :, cols(i)] + two_quarters(a, zq, blk, 0, 0, 3), zq, cols(0), last_sums(zq, 0))
            send_result(i, zq, 0)

        @pl.loop(1, pieces)
        def _(j):
            @pl.loop(0, 2)
            def _(i):
                zq = zc + i * (zco - zc)
                expand(zq, j, last_sums(zq, j))
                send_result(i, zq, j)

        @pl.loop(0, 2 * pieces)
        def _(i):
            zq = zmo + (i // pieces) * (zm - zmo)
            j = i % pieces
            expand(zq, j, last_sums(zq, j))

        send_sums(third)
        remote(acc.at[zmo], m_out.at[out_rows(side), :], fin_send.at[2], fin_recv.at[0, 0], other).start()
        m_out[out_rows(side), :] = acc[zm]

        @pl.loop(0, pieces)
        def _(j):
            ref = fin.at[:, cols(j)]
            wait_for(ref, fin_recv.at[2, j])
            remote(ref, m_out.at[out_rows(1 - side), cols(j)], fin_send.at[3], fin_recv.at[2, j], corner).start()

        sc[...] = scales(third)
        remote(sc.at[1], s_out, sc_sem.at[0], sc_sem.at[1], corner).start()
        s_out[...] = sc[0]

        wait_sent(snd, send_sem.at[3])
        wait_sent(g.at[0, pl.ds(0, 2 * blk), :], send_sem.at[0])
        wait_sent(g.at[0, pl.ds(0, 3 * blk), :], send_sem.at[1])
        for zq in range(n_col):
            wait_sent(g.at[0, pl.ds(0, 2 * blk), :], send_sem.at[4 + zq])
        for i in range(len(exchanges)):
            wait_sent(peer_slots(i), ar_send.at[i])
        for i in range(4):
            wait_sent(acc.at[0], fin_send.at[i])
        wait_sent(sc.at[0], sc_sem.at[0])
        wait_for(m_out.at[out_rows(1 - side), :], fin_recv.at[0, 0])


def solution(mesh):
    num_cols = mesh.shape["col"]
    num_rows = mesh.shape["row"]
    block_spec = P(("graph", "row"), "col")

    def device_step(init_blk, graph_blk):
        blk = init_blk.shape[0]
        n = blk * num_rows
        half = blk // 2
        pieces = blk // TILE
        cores = 2 * num_rows
        any_spec = pl.BlockSpec(memory_space=pl.ANY)
        vmem_spec = pl.BlockSpec(memory_space=pltpu.VMEM)
        squares, scale = pl.pallas_call(
            mcl_kernel,
            out_shape=(pltpu.VMEM((blk, blk), jnp.float32), pltpu.VMEM((1, blk), jnp.float32)),
            in_specs=[any_spec, any_spec],
            out_specs=(vmem_spec, vmem_spec),
            scratch_shapes=[
                pltpu.VMEM((num_cols, n, blk), jnp.bfloat16),
                pltpu.VMEM((half, n), jnp.bfloat16),
                pltpu.VMEM((half, n), jnp.bfloat16),
                pltpu.VMEM((2, half, blk), jnp.bfloat16),
                pltpu.VMEM((num_cols, half, blk), jnp.float32),
                pltpu.VMEM((half, blk), jnp.float32),
                pltpu.VMEM((3, 2, 1, blk), jnp.float32),
                pltpu.VMEM((3, cores, 2, 1, blk), jnp.float32),
                pltpu.VMEM((pieces, 2, 1, TILE), jnp.float32),
                pltpu.VMEM((pieces, cores, 2, 1, TILE), jnp.float32),
                pltpu.VMEM((2, 2, 1, blk), jnp.float32),
                pltpu.VMEM((cores, 2, 1, blk), jnp.float32),
                pltpu.VMEM((2, 1, blk), jnp.float32),
                pltpu.SemaphoreType.DMA((4,)),
                pltpu.SemaphoreType.DMA((2, pieces, SUBS)),
                pltpu.SemaphoreType.DMA((2, pieces)),
                pltpu.SemaphoreType.DMA((3, pieces)),
                pltpu.SemaphoreType.DMA((num_cols, pieces)),
                pltpu.SemaphoreType.DMA((SUBS,)),
                pltpu.SemaphoreType.DMA((3,)),
                pltpu.SemaphoreType.DMA((4 + num_cols,)),
                pltpu.SemaphoreType.DMA((4,)),
                pltpu.SemaphoreType.DMA((pieces + 4,)),
                pltpu.SemaphoreType.DMA((pieces + 4,)),
                pltpu.SemaphoreType.DMA((3, pieces)),
                pltpu.SemaphoreType.DMA((2,)),
            ],
            compiler_params=pltpu.CompilerParams(
                collective_id=0, has_side_effects=True, vmem_limit_bytes=60_000_000),
        )(init_blk, graph_blk)
        return squares * scale

    return jax.shard_map(device_step, mesh=mesh, in_specs=(block_spec, block_spec), out_specs=block_spec, check_vma=False)
```

```python
import jax
import jax.numpy as jnp
from jax import lax
from jax.experimental import pallas as pl
from jax.experimental.pallas import tpu as pltpu
from jax.sharding import PartitionSpec as P

SUBS = 4
TILE = 256
AHEAD = 3
LAG = 2
MESH = pl.DeviceIdType.MESH


def mcl_kernel(a_hbm, g_hbm, out, g, a, a1, snd, acc, fin, ps_mid, ar_mid, ps_edge, ar_edge, ps, ar, sc,
               load_sem, rm, re, ry, rp, ra_relay, ra, send_sem, fin_send, ar_send, ar_recv, fin_recv, sc_sem):
    n_col = g.shape[0]
    blk = g.shape[2]
    n = g.shape[1]
    half = blk // 2
    pieces = blk // TILE
    rows_s = blk // SUBS
    rows_a = half // SUBS
    turn = SUBS // 4

    z = lax.axis_index("col")
    r = lax.axis_index("row")
    y = r // 2
    c = r % 2
    side = z // 2
    middle = jnp.logical_or(z == 1, z == 2)
    zm = 1 + side
    zc = 3 * side
    zmo = 2 - side
    zco = 3 - 3 * side
    r_y = 2 * (1 - y) + c
    r_p = 2 * y + 1 - c

    def dev(zq, rq):
        return {"col": zq, "row": rq}

    def remote(src, dst, ssem, rsem, d):
        return pltpu.make_async_remote_copy(
            src_ref=src, dst_ref=dst, send_sem=ssem, recv_sem=rsem, device_id=d, device_id_type=MESH)

    def cols(j):
        return pl.ds(pl.multiple_of(j * TILE, TILE), TILE)

    def g_sub(zq, rq, j, s):
        return g.at[zq, pl.ds(pl.multiple_of(rq * blk + s * rows_s, rows_s), rows_s), cols(j)]

    def g_piece(zq, rq, j):
        return g.at[zq, pl.ds(pl.multiple_of(rq * blk, blk), blk), cols(j)]

    def g_block(zq, rq):
        return g.at[zq, pl.ds(pl.multiple_of(rq * blk, blk), blk), :]

    def copy_to(ref, ssem, rsem, d):
        remote(ref, ref, ssem, rsem, d).start()

    def wait_for(ref, rsem):
        remote(ref, ref, send_sem.at[0], rsem, dev(z, r)).wait_recv()

    def wait_sent(ref, ssem):
        remote(ref, ref, ssem, re.at[0, 0], dev(z, r)).wait_send()

    def send_partner(zq, rq, j):
        copy_to(g_piece(zq, rq, j), send_sem.at[4 + zq], rp.at[zq, j], dev(zm, r_p))

    def wait_partner(zq, j):
        wait_for(g.at[zq, pl.ds(0, 2 * blk), cols(j)], rp.at[zq, j])

    def quarter(zq):
        return pl.ds(pl.multiple_of(zq * blk, blk), blk)

    def a_quarter(zq):
        return a.at[:, quarter(zq)]

    def a_sub(s):
        return pl.ds(pl.multiple_of(s * rows_a, rows_a), rows_a)

    def out_rows(h):
        return pl.ds(pl.multiple_of(h * half, half), half)

    barrier = pltpu.get_barrier_semaphore()

    @pl.when(middle)
    def _():
        for dz in range(2):
            for dr in range(n_col):
                peer_z = zm if dz == 0 else zmo
                if dz == 0 and dr == 0:
                    peer_z = zc
                pl.semaphore_signal(barrier, inc=1, device_id=dev(peer_z, (r + dr) % n_col), device_id_type=MESH)

    @pl.when(jnp.logical_not(middle))
    def _():
        pl.semaphore_signal(barrier, inc=1, device_id=dev(zm, r), device_id_type=MESH)
        pl.semaphore_signal(barrier, inc=1, device_id=dev(zc, r_y), device_id_type=MESH)

    def load(src, h, slot):
        return pltpu.make_async_copy(src.at[out_rows(h), :], acc.at[slot], load_sem.at[slot])

    loads = (load(a_hbm, 1 - side, 0), load(g_hbm, 0, 1), load(g_hbm, 1, 2), load(a_hbm, side, 3))
    for copy in loads:
        copy.start()
    loads[0].wait()
    snd[0] = acc[0].astype(jnp.bfloat16)
    pl.semaphore_wait(barrier, jnp.where(middle, 2 * n_col, 2))

    @pl.when(middle)
    def _():
        remote(snd.at[0], a_quarter(zm), send_sem.at[3], ra.at[1], dev(zmo, r)).start()

    @pl.when(jnp.logical_not(middle))
    def _():
        @pl.loop(0, SUBS)
        def _(s):
            remote(snd.at[0, a_sub(s), :], snd.at[1, a_sub(s), :], send_sem.at[3], ra_relay.at[s], dev(zm, r)).start()

    for h in range(2):
        loads[1 + h].wait()
        g[z, pl.ds(pl.multiple_of(r * blk + h * half, half), half), :] = acc[1 + h].astype(jnp.bfloat16)

    def receive(kind, h, j, scale):
        wait_for(out.at[out_rows(h), cols(j)], fin_recv.at[kind, j])
        out[out_rows(h), cols(j)] = out[out_rows(h), cols(j)] * scale

    @pl.when(jnp.logical_not(middle))
    def _():
        inner = dev(zm, r)

        @pl.loop(0, pieces)
        def _(j):
            copy_to(g_piece(z, r, j), send_sem.at[1], ry.at[0, j], dev(zc, r_y))

        loads[3].wait()
        a[:, quarter(z)] = acc[3].astype(jnp.bfloat16)
        remote(a_quarter(z), a_quarter(z), send_sem.at[3], ra.at[0], inner).start()

        @pl.loop(0, pieces)
        def _(j):
            copy_to(g_piece(z, r, j), send_sem.at[2], re.at[0, j], inner)

        @pl.loop(0, pieces)
        def _(j):
            wait_for(g_piece(z, r_y, j), ry.at[0, j])
            copy_to(g_piece(z, r_y, j), send_sem.at[2], re.at[1, j], inner)

        wait_sent(snd, send_sem.at[3])
        wait_sent(g_block(z, r), send_sem.at[1])
        wait_sent(g.at[0, pl.ds(0, 2 * blk), :], send_sem.at[2])

        wait_for(sc.at[1], sc_sem.at[1])
        for kind, h in ((1, side), (2, 1 - side)):
            @pl.loop(0, pieces)
            def _(j):
                receive(kind, h, j, sc[1, :, cols(j)])

    @pl.when(middle)
    def _():
        other = dev(zmo, r)
        across = dev(zm, r_y)
        corner = dev(zc, r)
        me = side * n_col + r

        def peers():
            for dz in range(2):
                for dr in range(n_col):
                    if dz or dr:
                        yield dz == 0, (zmo if dz else zm), (r + dr) % n_col

        exchanges = [(ps_mid.at[0], ar_mid.at[0])]
        exchanges += [(ps_edge.at[j], ar_edge.at[j]) for j in range(pieces)]
        exchanges += [(ps_mid.at[1], ar_mid.at[1]), (ps_mid.at[2], ar_mid.at[2]), (ps, ar)]
        second_mid, second_edge, third = pieces + 1, pieces + 2, pieces + 3

        def sums_of(i):
            return exchanges[i]

        def send_sums(i):
            src, slots = sums_of(i)
            for same, pz, pr in peers():
                part = src.at[side if same else 1 - side] if i == third else src
                remote(part, slots.at[me], ar_send.at[i], ar_recv.at[i], dev(pz, pr)).start()
            slots[me] = src[side] if i == third else src[...]

        def peer_slots(i):
            return sums_of(i)[1].at[pl.ds(0, 2 * n_col - 1)]

        def scales(i):
            src, slots = sums_of(i)
            wait_for(peer_slots(i), ar_recv.at[i])
            total = slots[0]
            for peer in range(1, 2 * n_col):
                total = total + slots[peer]
            return n / total

        def square(value, zq, span, slot, keep=None):
            value = value * value
            if keep is None:
                acc[zq, :, span] = value
            else:
                fin[:, keep] = value
            slot[...] = jnp.sum(value, axis=0, keepdims=True)

        def expand(zq, j, slot, keep=None):
            square(jnp.dot(a[...], g[zq, :, cols(j)], preferred_element_type=jnp.float32), zq, cols(j), slot, keep)

        @pl.loop(0, pieces)
        def _(j):
            copy_to(g_piece(zm, r, j), send_sem.at[1], ry.at[0, j], across)
            send_partner(zm, r, j)

        loads[3].wait()
        a[:, quarter(zm)] = acc[3].astype(jnp.bfloat16)

        @pl.loop(0, SUBS)
        def _(s):
            wait_for(snd.at[1, a_sub(s), :], ra_relay.at[s])
            remote(snd.at[1, a_sub(s), :], a.at[a_sub(s), quarter(zc)], send_sem.at[3], ra.at[2], other).start()

        @pl.loop(0, pieces * SUBS)
        def _(i):
            copy_to(g_sub(zm, r, i // SUBS, i % SUBS), send_sem.at[0], rm.at[0, i // SUBS, i % SUBS], other)

        @pl.loop(0, pieces)
        def _(j):
            wait_for(g_piece(zm, r_y, j), ry.at[0, j])
            send_partner(zm, r_y, j)

        for idx, zq in ((1, zmo), (2, zco), (0, zc)):
            wait_for(a_quarter(zq), ra.at[idx])

        def finish_mid():
            scale = scales(0)
            for idx, zq in ((0, 1), (1, 2)):
                a1[:, pl.ds(zq * blk, blk)] = (acc[zq] * scale[idx]).astype(jnp.bfloat16)

        def finish_edge(j):
            scale = scales(1 + j)
            for idx, zq in ((0, 0), (1, 3)):
                kept = fin[:, cols(idx)] if j == pieces - 1 else acc[zq, :, pl.ds(j * TILE, TILE)]
                a1[:, pl.ds(zq * blk + j * TILE, TILE)] = (kept * scale[idx]).astype(jnp.bfloat16)

        def partial(rows, zq, k0, k_len, n0, n_len):
            k = pl.ds(pl.multiple_of(k0, TILE), k_len)
            return jnp.dot(rows[:, k], g[zq, k, pl.ds(pl.multiple_of(n0, TILE), n_len)],
                           preferred_element_type=jnp.float32)

        def two_quarters(rows, zq, k_len, n0, *k_z):
            first, second = (partial(rows, zq, k * blk, k_len, n0, TILE) for k in k_z)
            return first + second

        def mid_by_mid(zq):
            @pl.loop(0, pieces)
            def _(j):
                acc[zq, :, cols(j)] = two_quarters(a1, zq, blk, j * TILE, 1, 2)

        def new_columns(j):
            @pl.loop(0, 2)
            def _(i):
                zq = 3 * i
                acc[zq, :, pl.ds(j * TILE, TILE)] = (two_quarters(a1, zq, blk, j * TILE, 1, 2)
                                                     + two_quarters(a1, zq, (j + 1) * TILE, j * TILE, 0, 3))

        def last_new_columns(j):
            @pl.loop(0, 2)
            def _(i):
                zq = 3 * i
                acc[zq, :, cols(j)] = (two_quarters(a1, zq, blk, j * TILE, 1, 2)
                                   + two_quarters(a1, zq, j * TILE, j * TILE, 0, 3))

        def piece_update(j, zq, n0, width):
            return partial(a1, zq, j * TILE, TILE, n0, width) + partial(a1, zq, 3 * blk + j * TILE, TILE, n0, width)

        def old_columns(j, zq, width, slot):
            span = pl.ds(0, width)
            total = acc[zq, :, span] + piece_update(j, zq, 0, width)
            if j == pieces - 1:
                square(total, zq, span, slot.at[:, span])
            else:
                acc[zq, :, span] = total

        def old_mid(j):
            @pl.loop(0, 2)
            def _(i):
                old_columns(j, 1 + i, blk, ps_mid.at[1, i])

        def old_edge(j):
            if j:
                @pl.loop(0, 2)
                def _(i):
                    old_columns(j, 3 * i, blk if j == pieces - 1 else j * TILE, ps_mid.at[2, i])

        n_slices = pieces * SUBS

        def from_other(q):
            return zmo + (q // pieces) * (zco - zmo)

        def relay_ahead(i):
            ahead = i + AHEAD - n_slices

            @pl.when(jnp.logical_and(ahead >= 0, ahead < n_slices))
            def _():
                ref = g_sub(zc, r, ahead // SUBS, ahead % SUBS)
                copy_to(ref, send_sem.at[0], rm.at[1, ahead // SUBS, ahead % SUBS], other)

        def pump(i):
            q, s = i // SUBS, i % SUBS
            late, j = q // pieces, q % pieces
            z_m = from_other(q)
            ref = g_sub(z_m, r, j, s)
            wait_for(ref, rm.at[late, j, s])
            copy_to(ref, send_sem.at[1], ry.at[1 + late, j], across)

            @pl.when(s == SUBS - 1)
            def _():
                r_e = r + late * (r_y - r)
                send_partner(z_m, r, j)
                wait_for(g_piece(zc, r_e, j), re.at[late, j])
                send_partner(zc, r_e, j)

            @pl.when(jnp.logical_and(i >= LAG, (i - LAG) % SUBS == SUBS - 1))
            def _():
                piece_across((i - LAG) // SUBS)

        def piece_across(q):
            late, j = q // pieces, q % pieces
            wait_for(g_piece(from_other(q), r_y, j), ry.at[1 + late, j])
            send_partner(from_other(q), r_y, j)

        @pl.loop(0, pieces + 1)
        def _(q):
            @pl.loop(0, SUBS)
            def _(s):
                relay_ahead(q * SUBS + s)
                pump(q * SUBS + s)
                first = q == 0
                zq = jnp.where(first, zm, zmo)
                jq = jnp.where(first, s // turn, q - 1)

                @pl.when(jnp.logical_or(jnp.logical_and(first, s % turn == turn - 1), s == SUBS - 1))
                def _():
                    wait_partner(zq, jq)
                    expand(zq, jq, ps_mid.at[0, zq - 1, :, cols(jq)])

        send_sums(0)

        def edge_step(j, tasks):
            @pl.loop(0, SUBS)
            def _(s):
                i = (pieces + 1 + j) * SUBS + s
                pl.when(s != 3 * turn - 1)(lambda: relay_ahead(i))
                pump(i)

                @pl.when(s % (2 * turn) == turn - 1)
                def _():
                    zq = jnp.where(s == turn - 1, zc, zco)
                    wait_partner(zq, j)
                    expand(zq, j, ps_edge.at[j, zq // 3])

                @pl.when(s == 3 * turn - 1)
                def _():
                    send_sums(1 + j)
                    relay_ahead(i)

                for at, task in tasks.items():
                    pl.when(s == (at + 1) * turn - 1)(task)

        def mid_start():
            finish_mid()
            mid_by_mid(1)

        def edge_start(j):
            finish_edge(j)
            new_columns(j)

        def old(j):
            old_mid(j)
            old_edge(j)

        def first_piece():
            edge_start(0)
            old(0)

        edge_step(0, {3: mid_start})
        edge_step(1, {1: lambda: mid_by_mid(2), 3: first_piece})
        edge_step(2, {1: lambda: edge_start(1), 2: lambda: old_edge(1)})
        old_mid(1)

        last = pieces - 1

        def last_piece(zq):
            wait_partner(zq, last)
            expand(zq, last, ps_edge.at[last, zq // 3], cols(zq // 3))

        last_piece(zc)
        edge_start(last - 1)
        piece_across(2 * pieces - 1)
        old_mid(last - 1)
        last_piece(zco)
        send_sums(pieces)
        old_edge(last - 1)
        last_new_columns(last)
        finish_edge(last)
        old_mid(last)
        send_sums(second_mid)
        old_edge(last)
        send_sums(second_edge)

        def finish_second(i, *quarters):
            scale = scales(i)
            for idx, zq in enumerate(quarters):
                a[:, quarter(zq)] = (acc[zq] * scale[idx]).astype(jnp.bfloat16)

        finish_second(second_mid, 1, 2)

        @pl.loop(0, 2)
        def _(i):
            acc[zm, :, cols(i)] = two_quarters(a, zc + i * (zco - zc), blk, 0, 1, 2)

        finish_second(second_edge, 0, 3)

        def last_sums(zq, j):
            return ps.at[zq // 2, jnp.where(zq % 3 == 0, 1, 0), :, cols(j)]

        def send_result(i, zq, j):
            done = acc.at[zq, :, cols(j)]

            @pl.when(i == 0)
            def _():
                remote(done, out.at[out_rows(side), cols(j)], fin_send.at[1], fin_recv.at[1, j], corner).start()

            @pl.when(i == 1)
            def _():
                remote(done, fin.at[:, cols(j)], fin_send.at[0], fin_recv.at[2, j], other).start()

        @pl.loop(0, 2)
        def _(i):
            zq = zc + i * (zco - zc)
            square(acc[zm, :, cols(i)] + two_quarters(a, zq, blk, 0, 0, 3), zq, cols(0), last_sums(zq, 0))
            send_result(i, zq, 0)

        @pl.loop(1, pieces)
        def _(j):
            @pl.loop(0, 2)
            def _(i):
                zq = zc + i * (zco - zc)
                expand(zq, j, last_sums(zq, j))
                send_result(i, zq, j)

        @pl.loop(0, 2 * pieces)
        def _(i):
            zq = zmo + (i // pieces) * (zm - zmo)
            j = i % pieces
            expand(zq, j, last_sums(zq, j))

        send_sums(third)

        @pl.loop(0, pieces)
        def _(j):
            remote(acc.at[zmo, :, cols(j)], out.at[out_rows(side), cols(j)], fin_send.at[2], fin_recv.at[0, j],
                   other).start()

        @pl.loop(0, pieces)
        def _(j):
            ref = fin.at[:, cols(j)]
            wait_for(ref, fin_recv.at[2, j])
            remote(ref, out.at[out_rows(1 - side), cols(j)], fin_send.at[3], fin_recv.at[2, j], corner).start()

        sc[...] = scales(third)
        remote(sc.at[1], sc.at[1], sc_sem.at[0], sc_sem.at[1], corner).start()
        out[out_rows(side), :] = acc[zm] * sc[0]

        wait_sent(snd, send_sem.at[3])
        wait_sent(g.at[0, pl.ds(0, 2 * blk), :], send_sem.at[0])
        wait_sent(g.at[0, pl.ds(0, 3 * blk), :], send_sem.at[1])
        for zq in range(n_col):
            wait_sent(g.at[0, pl.ds(0, 2 * blk), :], send_sem.at[4 + zq])
        for i in range(len(exchanges)):
            wait_sent(peer_slots(i), ar_send.at[i])
        for i in range(4):
            wait_sent(acc.at[0], fin_send.at[i])
        wait_sent(sc.at[0], sc_sem.at[0])

        @pl.loop(0, pieces)
        def _(j):
            receive(0, 1 - side, j, sc[0, :, cols(j)])


def solution(mesh):
    num_cols = mesh.shape["col"]
    num_rows = mesh.shape["row"]
    block_spec = P(("graph", "row"), "col")

    def device_step(init_blk, graph_blk):
        blk = init_blk.shape[0]
        n = blk * num_rows
        half = blk // 2
        pieces = blk // TILE
        cores = 2 * num_rows
        any_spec = pl.BlockSpec(memory_space=pl.ANY)
        return pl.pallas_call(
            mcl_kernel,
            out_shape=pltpu.VMEM((blk, blk), jnp.float32),
            in_specs=[any_spec, any_spec],
            out_specs=pl.BlockSpec(memory_space=pltpu.VMEM),
            scratch_shapes=[
                pltpu.VMEM((num_cols, n, blk), jnp.bfloat16),
                pltpu.VMEM((half, n), jnp.bfloat16),
                pltpu.VMEM((half, n), jnp.bfloat16),
                pltpu.VMEM((2, half, blk), jnp.bfloat16),
                pltpu.VMEM((num_cols, half, blk), jnp.float32),
                pltpu.VMEM((half, blk), jnp.float32),
                pltpu.VMEM((3, 2, 1, blk), jnp.float32),
                pltpu.VMEM((3, cores, 2, 1, blk), jnp.float32),
                pltpu.VMEM((pieces, 2, 1, TILE), jnp.float32),
                pltpu.VMEM((pieces, cores, 2, 1, TILE), jnp.float32),
                pltpu.VMEM((2, 2, 1, blk), jnp.float32),
                pltpu.VMEM((cores, 2, 1, blk), jnp.float32),
                pltpu.VMEM((2, 1, blk), jnp.float32),
                pltpu.SemaphoreType.DMA((4,)),
                pltpu.SemaphoreType.DMA((2, pieces, SUBS)),
                pltpu.SemaphoreType.DMA((2, pieces)),
                pltpu.SemaphoreType.DMA((3, pieces)),
                pltpu.SemaphoreType.DMA((num_cols, pieces)),
                pltpu.SemaphoreType.DMA((SUBS,)),
                pltpu.SemaphoreType.DMA((3,)),
                pltpu.SemaphoreType.DMA((4 + num_cols,)),
                pltpu.SemaphoreType.DMA((4,)),
                pltpu.SemaphoreType.DMA((pieces + 4,)),
                pltpu.SemaphoreType.DMA((pieces + 4,)),
                pltpu.SemaphoreType.DMA((3, pieces)),
                pltpu.SemaphoreType.DMA((2,)),
            ],
            compiler_params=pltpu.CompilerParams(
                collective_id=0, has_side_effects=True, vmem_limit_bytes=60_000_000),
        )(init_blk, graph_blk)

    return jax.shard_map(device_step, mesh=mesh, in_specs=(block_spec, block_spec), out_specs=block_spec, check_vma=False)
```

```python
import jax
import jax.numpy as jnp
from jax import lax
from jax.experimental import pallas as pl
from jax.experimental.pallas import tpu as pltpu
from jax.sharding import PartitionSpec as P

SUBS = 4
TILE = 256
AHEAD = 3
LAG = 2
MESH = pl.DeviceIdType.MESH


def mcl_kernel(a_hbm, g_hbm, m_out, s_out, g, a, a1, snd, acc, fin, ps_mid, ar_mid, ps_edge, ar_edge, ps, ar, sc,
               load_sem, rm, re, ry, rp, ra_relay, ra, send_sem, fin_send, ar_send, ar_recv, fin_recv, sc_sem):
    n_col = g.shape[0]
    blk = g.shape[2]
    n = g.shape[1]
    half = blk // 2
    pieces = blk // TILE
    rows_s = blk // SUBS
    rows_a = half // SUBS
    turn = SUBS // 4

    z = lax.axis_index("col")
    r = lax.axis_index("row")
    y = r // 2
    c = r % 2
    side = z // 2
    middle = jnp.logical_or(z == 1, z == 2)
    zm = 1 + side
    zc = 3 * side
    zmo = 2 - side
    zco = 3 - 3 * side
    r_y = 2 * (1 - y) + c
    r_p = 2 * y + 1 - c

    def dev(zq, rq):
        return {"col": zq, "row": rq}

    def remote(src, dst, ssem, rsem, d):
        return pltpu.make_async_remote_copy(
            src_ref=src, dst_ref=dst, send_sem=ssem, recv_sem=rsem, device_id=d, device_id_type=MESH)

    def cols(j):
        return pl.ds(pl.multiple_of(j * TILE, TILE), TILE)

    def g_sub(zq, rq, j, s):
        return g.at[zq, pl.ds(pl.multiple_of(rq * blk + s * rows_s, rows_s), rows_s), cols(j)]

    def g_piece(zq, rq, j):
        return g.at[zq, pl.ds(pl.multiple_of(rq * blk, blk), blk), cols(j)]

    def g_block(zq, rq):
        return g.at[zq, pl.ds(pl.multiple_of(rq * blk, blk), blk), :]

    def copy_to(ref, ssem, rsem, d):
        remote(ref, ref, ssem, rsem, d).start()

    def wait_for(ref, rsem):
        remote(ref, ref, send_sem.at[0], rsem, dev(z, r)).wait_recv()

    def wait_sent(ref, ssem):
        remote(ref, ref, ssem, re.at[0, 0], dev(z, r)).wait_send()

    def send_partner(zq, rq, j):
        copy_to(g_piece(zq, rq, j), send_sem.at[4 + zq], rp.at[zq, j], dev(zm, r_p))

    def wait_partner(zq, j):
        wait_for(g.at[zq, pl.ds(0, 2 * blk), cols(j)], rp.at[zq, j])

    def quarter(zq):
        return pl.ds(pl.multiple_of(zq * blk, blk), blk)

    def a_quarter(zq):
        return a.at[:, quarter(zq)]

    def a_sub(s):
        return pl.ds(pl.multiple_of(s * rows_a, rows_a), rows_a)

    def out_rows(h):
        return pl.ds(pl.multiple_of(h * half, half), half)

    barrier = pltpu.get_barrier_semaphore()

    @pl.when(middle)
    def _():
        for dz in range(2):
            for dr in range(n_col):
                peer_z = zm if dz == 0 else zmo
                if dz == 0 and dr == 0:
                    peer_z = zc
                pl.semaphore_signal(barrier, inc=1, device_id=dev(peer_z, (r + dr) % n_col), device_id_type=MESH)

    @pl.when(jnp.logical_not(middle))
    def _():
        pl.semaphore_signal(barrier, inc=1, device_id=dev(zm, r), device_id_type=MESH)
        pl.semaphore_signal(barrier, inc=1, device_id=dev(zc, r_y), device_id_type=MESH)

    def load(src, h, slot):
        return pltpu.make_async_copy(src.at[out_rows(h), :], acc.at[slot], load_sem.at[slot])

    loads = (load(a_hbm, 1 - side, 0), load(g_hbm, 0, 1), load(g_hbm, 1, 2), load(a_hbm, side, 3))
    for copy in loads:
        copy.start()
    loads[0].wait()
    snd[0] = acc[0].astype(jnp.bfloat16)
    pl.semaphore_wait(barrier, jnp.where(middle, 2 * n_col, 2))

    @pl.when(middle)
    def _():
        remote(snd.at[0], a_quarter(zm), send_sem.at[3], ra.at[1], dev(zmo, r)).start()

    @pl.when(jnp.logical_not(middle))
    def _():
        @pl.loop(0, SUBS)
        def _(s):
            remote(snd.at[0, a_sub(s), :], snd.at[1, a_sub(s), :], send_sem.at[3], ra_relay.at[s], dev(zm, r)).start()

    for h in range(2):
        loads[1 + h].wait()
        g[z, pl.ds(pl.multiple_of(r * blk + h * half, half), half), :] = acc[1 + h].astype(jnp.bfloat16)

    @pl.when(jnp.logical_not(middle))
    def _():
        inner = dev(zm, r)

        @pl.loop(0, pieces)
        def _(j):
            copy_to(g_piece(z, r, j), send_sem.at[1], ry.at[0, j], dev(zc, r_y))

        loads[3].wait()
        a[:, quarter(z)] = acc[3].astype(jnp.bfloat16)
        remote(a_quarter(z), a_quarter(z), send_sem.at[3], ra.at[0], inner).start()

        @pl.loop(0, pieces)
        def _(j):
            copy_to(g_piece(z, r, j), send_sem.at[2], re.at[0, j], inner)

        @pl.loop(0, pieces)
        def _(j):
            wait_for(g_piece(z, r_y, j), ry.at[0, j])
            copy_to(g_piece(z, r_y, j), send_sem.at[2], re.at[1, j], inner)

        wait_sent(snd, send_sem.at[3])
        wait_sent(g_block(z, r), send_sem.at[1])
        wait_sent(g.at[0, pl.ds(0, 2 * blk), :], send_sem.at[2])

        for kind, h in ((1, side), (2, 1 - side)):
            @pl.loop(0, pieces)
            def _(j):
                wait_for(m_out.at[out_rows(h), cols(j)], fin_recv.at[kind, j])

        wait_for(s_out, sc_sem.at[1])

    @pl.when(middle)
    def _():
        other = dev(zmo, r)
        across = dev(zm, r_y)
        corner = dev(zc, r)
        me = side * n_col + r

        def peers():
            for dz in range(2):
                for dr in range(n_col):
                    if dz or dr:
                        yield dz == 0, (zmo if dz else zm), (r + dr) % n_col

        exchanges = [(ps_mid.at[0], ar_mid.at[0])]
        exchanges += [(ps_edge.at[j], ar_edge.at[j]) for j in range(pieces)]
        exchanges += [(ps_mid.at[1], ar_mid.at[1]), (ps_mid.at[2], ar_mid.at[2]), (ps, ar)]
        second_mid, second_edge, third = pieces + 1, pieces + 2, pieces + 3

        def sums_of(i):
            return exchanges[i]

        def send_sums(i):
            src, slots = sums_of(i)
            for same, pz, pr in peers():
                part = src.at[side if same else 1 - side] if i == third else src
                remote(part, slots.at[me], ar_send.at[i], ar_recv.at[i], dev(pz, pr)).start()
            slots[me] = src[side] if i == third else src[...]

        def peer_slots(i):
            return sums_of(i)[1].at[pl.ds(0, 2 * n_col - 1)]

        def scales(i):
            src, slots = sums_of(i)
            wait_for(peer_slots(i), ar_recv.at[i])
            total = slots[0]
            for peer in range(1, 2 * n_col):
                total = total + slots[peer]
            return n / total

        def square(value, zq, span, slot, keep=None):
            value = value * value
            if keep is None:
                acc[zq, :, span] = value
            else:
                fin[:, keep] = value
            slot[...] = jnp.sum(value, axis=0, keepdims=True)

        def expand(zq, j, slot, keep=None):
            square(jnp.dot(a[...], g[zq, :, cols(j)], preferred_element_type=jnp.float32), zq, cols(j), slot, keep)

        @pl.loop(0, pieces)
        def _(j):
            copy_to(g_piece(zm, r, j), send_sem.at[1], ry.at[0, j], across)
            send_partner(zm, r, j)

        loads[3].wait()
        a[:, quarter(zm)] = acc[3].astype(jnp.bfloat16)

        @pl.loop(0, SUBS)
        def _(s):
            wait_for(snd.at[1, a_sub(s), :], ra_relay.at[s])
            remote(snd.at[1, a_sub(s), :], a.at[a_sub(s), quarter(zc)], send_sem.at[3], ra.at[2], other).start()

        @pl.loop(0, pieces * SUBS)
        def _(i):
            copy_to(g_sub(zm, r, i // SUBS, i % SUBS), send_sem.at[0], rm.at[0, i // SUBS, i % SUBS], other)

        @pl.loop(0, pieces)
        def _(j):
            wait_for(g_piece(zm, r_y, j), ry.at[0, j])
            send_partner(zm, r_y, j)

        for idx, zq in ((1, zmo), (2, zco), (0, zc)):
            wait_for(a_quarter(zq), ra.at[idx])

        def finish_mid():
            scale = scales(0)
            for idx, zq in ((0, 1), (1, 2)):
                a1[:, pl.ds(zq * blk, blk)] = (acc[zq] * scale[idx]).astype(jnp.bfloat16)

        def finish_edge(j):
            scale = scales(1 + j)
            for idx, zq in ((0, 0), (1, 3)):
                kept = fin[:, cols(idx)] if j == pieces - 1 else acc[zq, :, pl.ds(j * TILE, TILE)]
                a1[:, pl.ds(zq * blk + j * TILE, TILE)] = (kept * scale[idx]).astype(jnp.bfloat16)

        def partial(rows, zq, k0, k_len, n0, n_len):
            k = pl.ds(pl.multiple_of(k0, TILE), k_len)
            return jnp.dot(rows[:, k], g[zq, k, pl.ds(pl.multiple_of(n0, TILE), n_len)],
                           preferred_element_type=jnp.float32)

        def two_quarters(rows, zq, k_len, n0, *k_z):
            first, second = (partial(rows, zq, k * blk, k_len, n0, TILE) for k in k_z)
            return first + second

        def mid_by_mid(zq):
            @pl.loop(0, pieces)
            def _(j):
                acc[zq, :, cols(j)] = two_quarters(a1, zq, blk, j * TILE, 1, 2)

        def new_columns(j):
            @pl.loop(0, 2)
            def _(i):
                zq = 3 * i
                acc[zq, :, pl.ds(j * TILE, TILE)] = (two_quarters(a1, zq, blk, j * TILE, 1, 2)
                                                     + two_quarters(a1, zq, (j + 1) * TILE, j * TILE, 0, 3))

        def last_new_columns(j):
            @pl.loop(0, 2)
            def _(i):
                zq = 3 * i
                acc[zq, :, cols(j)] = (two_quarters(a1, zq, blk, j * TILE, 1, 2)
                                   + two_quarters(a1, zq, j * TILE, j * TILE, 0, 3))

        def piece_update(j, zq, n0, width):
            return partial(a1, zq, j * TILE, TILE, n0, width) + partial(a1, zq, 3 * blk + j * TILE, TILE, n0, width)

        def old_columns(j, zq, width, slot):
            span = pl.ds(0, width)
            total = acc[zq, :, span] + piece_update(j, zq, 0, width)
            if j == pieces - 1:
                square(total, zq, span, slot.at[:, span])
            else:
                acc[zq, :, span] = total

        def old_mid(j):
            @pl.loop(0, 2)
            def _(i):
                old_columns(j, 1 + i, blk, ps_mid.at[1, i])

        def old_edge(j):
            if j:
                @pl.loop(0, 2)
                def _(i):
                    old_columns(j, 3 * i, blk if j == pieces - 1 else j * TILE, ps_mid.at[2, i])

        n_slices = pieces * SUBS

        def from_other(q):
            return zmo + (q // pieces) * (zco - zmo)

        def relay_ahead(i):
            ahead = i + AHEAD - n_slices

            @pl.when(jnp.logical_and(ahead >= 0, ahead < n_slices))
            def _():
                ref = g_sub(zc, r, ahead // SUBS, ahead % SUBS)
                copy_to(ref, send_sem.at[0], rm.at[1, ahead // SUBS, ahead % SUBS], other)

        def pump(i):
            q, s = i // SUBS, i % SUBS
            late, j = q // pieces, q % pieces
            z_m = from_other(q)
            ref = g_sub(z_m, r, j, s)
            wait_for(ref, rm.at[late, j, s])
            copy_to(ref, send_sem.at[1], ry.at[1 + late, j], across)

            @pl.when(s == SUBS - 1)
            def _():
                r_e = r + late * (r_y - r)
                send_partner(z_m, r, j)
                wait_for(g_piece(zc, r_e, j), re.at[late, j])
                send_partner(zc, r_e, j)

            @pl.when(jnp.logical_and(i >= LAG, (i - LAG) % SUBS == SUBS - 1))
            def _():
                piece_across((i - LAG) // SUBS)

        def piece_across(q):
            late, j = q // pieces, q % pieces
            wait_for(g_piece(from_other(q), r_y, j), ry.at[1 + late, j])
            send_partner(from_other(q), r_y, j)

        @pl.loop(0, pieces + 1)
        def _(q):
            @pl.loop(0, SUBS)
            def _(s):
                relay_ahead(q * SUBS + s)
                pump(q * SUBS + s)
                first = q == 0
                zq = jnp.where(first, zm, zmo)
                jq = jnp.where(first, s // turn, q - 1)

                @pl.when(jnp.logical_or(jnp.logical_and(first, s % turn == turn - 1), s == SUBS - 1))
                def _():
                    wait_partner(zq, jq)
                    expand(zq, jq, ps_mid.at[0, zq - 1, :, cols(jq)])

        send_sums(0)

        def edge_step(j, tasks):
            @pl.loop(0, SUBS)
            def _(s):
                i = (pieces + 1 + j) * SUBS + s
                pl.when(s != 3 * turn - 1)(lambda: relay_ahead(i))
                pump(i)

                @pl.when(s % (2 * turn) == turn - 1)
                def _():
                    zq = jnp.where(s == turn - 1, zc, zco)
                    wait_partner(zq, j)
                    expand(zq, j, ps_edge.at[j, zq // 3])

                @pl.when(s == 3 * turn - 1)
                def _():
                    send_sums(1 + j)
                    relay_ahead(i)

                for at, task in tasks.items():
                    pl.when(s == (at + 1) * turn - 1)(task)

        def mid_start():
            finish_mid()
            mid_by_mid(1)

        def edge_start(j):
            finish_edge(j)
            new_columns(j)

        def old(j):
            old_mid(j)
            old_edge(j)

        def first_piece():
            edge_start(0)
            old(0)

        edge_step(0, {3: mid_start})
        edge_step(1, {1: lambda: mid_by_mid(2), 3: first_piece})
        edge_step(2, {1: lambda: edge_start(1), 2: lambda: old_edge(1)})
        old_mid(1)

        last = pieces - 1

        def last_piece(zq):
            wait_partner(zq, last)
            expand(zq, last, ps_edge.at[last, zq // 3], cols(zq // 3))

        last_piece(zc)
        edge_start(last - 1)
        piece_across(2 * pieces - 1)
        old_mid(last - 1)
        last_piece(zco)
        send_sums(pieces)
        old_edge(last - 1)
        last_new_columns(last)
        finish_edge(last)
        old_mid(last)
        send_sums(second_mid)
        old_edge(last)
        send_sums(second_edge)

        def finish_second(i, *quarters):
            scale = scales(i)
            for idx, zq in enumerate(quarters):
                a[:, quarter(zq)] = (acc[zq] * scale[idx]).astype(jnp.bfloat16)

        finish_second(second_mid, 1, 2)

        @pl.loop(0, 2)
        def _(i):
            acc[zm, :, cols(i)] = two_quarters(a, zc + i * (zco - zc), blk, 0, 1, 2)

        finish_second(second_edge, 0, 3)

        def last_sums(zq, j):
            return ps.at[zq // 2, jnp.where(zq % 3 == 0, 1, 0), :, cols(j)]

        def send_result(i, zq, j):
            done = acc.at[zq, :, cols(j)]

            @pl.when(i == 0)
            def _():
                remote(done, m_out.at[out_rows(side), cols(j)], fin_send.at[1], fin_recv.at[1, j], corner).start()

            @pl.when(i == 1)
            def _():
                remote(done, fin.at[:, cols(j)], fin_send.at[0], fin_recv.at[2, j], other).start()

        @pl.loop(0, 2)
        def _(i):
            zq = zc + i * (zco - zc)
            square(acc[zm, :, cols(i)] + two_quarters(a, zq, blk, 0, 0, 3), zq, cols(0), last_sums(zq, 0))
            send_result(i, zq, 0)

        @pl.loop(1, pieces)
        def _(j):
            @pl.loop(0, 2)
            def _(i):
                zq = zc + i * (zco - zc)
                expand(zq, j, last_sums(zq, j))
                send_result(i, zq, j)

        @pl.loop(0, 2 * pieces)
        def _(i):
            zq = zmo + (i // pieces) * (zm - zmo)
            j = i % pieces
            expand(zq, j, last_sums(zq, j))

        send_sums(third)
        remote(acc.at[zmo], m_out.at[out_rows(side), :], fin_send.at[2], fin_recv.at[0, 0], other).start()
        m_out[out_rows(side), :] = acc[zm]

        @pl.loop(0, pieces)
        def _(j):
            ref = fin.at[:, cols(j)]
            wait_for(ref, fin_recv.at[2, j])
            remote(ref, m_out.at[out_rows(1 - side), cols(j)], fin_send.at[3], fin_recv.at[2, j], corner).start()

        sc[...] = scales(third)
        remote(sc.at[1], s_out, sc_sem.at[0], sc_sem.at[1], corner).start()
        s_out[...] = sc[0]

        wait_sent(snd, send_sem.at[3])
        wait_sent(g.at[0, pl.ds(0, 2 * blk), :], send_sem.at[0])
        wait_sent(g.at[0, pl.ds(0, 3 * blk), :], send_sem.at[1])
        for zq in range(n_col):
            wait_sent(g.at[0, pl.ds(0, 2 * blk), :], send_sem.at[4 + zq])
        for i in range(len(exchanges)):
            wait_sent(peer_slots(i), ar_send.at[i])
        for i in range(4):
            wait_sent(acc.at[0], fin_send.at[i])
        wait_sent(sc.at[0], sc_sem.at[0])
        wait_for(m_out.at[out_rows(1 - side), :], fin_recv.at[0, 0])


def solution(mesh):
    num_cols = mesh.shape["col"]
    num_rows = mesh.shape["row"]
    block_spec = P(("graph", "row"), "col")

    def device_step(init_blk, graph_blk):
        blk = init_blk.shape[0]
        n = blk * num_rows
        half = blk // 2
        pieces = blk // TILE
        cores = 2 * num_rows
        any_spec = pl.BlockSpec(memory_space=pl.ANY)
        vmem_spec = pl.BlockSpec(memory_space=pltpu.VMEM)
        squares, scale = pl.pallas_call(
            mcl_kernel,
            out_shape=(pltpu.VMEM((blk, blk), jnp.float32), pltpu.VMEM((1, blk), jnp.float32)),
            in_specs=[any_spec, any_spec],
            out_specs=(vmem_spec, vmem_spec),
            scratch_shapes=[
                pltpu.VMEM((num_cols, n, blk), jnp.bfloat16),
                pltpu.VMEM((half, n), jnp.bfloat16),
                pltpu.VMEM((half, n), jnp.bfloat16),
                pltpu.VMEM((2, half, blk), jnp.bfloat16),
                pltpu.VMEM((num_cols, half, blk), jnp.float32),
                pltpu.VMEM((half, blk), jnp.float32),
                pltpu.VMEM((3, 2, 1, blk), jnp.float32),
                pltpu.VMEM((3, cores, 2, 1, blk), jnp.float32),
                pltpu.VMEM((pieces, 2, 1, TILE), jnp.float32),
                pltpu.VMEM((pieces, cores, 2, 1, TILE), jnp.float32),
                pltpu.VMEM((2, 2, 1, blk), jnp.float32),
                pltpu.VMEM((cores, 2, 1, blk), jnp.float32),
                pltpu.VMEM((2, 1, blk), jnp.float32),
                pltpu.SemaphoreType.DMA((4,)),
                pltpu.SemaphoreType.DMA((2, pieces, SUBS)),
                pltpu.SemaphoreType.DMA((2, pieces)),
                pltpu.SemaphoreType.DMA((3, pieces)),
                pltpu.SemaphoreType.DMA((num_cols, pieces)),
                pltpu.SemaphoreType.DMA((SUBS,)),
                pltpu.SemaphoreType.DMA((3,)),
                pltpu.SemaphoreType.DMA((4 + num_cols,)),
                pltpu.SemaphoreType.DMA((4,)),
                pltpu.SemaphoreType.DMA((pieces + 4,)),
                pltpu.SemaphoreType.DMA((pieces + 4,)),
                pltpu.SemaphoreType.DMA((3, pieces)),
                pltpu.SemaphoreType.DMA((2,)),
            ],
            compiler_params=pltpu.CompilerParams(
                collective_id=0, has_side_effects=True, vmem_limit_bytes=60_000_000),
        )(init_blk, graph_blk)
        return squares * scale

    return jax.shard_map(device_step, mesh=mesh, in_specs=(block_spec, block_spec), out_specs=block_spec, check_vma=False)
```

```python
import jax
import jax.numpy as jnp
from jax import lax
from jax.experimental import pallas as pl
from jax.experimental.pallas import tpu as pltpu
from jax.sharding import PartitionSpec as P

SUBS = 4
TILE = 256
AHEAD = 3
LAG = 2
MESH = pl.DeviceIdType.MESH


def mcl_kernel(a_hbm, g_hbm, m_out, s_out, g, a, a1, snd, acc, fin, ps_mid, ar_mid, ps_edge, ar_edge, ps, ar, sc,
               load_sem, rm, re, ry, rp, ra_relay, ra, send_sem, fin_send, ar_send, ar_recv, fin_recv, sc_sem):
    n_col = g.shape[0]
    blk = g.shape[2]
    n = g.shape[1]
    half = blk // 2
    pieces = blk // TILE
    rows_s = blk // SUBS
    rows_a = half // SUBS
    turn = SUBS // 4

    z = lax.axis_index("col")
    r = lax.axis_index("row")
    y = r // 2
    c = r % 2
    side = z // 2
    middle = jnp.logical_or(z == 1, z == 2)
    zm = 1 + side
    zc = 3 * side
    zmo = 2 - side
    zco = 3 - 3 * side
    r_y = 2 * (1 - y) + c
    r_p = 2 * y + 1 - c

    def dev(zq, rq):
        return {"col": zq, "row": rq}

    def remote(src, dst, ssem, rsem, d):
        return pltpu.make_async_remote_copy(
            src_ref=src, dst_ref=dst, send_sem=ssem, recv_sem=rsem, device_id=d, device_id_type=MESH)

    def cols(j):
        return pl.ds(pl.multiple_of(j * TILE, TILE), TILE)

    def g_sub(zq, rq, j, s):
        return g.at[zq, pl.ds(pl.multiple_of(rq * blk + s * rows_s, rows_s), rows_s), cols(j)]

    def g_piece(zq, rq, j):
        return g.at[zq, pl.ds(pl.multiple_of(rq * blk, blk), blk), cols(j)]

    def g_block(zq, rq):
        return g.at[zq, pl.ds(pl.multiple_of(rq * blk, blk), blk), :]

    def copy_to(ref, ssem, rsem, d):
        remote(ref, ref, ssem, rsem, d).start()

    def wait_for(ref, rsem):
        remote(ref, ref, send_sem.at[0], rsem, dev(z, r)).wait_recv()

    def wait_sent(ref, ssem):
        remote(ref, ref, ssem, re.at[0, 0], dev(z, r)).wait_send()

    def send_partner(zq, rq, j):
        copy_to(g_piece(zq, rq, j), send_sem.at[4 + zq], rp.at[zq, j], dev(zm, r_p))

    def wait_partner(zq, j):
        wait_for(g.at[zq, pl.ds(0, 2 * blk), cols(j)], rp.at[zq, j])

    def quarter(zq):
        return pl.ds(pl.multiple_of(zq * blk, blk), blk)

    def a_quarter(zq):
        return a.at[:, quarter(zq)]

    def a_sub(s):
        return pl.ds(pl.multiple_of(s * rows_a, rows_a), rows_a)

    def out_rows(h):
        return pl.ds(pl.multiple_of(h * half, half), half)

    barrier = pltpu.get_barrier_semaphore()

    @pl.when(middle)
    def _():
        for dz in range(2):
            for dr in range(n_col):
                peer_z = zm if dz == 0 else zmo
                if dz == 0 and dr == 0:
                    peer_z = zc
                pl.semaphore_signal(barrier, inc=1, device_id=dev(peer_z, (r + dr) % n_col), device_id_type=MESH)

    @pl.when(jnp.logical_not(middle))
    def _():
        pl.semaphore_signal(barrier, inc=1, device_id=dev(zm, r), device_id_type=MESH)
        pl.semaphore_signal(barrier, inc=1, device_id=dev(zc, r_y), device_id_type=MESH)

    def load(src, h, slot):
        return pltpu.make_async_copy(src.at[out_rows(h), :], acc.at[slot], load_sem.at[slot])

    loads = (load(a_hbm, 1 - side, 0), load(g_hbm, 0, 1), load(g_hbm, 1, 2), load(a_hbm, side, 3))
    for copy in loads:
        copy.start()
    loads[0].wait()
    snd[0] = acc[0].astype(jnp.bfloat16)
    pl.semaphore_wait(barrier, jnp.where(middle, 2 * n_col, 2))

    @pl.when(middle)
    def _():
        remote(snd.at[0], a_quarter(zm), send_sem.at[3], ra.at[1], dev(zmo, r)).start()

    @pl.when(jnp.logical_not(middle))
    def _():
        @pl.loop(0, SUBS)
        def _(s):
            remote(snd.at[0, a_sub(s), :], snd.at[1, a_sub(s), :], send_sem.at[3], ra_relay.at[s], dev(zm, r)).start()

    for h in range(2):
        loads[1 + h].wait()
        g[z, pl.ds(pl.multiple_of(r * blk + h * half, half), half), :] = acc[1 + h].astype(jnp.bfloat16)

    @pl.when(jnp.logical_not(middle))
    def _():
        inner = dev(zm, r)

        @pl.loop(0, pieces)
        def _(j):
            copy_to(g_piece(z, r, j), send_sem.at[1], ry.at[0, j], dev(zc, r_y))

        loads[3].wait()
        a[:, quarter(z)] = acc[3].astype(jnp.bfloat16)
        remote(a_quarter(z), a_quarter(z), send_sem.at[3], ra.at[0], inner).start()

        @pl.loop(0, pieces)
        def _(j):
            copy_to(g_piece(z, r, j), send_sem.at[2], re.at[0, j], inner)

        @pl.loop(0, pieces)
        def _(j):
            wait_for(g_piece(z, r_y, j), ry.at[0, j])
            copy_to(g_piece(z, r_y, j), send_sem.at[2], re.at[1, j], inner)

        wait_sent(snd, send_sem.at[3])
        wait_sent(g_block(z, r), send_sem.at[1])
        wait_sent(g.at[0, pl.ds(0, 2 * blk), :], send_sem.at[2])

        for kind, h in ((1, side), (2, 1 - side)):
            @pl.loop(0, pieces)
            def _(j):
                wait_for(m_out.at[out_rows(h), cols(j)], fin_recv.at[kind, j])

        wait_for(s_out, sc_sem.at[1])

    @pl.when(middle)
    def _():
        other = dev(zmo, r)
        across = dev(zm, r_y)
        corner = dev(zc, r)
        me = side * n_col + r

        def peers():
            for dz in range(2):
                for dr in range(n_col):
                    if dz or dr:
                        yield dz == 0, (zmo if dz else zm), (r + dr) % n_col

        exchanges = [(ps_mid.at[0], ar_mid.at[0])]
        exchanges += [(ps_edge.at[j], ar_edge.at[j]) for j in range(pieces)]
        exchanges += [(ps_mid.at[1], ar_mid.at[1]), (ps_mid.at[2], ar_mid.at[2]), (ps, ar)]
        second_mid, second_edge, third = pieces + 1, pieces + 2, pieces + 3

        def sums_of(i):
            return exchanges[i]

        def send_sums(i):
            src, slots = sums_of(i)
            for same, pz, pr in peers():
                part = src.at[side if same else 1 - side] if i == third else src
                remote(part, slots.at[me], ar_send.at[i], ar_recv.at[i], dev(pz, pr)).start()
            slots[me] = src[side] if i == third else src[...]

        def peer_slots(i):
            return sums_of(i)[1].at[pl.ds(0, 2 * n_col - 1)]

        def scales(i):
            src, slots = sums_of(i)
            wait_for(peer_slots(i), ar_recv.at[i])
            total = slots[0]
            for peer in range(1, 2 * n_col):
                total = total + slots[peer]
            return n / total

        def square(value, zq, span, slot, keep=None):
            value = value * value
            if keep is None:
                acc[zq, :, span] = value
            else:
                fin[:, keep] = value
            slot[...] = jnp.sum(value, axis=0, keepdims=True)

        def expand(zq, j, slot, keep=None):
            square(jnp.dot(a[...], g[zq, :, cols(j)], preferred_element_type=jnp.float32), zq, cols(j), slot, keep)

        @pl.loop(0, pieces)
        def _(j):
            copy_to(g_piece(zm, r, j), send_sem.at[1], ry.at[0, j], across)
            send_partner(zm, r, j)

        loads[3].wait()
        a[:, quarter(zm)] = acc[3].astype(jnp.bfloat16)

        @pl.loop(0, SUBS)
        def _(s):
            wait_for(snd.at[1, a_sub(s), :], ra_relay.at[s])
            remote(snd.at[1, a_sub(s), :], a.at[a_sub(s), quarter(zc)], send_sem.at[3], ra.at[2], other).start()

        @pl.loop(0, pieces * SUBS)
        def _(i):
            copy_to(g_sub(zm, r, i // SUBS, i % SUBS), send_sem.at[0], rm.at[0, i // SUBS, i % SUBS], other)

        @pl.loop(0, pieces)
        def _(j):
            wait_for(g_piece(zm, r_y, j), ry.at[0, j])
            send_partner(zm, r_y, j)

        for idx, zq in ((1, zmo), (2, zco), (0, zc)):
            wait_for(a_quarter(zq), ra.at[idx])

        def finish_mid():
            scale = scales(0)
            for idx, zq in ((0, 1), (1, 2)):
                a1[:, pl.ds(zq * blk, blk)] = (acc[zq] * scale[idx]).astype(jnp.bfloat16)

        def finish_edge(j):
            scale = scales(1 + j)
            for idx, zq in ((0, 0), (1, 3)):
                kept = fin[:, cols(idx)] if j == pieces - 1 else acc[zq, :, pl.ds(j * TILE, TILE)]
                a1[:, pl.ds(zq * blk + j * TILE, TILE)] = (kept * scale[idx]).astype(jnp.bfloat16)

        def partial(rows, zq, k0, k_len, n0, n_len):
            k = pl.ds(pl.multiple_of(k0, TILE), k_len)
            return jnp.dot(rows[:, k], g[zq, k, pl.ds(pl.multiple_of(n0, TILE), n_len)],
                           preferred_element_type=jnp.float32)

        def two_quarters(rows, zq, k_len, n0, *k_z):
            first, second = (partial(rows, zq, k * blk, k_len, n0, TILE) for k in k_z)
            return first + second

        def mid_by_mid(zq, j0, j1):
            @pl.loop(j0, j1)
            def _(j):
                acc[zq, :, cols(j)] = two_quarters(a1, zq, blk, j * TILE, 1, 2)

        def new_columns(j):
            @pl.loop(0, 2)
            def _(i):
                zq = 3 * i
                acc[zq, :, pl.ds(j * TILE, TILE)] = (two_quarters(a1, zq, blk, j * TILE, 1, 2)
                                                     + two_quarters(a1, zq, (j + 1) * TILE, j * TILE, 0, 3))

        def last_new_columns(j):
            @pl.loop(0, 2)
            def _(i):
                zq = 3 * i
                acc[zq, :, cols(j)] = (two_quarters(a1, zq, blk, j * TILE, 1, 2)
                                   + two_quarters(a1, zq, j * TILE, j * TILE, 0, 3))

        def piece_update(j, zq, n0, width):
            return partial(a1, zq, j * TILE, TILE, n0, width) + partial(a1, zq, 3 * blk + j * TILE, TILE, n0, width)

        def old_columns(j, zq, width, slot):
            span = pl.ds(0, width)
            total = acc[zq, :, span] + piece_update(j, zq, 0, width)
            if j == pieces - 1:
                square(total, zq, span, slot.at[:, span])
            else:
                acc[zq, :, span] = total

        def old_mid(j):
            @pl.loop(0, 2)
            def _(i):
                old_columns(j, 1 + i, blk, ps_mid.at[1, i])

        def old_edge(j):
            if j:
                @pl.loop(0, 2)
                def _(i):
                    old_columns(j, 3 * i, blk if j == pieces - 1 else j * TILE, ps_mid.at[2, i])

        n_slices = pieces * SUBS

        def from_other(q):
            return zmo + (q // pieces) * (zco - zmo)

        def relay_ahead(i):
            ahead = i + AHEAD - n_slices

            @pl.when(jnp.logical_and(ahead >= 0, ahead < n_slices))
            def _():
                ref = g_sub(zc, r, ahead // SUBS, ahead % SUBS)
                copy_to(ref, send_sem.at[0], rm.at[1, ahead // SUBS, ahead % SUBS], other)

        def pump(i):
            q, s = i // SUBS, i % SUBS
            late, j = q // pieces, q % pieces
            z_m = from_other(q)
            ref = g_sub(z_m, r, j, s)
            wait_for(ref, rm.at[late, j, s])
            copy_to(ref, send_sem.at[1], ry.at[1 + late, j], across)

            @pl.when(s == SUBS - 1)
            def _():
                r_e = r + late * (r_y - r)
                send_partner(z_m, r, j)
                wait_for(g_piece(zc, r_e, j), re.at[late, j])
                send_partner(zc, r_e, j)

            @pl.when(jnp.logical_and(i >= LAG, (i - LAG) % SUBS == SUBS - 1))
            def _():
                piece_across((i - LAG) // SUBS)

        def piece_across(q):
            late, j = q // pieces, q % pieces
            wait_for(g_piece(from_other(q), r_y, j), ry.at[1 + late, j])
            send_partner(from_other(q), r_y, j)

        @pl.loop(0, pieces + 1)
        def _(q):
            @pl.loop(0, SUBS)
            def _(s):
                relay_ahead(q * SUBS + s)
                pump(q * SUBS + s)
                first = q == 0
                zq = jnp.where(first, zm, zmo)
                jq = jnp.where(first, s // turn, q - 1)

                @pl.when(jnp.logical_or(jnp.logical_and(first, s % turn == turn - 1), s == SUBS - 1))
                def _():
                    wait_partner(zq, jq)
                    expand(zq, jq, ps_mid.at[0, zq - 1, :, cols(jq)])

        send_sums(0)

        def edge_step(j, tasks):
            @pl.loop(0, SUBS)
            def _(s):
                i = (pieces + 1 + j) * SUBS + s
                pl.when(s != 3 * turn - 1)(lambda: relay_ahead(i))
                pump(i)

                @pl.when(s % (2 * turn) == turn - 1)
                def _():
                    zq = jnp.where(s == turn - 1, zc, zco)
                    wait_partner(zq, j)
                    expand(zq, j, ps_edge.at[j, zq // 3])

                @pl.when(s == 3 * turn - 1)
                def _():
                    send_sums(1 + j)
                    relay_ahead(i)

                for at, task in tasks.items():
                    pl.when(s == (at + 1) * turn - 1)(task)

        def mid_start():
            finish_mid()
            mid_by_mid(1, 0, pieces // 2)

        def edge_start(j):
            finish_edge(j)
            new_columns(j)

        def old(j):
            old_mid(j)
            old_edge(j)

        edge_step(0, {3: mid_start})
        edge_step(1, {0: lambda: mid_by_mid(1, pieces // 2, pieces), 1: lambda: mid_by_mid(2, 0, pieces),
                      3: lambda: edge_start(0)})
        edge_step(2, {0: lambda: old(0), 1: lambda: edge_start(1), 2: lambda: old_edge(1)})
        old_mid(1)

        last = pieces - 1

        def last_piece(zq):
            wait_partner(zq, last)
            expand(zq, last, ps_edge.at[last, zq // 3], cols(zq // 3))

        last_piece(zc)
        edge_start(last - 1)
        piece_across(2 * pieces - 1)
        old_mid(last - 1)
        last_piece(zco)
        send_sums(pieces)
        old_edge(last - 1)
        last_new_columns(last)
        finish_edge(last)
        old_mid(last)
        send_sums(second_mid)
        old_edge(last)
        send_sums(second_edge)

        def finish_second(i, *quarters):
            scale = scales(i)
            for idx, zq in enumerate(quarters):
                a[:, quarter(zq)] = (acc[zq] * scale[idx]).astype(jnp.bfloat16)

        finish_second(second_mid, 1, 2)

        @pl.loop(0, 2)
        def _(i):
            acc[zm, :, cols(i)] = two_quarters(a, zc + i * (zco - zc), blk, 0, 1, 2)

        finish_second(second_edge, 0, 3)

        def last_sums(zq, j):
            return ps.at[zq // 2, jnp.where(zq % 3 == 0, 1, 0), :, cols(j)]

        def send_result(i, zq, j):
            done = acc.at[zq, :, cols(j)]

            @pl.when(i == 0)
            def _():
                remote(done, m_out.at[out_rows(side), cols(j)], fin_send.at[1], fin_recv.at[1, j], corner).start()

            @pl.when(i == 1)
            def _():
                remote(done, fin.at[:, cols(j)], fin_send.at[0], fin_recv.at[2, j], other).start()

        @pl.loop(0, 2)
        def _(i):
            zq = zc + i * (zco - zc)
            square(acc[zm, :, cols(i)] + two_quarters(a, zq, blk, 0, 0, 3), zq, cols(0), last_sums(zq, 0))
            send_result(i, zq, 0)

        @pl.loop(1, pieces)
        def _(j):
            @pl.loop(0, 2)
            def _(i):
                zq = zc + i * (zco - zc)
                expand(zq, j, last_sums(zq, j))
                send_result(i, zq, j)

        @pl.loop(0, 2 * pieces)
        def _(i):
            zq = zmo + (i // pieces) * (zm - zmo)
            j = i % pieces
            expand(zq, j, last_sums(zq, j))

        send_sums(third)
        remote(acc.at[zmo], m_out.at[out_rows(side), :], fin_send.at[2], fin_recv.at[0, 0], other).start()
        m_out[out_rows(side), :] = acc[zm]

        @pl.loop(0, pieces)
        def _(j):
            ref = fin.at[:, cols(j)]
            wait_for(ref, fin_recv.at[2, j])
            remote(ref, m_out.at[out_rows(1 - side), cols(j)], fin_send.at[3], fin_recv.at[2, j], corner).start()

        sc[...] = scales(third)
        remote(sc.at[1], s_out, sc_sem.at[0], sc_sem.at[1], corner).start()
        s_out[...] = sc[0]

        wait_sent(snd, send_sem.at[3])
        wait_sent(g.at[0, pl.ds(0, 2 * blk), :], send_sem.at[0])
        wait_sent(g.at[0, pl.ds(0, 3 * blk), :], send_sem.at[1])
        for zq in range(n_col):
            wait_sent(g.at[0, pl.ds(0, 2 * blk), :], send_sem.at[4 + zq])
        for i in range(len(exchanges)):
            wait_sent(peer_slots(i), ar_send.at[i])
        for i in range(4):
            wait_sent(acc.at[0], fin_send.at[i])
        wait_sent(sc.at[0], sc_sem.at[0])
        wait_for(m_out.at[out_rows(1 - side), :], fin_recv.at[0, 0])


def solution(mesh):
    num_cols = mesh.shape["col"]
    num_rows = mesh.shape["row"]
    block_spec = P(("graph", "row"), "col")

    def device_step(init_blk, graph_blk):
        blk = init_blk.shape[0]
        n = blk * num_rows
        half = blk // 2
        pieces = blk // TILE
        cores = 2 * num_rows
        any_spec = pl.BlockSpec(memory_space=pl.ANY)
        vmem_spec = pl.BlockSpec(memory_space=pltpu.VMEM)
        squares, scale = pl.pallas_call(
            mcl_kernel,
            out_shape=(pltpu.VMEM((blk, blk), jnp.float32), pltpu.VMEM((1, blk), jnp.float32)),
            in_specs=[any_spec, any_spec],
            out_specs=(vmem_spec, vmem_spec),
            scratch_shapes=[
                pltpu.VMEM((num_cols, n, blk), jnp.bfloat16),
                pltpu.VMEM((half, n), jnp.bfloat16),
                pltpu.VMEM((half, n), jnp.bfloat16),
                pltpu.VMEM((2, half, blk), jnp.bfloat16),
                pltpu.VMEM((num_cols, half, blk), jnp.float32),
                pltpu.VMEM((half, blk), jnp.float32),
                pltpu.VMEM((3, 2, 1, blk), jnp.float32),
                pltpu.VMEM((3, cores, 2, 1, blk), jnp.float32),
                pltpu.VMEM((pieces, 2, 1, TILE), jnp.float32),
                pltpu.VMEM((pieces, cores, 2, 1, TILE), jnp.float32),
                pltpu.VMEM((2, 2, 1, blk), jnp.float32),
                pltpu.VMEM((cores, 2, 1, blk), jnp.float32),
                pltpu.VMEM((2, 1, blk), jnp.float32),
                pltpu.SemaphoreType.DMA((4,)),
                pltpu.SemaphoreType.DMA((2, pieces, SUBS)),
                pltpu.SemaphoreType.DMA((2, pieces)),
                pltpu.SemaphoreType.DMA((3, pieces)),
                pltpu.SemaphoreType.DMA((num_cols, pieces)),
                pltpu.SemaphoreType.DMA((SUBS,)),
                pltpu.SemaphoreType.DMA((3,)),
                pltpu.SemaphoreType.DMA((4 + num_cols,)),
                pltpu.SemaphoreType.DMA((4,)),
                pltpu.SemaphoreType.DMA((pieces + 4,)),
                pltpu.SemaphoreType.DMA((pieces + 4,)),
                pltpu.SemaphoreType.DMA((3, pieces)),
                pltpu.SemaphoreType.DMA((2,)),
            ],
            compiler_params=pltpu.CompilerParams(
                collective_id=0, has_side_effects=True, vmem_limit_bytes=60_000_000),
        )(init_blk, graph_blk)
        return squares * scale

    return jax.shard_map(device_step, mesh=mesh, in_specs=(block_spec, block_spec), out_specs=block_spec, check_vma=False)
```
